32 devices in a mesh: seq: 16 (over z, x, core), zero: 2 (over y).
Axes of the slice: x: 2, y: 2, z: 4, core: 2. Of those that a mesh axis runs over, the one named last changes fastest.
Arguments:
- tokens: bfloat16 [2, 2048, 2048], P('zero', 'seq'), may hold values from -6 to 6
- w_in: bfloat16 [2048, 2336], P('zero'), may hold values from -0.0625 to 0.0625
- a_log: float32 [32], replicated, may hold values from -8 to 0
- dt_bias: float32 [32], replicated, may hold values from -4.5 to -3.5
- d_skip: float32 [32], replicated, may hold values from 0.5 to 1.5
- grad_y: bfloat16 [2, 2048, 2048], P('zero', 'seq'), may hold values from -6 to 6
Outputs:
- y_out: bfloat16 [2, 2048, 2048], P('zero', 'seq')
- grad_tokens: bfloat16 [2, 2048, 2048], P('zero', 'seq')
- grad_w: float32 [2048, 2336], P(('seq', 'zero'))
The draws below stay inside these ranges and needn't reach their ends.
All inputs are finite; a program needn't handle non-finite values.
Results may differ from the reference program's by a relative error of at most 0.013.
Values may be sent and summed in bfloat16 or wider, within the bound.
A program may use at most 128 MiB of HBM per device.

```python
import jax
import jax.numpy as jnp
from jax import lax

D = 2048
STATE = 128
HEADS = 32
HEAD_SIZE = 64
TOK_DEV = 128
INNER = 2048
PROJ = 2336
BATCH = 2
LENGTH = 2048
N_SEQ = 16


def block_scale(own_key, extent, shards, least, top_value):
    level, own = 1.0, jax.random.fold_in(own_key, 6)
    for axis_at, shards_of in shards:
        draws = jnp.exp(jax.random.uniform(jax.random.fold_in(own, axis_at), (shards_of,), jnp.float32, least / len(shards), top_value / len(shards)))
        level = level * jnp.repeat(draws, extent[axis_at] // shards_of).reshape([-1 if axis == axis_at else 1 for axis in range(len(extent))])
    return level


def noise(own_key, shape, scale, reach, cuts=(), kind=jnp.bfloat16):
    gain = block_scale(own_key, shape, cuts, -0.22, 0.18) if cuts else 1.0
    result = jax.random.normal(own_key, shape, jnp.float32) * scale * gain
    return jnp.minimum(jnp.maximum(result, -reach), reach).astype(kind)


def setup_inputs(seed: int = 0) -> dict:
    keys = jax.random.split(jax.random.key(seed), 7)
    return {
        "tokens": noise(keys[0], (BATCH, LENGTH, D), 1.0, 6.0, ((0, 2), (1, 16))),
        "w_in": noise(keys[1], (D, PROJ), (4 * D) ** -0.5, 0.0625, ((0, 2),)),
        "a_log": jnp.clip(jax.random.uniform(keys[2], (HEADS,), jnp.float32, -8.0, 0.0), -8.0, 0.0),
        "dt_bias": jnp.clip(jax.random.uniform(keys[3], (HEADS,), jnp.float32, -4.5, -3.5), -4.5, -3.5),
        "d_skip": jnp.clip(jax.random.uniform(keys[4], (HEADS,), jnp.float32, 0.5, 1.5), 0.5, 1.5),
        "grad_y": noise(keys[5], (BATCH, LENGTH, INNER), 1.0, 6.0, ((0, 2), (1, 16))),
    }


def block_ssd(xs, bm, cm, raw, start, a_log, dt_bias, d_skip):
    high = lax.Precision.HIGHEST
    dt = jax.nn.softplus(raw + dt_bias)
    loga = -jnp.exp(a_log) * dt
    cum = jnp.cumsum(loga, axis=0)
    count = xs.shape[0]
    later = (jnp.arange(count)[:, None] >= jnp.arange(count)[None, :])[:, :, None]
    spans = cum[:, None, :] - cum[None, :, :]
    decay = jnp.where(later, jnp.exp(jnp.where(later, spans, 0.0)), 0.0)
    scores = jnp.dot(cm, bm.T, precision=high)
    mixing = scores[:, :, None] * decay * dt[None, :, :]
    ssd = jnp.einsum('tsh,shp->thp', mixing, xs, precision=high)
    ssd = ssd + jnp.einsum('tn,th,hpn->thp', cm, jnp.exp(cum), start, precision=high)
    out = ssd + d_skip[None, :, None] * xs
    tail = jnp.exp(cum[-1:] - cum) * dt
    state = jnp.exp(cum[-1])[:, None, None] * start + jnp.einsum('sh,sn,shp->hpn', tail, bm, xs, precision=high)
    return (out, state)

def reference(tokens, w_in, a_log, dt_bias, d_skip, grad_y):
    proj = jnp.dot(tokens.reshape(BATCH * LENGTH, D), w_in, preferred_element_type=jnp.float32)
    proj = proj.reshape(BATCH, LENGTH, PROJ)
    xs = lax.optimization_barrier(proj[:, :, :INNER].astype(jnp.bfloat16)).astype(jnp.float32)
    bm = lax.optimization_barrier(proj[:, :, INNER:INNER + STATE].astype(jnp.bfloat16)).astype(jnp.float32)
    cm = lax.optimization_barrier(proj[:, :, INNER + STATE:INNER + 2 * STATE].astype(jnp.bfloat16)).astype(jnp.float32)
    raw = proj[:, :, INNER + 2 * STATE:]
    blocks = LENGTH // TOK_DEV

    def forward(xseq, bseq, cseq, rseq):
        xb = xseq.reshape(blocks, TOK_DEV, HEADS, HEAD_SIZE)
        bb = bseq.reshape(blocks, TOK_DEV, STATE)
        cb = cseq.reshape(blocks, TOK_DEV, STATE)
        rb = rseq.reshape(blocks, TOK_DEV, HEADS)

        def step(carry, item):
            out, state = block_ssd(item[0], item[1], item[2], item[3], carry, a_log, dt_bias, d_skip)
            return (state, out)
        initial = jnp.zeros((HEADS, HEAD_SIZE, STATE), jnp.float32)
        final, outs = lax.scan(step, initial, (xb, bb, cb, rb))
        return outs.reshape(LENGTH, INNER)

    def one_sequence(item):
        xseq, bseq, cseq, rseq, gseq = item
        out, pullback = jax.vjp(forward, xseq, bseq, cseq, rseq)
        gx, gb, gc, gr = pullback(gseq.astype(jnp.float32))
        return (out, jnp.concatenate([gx, gb, gc, gr], axis=1))
    outs, grads = lax.map(one_sequence, (xs, bm, cm, raw, grad_y))
    y_out = outs.astype(jnp.bfloat16)
    gproj = grads.astype(jnp.bfloat16)
    grad_tokens = jnp.dot(gproj.reshape(BATCH * LENGTH, PROJ), w_in.T, preferred_element_type=jnp.float32)
    grad_tokens = grad_tokens.astype(jnp.bfloat16).reshape(BATCH, LENGTH, D)
    ublocks = tokens.reshape(BATCH * N_SEQ, TOK_DEV, D)
    gblocks = gproj.reshape(BATCH * N_SEQ, TOK_DEV, PROJ)

    def add_part(total, item):
        part = jnp.dot(item[0].T, item[1], preferred_element_type=jnp.float32)
        part = lax.optimization_barrier(part.astype(jnp.bfloat16)).astype(jnp.float32)
        return (total + part, None)
    grad_w, unused = lax.scan(add_part, jnp.zeros((D, PROJ), jnp.float32), (ublocks, gblocks))
    return (y_out, grad_tokens, grad_w)
```

```python
import functools

import jax
import jax.numpy as jnp
from jax import lax
from jax.experimental import pallas as pl
from jax.experimental.pallas import tpu as pltpu
from jax.sharding import PartitionSpec as P

BF = jnp.bfloat16
F32 = jnp.float32
MESH = pl.DeviceIdType.MESH


def shift(value, axis, step):
    count = lax.axis_size(axis)
    return lax.ppermute(value, axis, [(i, (i + step) % count) for i in range(count)])


def dot(a, b, dims):
    return lax.dot_general(a, b, (dims, ((), ())), preferred_element_type=F32)


def bdot(a, b, spec):
    return jnp.einsum(spec, a, b, preferred_element_type=F32)


def greet(peers, mates=()):
    barrier = pltpu.get_barrier_semaphore()
    for peer in peers:
        pl.semaphore_signal(barrier, inc=1, device_id={"seq": peer}, device_id_type=MESH)
    for mate in mates:
        pl.semaphore_signal(barrier, inc=1, device_id={"zero": mate}, device_id_type=MESH)
    pl.semaphore_wait(barrier, len(peers) + len(mates))


def remote(src, dst, send, recv, peer):
    return pltpu.make_async_remote_copy(
        src_ref=src,
        dst_ref=dst,
        send_sem=send,
        recv_sem=recv,
        device_id={"seq": peer},
        device_id_type=MESH,
    )


def scan_kernel(
    pair, totals, start, end, both, marks, joined, sums, got, lengths, made, back, final, wide,
    send, recv, local
):
    chips, _, share = pair.shape[:3]
    me = lax.axis_index("seq")
    core, chip = lax.rem(me, 2), lax.div(me, 2)
    sibling = me + 1 - 2 * core
    places = [lax.rem(chip + d, chips) for d in range(1, chips)]
    peers = [place * 2 + core for place in places]
    greet([sibling] + peers)

    def move(copies):
        for copy in copies:
            copy.start()
        for copy in copies:
            copy.wait()

    move(
        [
            remote(pair.at[:, 1 - core], both.at[core], send.at[0, 0], recv.at[0, 0], sibling),
            remote(totals.at[:, 1 - core], marks.at[core], send.at[1, 0], recv.at[1, 0], sibling),
            pltpu.make_async_copy(pair.at[:, core], both.at[core], local.at[0]),
            pltpu.make_async_copy(totals.at[:, core], marks.at[core], local.at[1]),
        ]
    )

    def gain(ref, *at):
        return jnp.exp(ref[at])

    for k in range(chips):
        sums[k] = marks[0, k] + marks[1, k]
        for j in range(share):
            row = pl.ds(j, 1)
            joined[k, j, 0] = (
                gain(marks, 1, k, row) * both[0, k, j, 0].astype(F32)
                + both[1, k, j, 0].astype(F32)
            ).astype(BF)
            joined[k, j, 1] = (
                gain(marks, 0, k, row) * both[1, k, j, 1].astype(F32)
                + both[0, k, j, 1].astype(F32)
            ).astype(BF)
    copies = []
    for d, (place, peer) in enumerate(zip(places, peers)):
        copies.append(remote(joined.at[place], got.at[chip], send.at[2, d], recv.at[2, d], peer))
        copies.append(remote(sums.at[place], lengths.at[chip], send.at[3, d], recv.at[3, d], peer))
    copies.append(pltpu.make_async_copy(joined.at[chip], got.at[chip], local.at[2]))
    copies.append(pltpu.make_async_copy(sums.at[chip], lengths.at[chip], local.at[3]))
    move(copies)

    for j in range(share):
        row = pl.ds(j, 1)
        run = jnp.zeros(pair.shape[4:], F32)
        for k in range(chips):
            made[k, j, 0] = run.astype(BF)
            if k < chips - 1:
                run = gain(lengths, k, row) * run + got[k, j, 0].astype(F32)
        run = jnp.zeros(pair.shape[4:], F32)
        for k in reversed(range(chips)):
            made[k, j, 1] = run.astype(BF)
            if k > 0:
                run = gain(lengths, k, row) * run + got[k, j, 1].astype(F32)
    copies = [
        remote(made.at[place], back.at[chip], send.at[4, d], recv.at[4, d], peer)
        for d, (place, peer) in enumerate(zip(places, peers))
    ]
    move(copies + [pltpu.make_async_copy(made.at[chip], back.at[chip], local.at[4])])

    for k in range(chips):
        for j in range(share):
            row = pl.ds(j, 1)
            first, last = back[k, j, 0], back[k, j, 1]
            final[0, k, j, 0] = first
            final[1, k, j, 1] = last
            final[1, k, j, 0] = (
                gain(marks, 0, k, row) * first.astype(F32) + both[0, k, j, 0].astype(F32)
            ).astype(BF)
            final[0, k, j, 1] = (
                gain(marks, 1, k, row) * last.astype(F32) + both[1, k, j, 1].astype(F32)
            ).astype(BF)
    move(
        [
            remote(final.at[1 - core], wide.at[core], send.at[5, 0], recv.at[5, 0], sibling),
            pltpu.make_async_copy(final.at[core], wide.at[core], local.at[5]),
        ]
    )
    for parity in range(2):
        start[:, parity] = wide[parity, :, :, 0]
        end[:, parity] = wide[parity, :, :, 1]


def scan_states(pair, totals):
    chips, _, share, _, rows, lanes = pair.shape
    state = jax.ShapeDtypeStruct((chips, 2, share, rows, lanes), BF)
    half = (chips,) + pair.shape[2:]
    short = (chips,) + totals.shape[2:]
    return pl.pallas_call(
        scan_kernel,
        out_shape=(state, state),
        in_specs=[pl.BlockSpec(memory_space=pltpu.VMEM)] * 2,
        out_specs=[pl.BlockSpec(memory_space=pltpu.VMEM)] * 2,
        scratch_shapes=[
            pltpu.VMEM((2,) + half, BF),
            pltpu.VMEM((2,) + short, F32),
            pltpu.VMEM(half, BF),
            pltpu.VMEM(short, F32),
            pltpu.VMEM(half, BF),
            pltpu.VMEM(short, F32),
            pltpu.VMEM(half, BF),
            pltpu.VMEM(half, BF),
            pltpu.VMEM((2,) + half, BF),
            pltpu.VMEM((2,) + half, BF),
            pltpu.SemaphoreType.DMA((6, chips)),
            pltpu.SemaphoreType.DMA((6, chips)),
            pltpu.SemaphoreType.DMA((6,)),
        ],
        compiler_params=pltpu.CompilerParams(collective_id=0, has_side_effects=True),
    )(pair, totals)


def tail_kernel(spans, tile, own, left, weights, out, grads, right, *scratch):
    seq, zero = 2 * left.shape[1], left.shape[3] // own.shape[0]
    levels = (seq // 2).bit_length() - 1
    me, here = lax.axis_index("seq"), lax.axis_index("zero")
    core, place = lax.rem(me, 2), lax.div(me, 2)
    bits = [lax.rem(lax.div(place, 1 << b), 2) for b in range(levels)]
    sibling = me + 1 - 2 * core
    partners = [me + (1 - 2 * bits[b]) * (2 << b) for b in range(levels)]
    after = [lax.rem(here + s, zero) for s in range(zero)]
    before = [lax.rem(here + zero - s, zero) for s in range(zero)]
    greet([sibling] + partners, after[1:])
    pieces, piece, tokens = left.shape[1:]
    count = own.shape[0]
    parts = len(spans)
    up = list(range(levels))
    orders = [up[1:] + up[:1]] + [up] * (parts - 1)
    acc, away, come = (scratch[i * parts : (i + 1) * parts] for i in range(3))
    rest = scratch[3 * parts : -7]
    outs = [rest[h * levels : (h + 1) * levels] for h in range(parts)]
    ins = [rest[(parts + h) * levels : (parts + h + 1) * levels] for h in range(parts)]
    made, send, recv, put, got, leave, enter = scratch[-7:]

    arriving = []
    for h, (low, high) in enumerate(spans):
        arriving.append([])
        for s in range(1, zero):
            copy = pltpu.make_async_remote_copy(
                src_ref=own.at[:, low:high],
                dst_ref=right.at[s * count : (s + 1) * count, low:high],
                send_sem=put.at[h, s],
                recv_sem=got.at[h, s],
                device_id={"zero": after[s]},
                device_id_type=MESH,
            )
            copy.start()
            arriving[h].append(copy)
    right[:count] = own[...]

    owned = weights.shape[0]
    base = pl.multiple_of(here * owned, 128)

    def project(rows, target, first):
        @pl.loop(0, owned // tile)
        def _(i):
            at = pl.multiple_of(i * tile, 128)
            value = dot(rows[...], weights[pl.ds(at, tile)], ((1,), (1,)))
            target[:, pl.ds(pl.multiple_of(first + at, 128), tile)] = value.astype(BF)

    project(own, grads, base)

    def multiply(side, h, target):
        low, high = spans[h]
        rows = left[side].reshape(pieces * piece, tokens)
        value = jnp.dot(rows, right[:, low:high], preferred_element_type=F32)
        target[...] = value.reshape(target.shape).astype(target.dtype)

    first = []

    def front(h):
        for copy in arriving[h]:
            copy.wait()
        multiply(1 - core, h, away[h])
        copy = remote(away[h], come[h], send.at[h, levels], recv.at[h, levels], sibling)
        copy.start()
        first.append(copy)
        multiply(core, h, acc[h])

    def join(h):
        first[h].wait()

        @pl.loop(0, pieces)
        def _(i):
            acc[h][i] += come[h][i].astype(F32)

    def subsets(rest):
        found = [0]
        for b in rest:
            found = found + [value + (1 << b) for value in found]
        return found

    flying = {}

    def begin(h, s):
        order = orders[h]
        b = order[s]
        base = sum((bits[f] * (1 << f) for f in order[:s]), 0)
        for j, extra in enumerate(subsets(order[s + 1 :])):
            outs[h][s][j] = acc[h][base + (1 - bits[b]) * (1 << b) + extra].astype(BF)
        copy = remote(outs[h][s], ins[h][s], send.at[h, s], recv.at[h, s], partners[b])
        copy.start()
        flying[h] = copy

    def finish(h, s):
        flying[h].wait()
        order = orders[h]
        base = sum((bits[f] * (1 << f) for f in order[: s + 1]), 0)
        for j, extra in enumerate(subsets(order[s + 1 :])):
            acc[h][base + extra] += ins[h][s][j].astype(F32)

    lag = 4
    returning = []
    for k in range(parts + lag + levels):
        if k < parts:
            front(k)
        if 1 <= k <= parts:
            join(k - 1)
            begin(k - 1, 0)
        if k == parts:
            for s in range(1, zero):
                project(right.at[s * count : (s + 1) * count], made.at[s - 1], 0)
                copy = pltpu.make_async_remote_copy(
                    src_ref=made.at[s - 1],
                    dst_ref=grads.at[:, pl.ds(base, owned)],
                    send_sem=leave.at[s],
                    recv_sem=enter.at[s],
                    device_id={"zero": before[s]},
                    device_id_type=MESH,
                )
                copy.start()
                returning.append(copy)
        for s in reversed(range(levels)):
            h = k - lag - s
            if 0 <= h < parts:
                finish(h, s)
                if s + 1 < levels:
                    begin(h, s + 1)
                else:
                    out[:, spans[h][0] : spans[h][1]] = acc[h][place]
    for copy in returning:
        copy.wait()


def tail(own, left, weights):
    pieces, piece, tokens = left.shape[1:]
    count, cols = own.shape
    zero = tokens // count
    parts = max(2, cols // 256)
    levels = pieces.bit_length() - 1
    edges = [i * cols // parts // 128 * 128 for i in range(parts)] + [cols]
    spans = list(zip(edges[:-1], edges[1:]))
    widths = [high - low for low, high in spans]
    scratch = [pltpu.VMEM((tokens, cols), BF)]
    scratch += [pltpu.VMEM((pieces, piece, w), F32) for w in widths]
    scratch += [pltpu.VMEM((pieces, piece, w), BF) for w in widths] * 2
    for _ in range(2):
        for w in widths:
            scratch += [pltpu.VMEM((pieces >> (s + 1), piece, w), BF) for s in range(levels)]
    owned = weights.shape[0]
    scratch += [pltpu.VMEM((zero - 1, count, owned), BF)]
    scratch += [pltpu.SemaphoreType.DMA((parts, levels + 1))] * 2
    scratch += [pltpu.SemaphoreType.DMA((parts, zero))] * 2
    scratch += [pltpu.SemaphoreType.DMA((zero,))] * 2
    return pl.pallas_call(
        functools.partial(tail_kernel, spans, min(256, owned)),
        out_shape=(
            jax.ShapeDtypeStruct((piece, cols), F32),
            jax.ShapeDtypeStruct((count, zero * owned), BF),
        ),
        in_specs=[pl.BlockSpec(memory_space=pltpu.VMEM)] * 3,
        out_specs=[pl.BlockSpec(memory_space=pltpu.VMEM)] * 2,
        scratch_shapes=scratch,
        compiler_params=pltpu.CompilerParams(collective_id=1, has_side_effects=True),
    )(own, left, weights)


def ssd_block(proj, gy, a_log, dt_bias, d_skip):
    count, inner = gy.shape
    heads = a_log.shape[0]
    width = inner // heads
    size = (proj.shape[1] - inner - heads) // 2
    xs = proj[:, :inner].astype(BF)
    bm = proj[:, inner : inner + size].astype(BF)
    cm = proj[:, inner + size : inner + 2 * size].astype(BF)
    raw = proj[:, inner + 2 * size :] + dt_bias
    dt = jax.nn.softplus(raw)
    rate = -jnp.exp(a_log)
    lower = jnp.arange(count)[:, None] >= jnp.arange(count)[None, :]
    cum = jnp.dot(lower.astype(F32), rate * dt, precision=lax.Precision.HIGHEST)
    total = cum[-1]
    growth = jnp.exp(cum)
    fade = jnp.exp(total - cum)
    x3 = xs.reshape(count, heads, width).astype(F32)
    g3 = gy.reshape(count, heads, width).astype(F32)
    xd = (x3 * dt[:, :, None]).astype(BF)
    grown = (g3 * growth[:, :, None]).astype(BF).reshape(count, inner)
    faded = (xd.astype(F32) * fade[:, :, None]).astype(BF).reshape(count, inner)
    local_f = dot(faded, bm, ((0,), (0,)))
    local_g = dot(grown, cm, ((0,), (0,)))
    shape = (heads, width, size)
    pair = jnp.stack([local_f.reshape(shape), local_g.reshape(shape)], axis=1).astype(BF)

    seq = lax.axis_size("seq")
    share = heads // seq
    marks = jnp.pad(total.reshape(seq, share), ((0, 0), (0, -share % 8)))
    marks = jnp.broadcast_to(marks[:, :, None], marks.shape + (size,))
    marks = marks.reshape(seq // 2, 2, -1, size)
    start, end = scan_states(pair.reshape(seq // 2, 2, share, 2, width, size), marks)
    start, end = start.reshape(inner, size), end.reshape(inner, size)

    spans = cum.T[:, :, None] - cum.T[:, None, :]
    decay = jnp.where(lower[None], jnp.exp(jnp.where(lower[None], spans, 0.0)), 0.0)
    scores = dot(cm, bm, ((1,), (1,)))
    mixing = (scores[None] * decay).astype(BF)
    gb3 = gy.reshape(count, heads, width)
    y_in = bdot(mixing, xd, "hts,shp->thp")
    back_in = bdot(mixing, gb3, "hts,thp->shp")
    cross = bdot(gb3, xd, "thp,shp->hts")
    mixed = jnp.sum(cross * decay, axis=0).astype(BF)

    y3 = y_in + dot(cm, start, ((1,), (1,))).reshape(x3.shape) * growth[:, :, None]
    h3 = back_in + dot(bm, end, ((1,), (1,))).reshape(x3.shape) * fade[:, :, None]
    out = y3 + d_skip[:, None] * x3
    grad_x = h3 * dt[:, :, None] + d_skip[:, None] * g3
    grad_c = dot(mixed, bm, ((1,), (0,))) + dot(grown, start, ((1,), (0,)))
    grad_b = dot(mixed, cm, ((0,), (0,))) + dot(faded, end, ((1,), (0,)))
    row = jnp.sum(g3 * y3, axis=2)
    column = jnp.sum(xd.astype(F32) * h3, axis=2)
    grad_dt = jnp.sum(x3 * h3, axis=2)
    joint = jnp.sum((start.astype(F32) * end.astype(F32)).reshape(heads, -1), axis=1)
    tail = jnp.sum(
        xd.astype(F32) * dot(bm, end, ((1,), (1,))).reshape(x3.shape) * fade[:, :, None], axis=(0, 2)
    )
    last = tail + jnp.exp(total) * joint
    grad_log = jnp.dot(
        lower.astype(F32).T, row - column, precision=lax.Precision.HIGHEST
    ) + last
    grad_raw = (grad_dt + grad_log * rate) * jax.nn.sigmoid(raw)
    gproj = jnp.concatenate(
        [grad_x.reshape(count, inner), grad_b, grad_c, grad_raw], axis=1
    ).astype(BF)
    return out.reshape(count, inner).astype(BF), gproj


def per_device(tokens, w_in, a_log, dt_bias, d_skip, grad_y):
    count, width = tokens.shape[1:]
    inner = grad_y.shape[2]
    heads = a_log.shape[0]
    columns = w_in.shape[1]
    exact = columns - heads
    zero = lax.axis_size("zero")
    seq = lax.axis_size("seq")
    here = lax.axis_index("zero")
    owned = width // zero
    rows = tokens.reshape(count, width)

    def columns_of(z):
        return lax.dynamic_slice_in_dim(rows, z * owned, owned, axis=1)

    guests = [shift(columns_of((here + s) % zero), "zero", s) for s in range(1, zero)]
    proj = jnp.dot(columns_of(here), w_in, preferred_element_type=F32)
    for s, guest in zip(range(1, zero), guests):
        part = jnp.dot(guest, w_in, preferred_element_type=F32)
        wide = shift(part[:, :exact].astype(BF), "zero", zero - s)
        narrow = shift(part[:, exact:], "zero", zero - s)
        proj = proj + jnp.concatenate([wide.astype(F32), narrow], axis=1)

    piece = width // (seq * zero)
    cut = rows.reshape(count, seq, zero, piece)

    def pieces_of(z):
        return lax.dynamic_index_in_dim(cut, z, 2, keepdims=False).reshape(count, seq * piece)

    theirs = [shift(pieces_of((here + s) % zero), "zero", s) for s in range(1, zero)]

    y_out, gproj = ssd_block(proj, grad_y.reshape(count, inner), a_log, dt_bias, d_skip)

    left = jnp.concatenate([pieces_of(here)] + theirs, axis=0)
    left = left.reshape(left.shape[0], seq // 2, 2, piece).transpose(2, 1, 3, 0)
    grad_w, grad_tokens = tail(gproj, left, w_in)
    grad_tokens = grad_tokens.reshape(1, count, width)
    return (y_out.reshape(1, count, inner), grad_tokens, grad_w)


def solution(mesh):
    placed = (P("zero", "seq", None), P("zero", None), P(), P(), P(), P("zero", "seq", None))
    return jax.shard_map(
        per_device,
        mesh=mesh,
        in_specs=placed,
        out_specs=(P("zero", "seq", None), P("zero", "seq", None), P(("seq", "zero"), None)),
        check_vma=False,
    )
```

```python
import functools

import jax
import jax.numpy as jnp
from jax import lax
from jax.experimental import pallas as pl
from jax.experimental.pallas import tpu as pltpu
from jax.sharding import PartitionSpec as P

BF = jnp.bfloat16
F32 = jnp.float32
MESH = pl.DeviceIdType.MESH


def shift(value, axis, step):
    count = lax.axis_size(axis)
    return lax.ppermute(value, axis, [(i, (i + step) % count) for i in range(count)])


def dot(a, b, dims):
    return lax.dot_general(a, b, (dims, ((), ())), preferred_element_type=F32)


def bdot(a, b, spec):
    return jnp.einsum(spec, a, b, preferred_element_type=F32)


def greet(peers, mates=()):
    barrier = pltpu.get_barrier_semaphore()
    for peer in peers:
        pl.semaphore_signal(barrier, inc=1, device_id={"seq": peer}, device_id_type=MESH)
    for mate in mates:
        pl.semaphore_signal(barrier, inc=1, device_id={"zero": mate}, device_id_type=MESH)
    pl.semaphore_wait(barrier, len(peers) + len(mates))


def remote(src, dst, send, recv, peer):
    return pltpu.make_async_remote_copy(
        src_ref=src,
        dst_ref=dst,
        send_sem=send,
        recv_sem=recv,
        device_id={"seq": peer},
        device_id_type=MESH,
    )


def scan_kernel(
    pair, totals, start, end, both, marks, joined, sums, got, lengths, made, back, final, wide,
    send, recv, local
):
    chips, _, share = pair.shape[:3]
    me = lax.axis_index("seq")
    core, chip = lax.rem(me, 2), lax.div(me, 2)
    sibling = me + 1 - 2 * core
    places = [lax.rem(chip + d, chips) for d in range(1, chips)]
    peers = [place * 2 + core for place in places]
    greet([sibling] + peers)

    def move(copies):
        for copy in copies:
            copy.start()
        for copy in copies:
            copy.wait()

    move(
        [
            remote(pair.at[:, 1 - core], both.at[core], send.at[0, 0], recv.at[0, 0], sibling),
            remote(totals.at[:, 1 - core], marks.at[core], send.at[1, 0], recv.at[1, 0], sibling),
            pltpu.make_async_copy(pair.at[:, core], both.at[core], local.at[0]),
            pltpu.make_async_copy(totals.at[:, core], marks.at[core], local.at[1]),
        ]
    )

    def gain(ref, *at):
        return jnp.exp(ref[at])

    for k in range(chips):
        sums[k] = marks[0, k] + marks[1, k]
        for j in range(share):
            row = pl.ds(j, 1)
            joined[k, j, 0] = (
                gain(marks, 1, k, row) * both[0, k, j, 0].astype(F32)
                + both[1, k, j, 0].astype(F32)
            ).astype(BF)
            joined[k, j, 1] = (
                gain(marks, 0, k, row) * both[1, k, j, 1].astype(F32)
                + both[0, k, j, 1].astype(F32)
            ).astype(BF)
    copies = []
    for d, (place, peer) in enumerate(zip(places, peers)):
        copies.append(remote(joined.at[place], got.at[chip], send.at[2, d], recv.at[2, d], peer))
        copies.append(remote(sums.at[place], lengths.at[chip], send.at[3, d], recv.at[3, d], peer))
    copies.append(pltpu.make_async_copy(joined.at[chip], got.at[chip], local.at[2]))
    copies.append(pltpu.make_async_copy(sums.at[chip], lengths.at[chip], local.at[3]))
    move(copies)

    for j in range(share):
        row = pl.ds(j, 1)
        run = jnp.zeros(pair.shape[4:], F32)
        for k in range(chips):
            made[k, j, 0] = run.astype(BF)
            if k < chips - 1:
                run = gain(lengths, k, row) * run + got[k, j, 0].astype(F32)
        run = jnp.zeros(pair.shape[4:], F32)
        for k in reversed(range(chips)):
            made[k, j, 1] = run.astype(BF)
            if k > 0:
                run = gain(lengths, k, row) * run + got[k, j, 1].astype(F32)
    copies = [
        remote(made.at[place], back.at[chip], send.at[4, d], recv.at[4, d], peer)
        for d, (place, peer) in enumerate(zip(places, peers))
    ]
    move(copies + [pltpu.make_async_copy(made.at[chip], back.at[chip], local.at[4])])

    for k in range(chips):
        for j in range(share):
            row = pl.ds(j, 1)
            first, last = back[k, j, 0], back[k, j, 1]
            final[0, k, j, 0] = first
            final[1, k, j, 1] = last
            final[1, k, j, 0] = (
                gain(marks, 0, k, row) * first.astype(F32) + both[0, k, j, 0].astype(F32)
            ).astype(BF)
            final[0, k, j, 1] = (
                gain(marks, 1, k, row) * last.astype(F32) + both[1, k, j, 1].astype(F32)
            ).astype(BF)
    move(
        [
            remote(final.at[1 - core], wide.at[core], send.at[5, 0], recv.at[5, 0], sibling),
            pltpu.make_async_copy(final.at[core], wide.at[core], local.at[5]),
        ]
    )
    for parity in range(2):
        start[:, parity] = wide[parity, :, :, 0]
        end[:, parity] = wide[parity, :, :, 1]


def scan_states(pair, totals):
    chips, _, share, _, rows, lanes = pair.shape
    state = jax.ShapeDtypeStruct((chips, 2, share, rows, lanes), BF)
    half = (chips,) + pair.shape[2:]
    short = (chips,) + totals.shape[2:]
    return pl.pallas_call(
        scan_kernel,
        out_shape=(state, state),
        in_specs=[pl.BlockSpec(memory_space=pltpu.VMEM)] * 2,
        out_specs=[pl.BlockSpec(memory_space=pltpu.VMEM)] * 2,
        scratch_shapes=[
            pltpu.VMEM((2,) + half, BF),
            pltpu.VMEM((2,) + short, F32),
            pltpu.VMEM(half, BF),
            pltpu.VMEM(short, F32),
            pltpu.VMEM(half, BF),
            pltpu.VMEM(short, F32),
            pltpu.VMEM(half, BF),
            pltpu.VMEM(half, BF),
            pltpu.VMEM((2,) + half, BF),
            pltpu.VMEM((2,) + half, BF),
            pltpu.SemaphoreType.DMA((6, chips)),
            pltpu.SemaphoreType.DMA((6, chips)),
            pltpu.SemaphoreType.DMA((6,)),
        ],
        compiler_params=pltpu.CompilerParams(collective_id=0, has_side_effects=True),
    )(pair, totals)


def tail_kernel(spans, tile, own, left, weights, out, grads, right, *scratch):
    seq, zero = 2 * left.shape[1], left.shape[3] // own.shape[0]
    levels = (seq // 2).bit_length() - 1
    me, here = lax.axis_index("seq"), lax.axis_index("zero")
    core, place = lax.rem(me, 2), lax.div(me, 2)
    bits = [lax.rem(lax.div(place, 1 << b), 2) for b in range(levels)]
    sibling = me + 1 - 2 * core
    partners = [me + (1 - 2 * bits[b]) * (2 << b) for b in range(levels)]
    after = [lax.rem(here + s, zero) for s in range(zero)]
    before = [lax.rem(here + zero - s, zero) for s in range(zero)]
    greet([sibling] + partners, after[1:])
    pieces, piece, tokens = left.shape[1:]
    count = own.shape[0]
    parts = len(spans)
    up = list(range(levels))
    orders = [up[1:] + up[:1]] + [up] * (parts - 1)
    acc, away, come = (scratch[i * parts : (i + 1) * parts] for i in range(3))
    rest = scratch[3 * parts : -7]
    outs = [rest[h * levels : (h + 1) * levels] for h in range(parts)]
    ins = [rest[(parts + h) * levels : (parts + h + 1) * levels] for h in range(parts)]
    made, send, recv, put, got, leave, enter = scratch[-7:]

    arriving = []
    for h, (low, high) in enumerate(spans):
        arriving.append([])
        for s in range(1, zero):
            copy = pltpu.make_async_remote_copy(
                src_ref=own.at[:, low:high],
                dst_ref=right.at[s * count : (s + 1) * count, low:high],
                send_sem=put.at[h, s],
                recv_sem=got.at[h, s],
                device_id={"zero": after[s]},
                device_id_type=MESH,
            )
            copy.start()
            arriving[h].append(copy)
    right[:count] = own[...]

    owned, columns = weights.shape
    base = pl.multiple_of(here * owned, 128)

    def project(rows, target, first):
        @pl.loop(0, owned // tile)
        def _(i):
            at = pl.multiple_of(i * tile, 128)
            value = dot(rows[:, :columns], weights[pl.ds(at, tile)], ((1,), (1,)))
            target[:, pl.ds(pl.multiple_of(first + at, 128), tile)] = value.astype(BF)

    project(own, grads, base)

    def multiply(side, h, target):
        low, high = spans[h]
        rows = left[side].reshape(pieces * piece, tokens)
        value = jnp.dot(rows, right[:, low:high], preferred_element_type=F32)
        target[...] = value.reshape(target.shape).astype(target.dtype)

    first = []

    def front(h):
        for copy in arriving[h]:
            copy.wait()
        multiply(1 - core, h, away[h])
        copy = remote(away[h], come[h], send.at[h, levels], recv.at[h, levels], sibling)
        copy.start()
        first.append(copy)
        multiply(core, h, acc[h])

    def join(h):
        first[h].wait()

        @pl.loop(0, pieces)
        def _(i):
            acc[h][i] += come[h][i].astype(F32)

    def subsets(rest):
        found = [0]
        for b in rest:
            found = found + [value + (1 << b) for value in found]
        return found

    flying = {}

    def begin(h, s):
        order = orders[h]
        b = order[s]
        base = sum((bits[f] * (1 << f) for f in order[:s]), 0)
        for j, extra in enumerate(subsets(order[s + 1 :])):
            outs[h][s][j] = acc[h][base + (1 - bits[b]) * (1 << b) + extra].astype(BF)
        copy = remote(outs[h][s], ins[h][s], send.at[h, s], recv.at[h, s], partners[b])
        copy.start()
        flying[h] = copy

    def finish(h, s):
        flying[h].wait()
        order = orders[h]
        base = sum((bits[f] * (1 << f) for f in order[: s + 1]), 0)
        for j, extra in enumerate(subsets(order[s + 1 :])):
            acc[h][base + extra] += ins[h][s][j].astype(F32)

    lag, skew = 4, 2
    returning = []
    for k in range(parts + lag + skew * levels):
        if k < parts:
            front(k)
        if 1 <= k <= parts:
            join(k - 1)
            begin(k - 1, 0)
        if k == parts:
            for s in range(1, zero):
                project(right.at[s * count : (s + 1) * count], made.at[s - 1], 0)
                copy = pltpu.make_async_remote_copy(
                    src_ref=made.at[s - 1],
                    dst_ref=grads.at[:, pl.ds(base, owned)],
                    send_sem=leave.at[s],
                    recv_sem=enter.at[s],
                    device_id={"zero": before[s]},
                    device_id_type=MESH,
                )
                copy.start()
                returning.append(copy)
        for s in reversed(range(levels)):
            h = k - lag - skew * s
            if 0 <= h < parts:
                finish(h, s)
                if s + 1 < levels:
                    begin(h, s + 1)
                else:
                    low, high = spans[h][0], min(spans[h][1], columns)
                    out[:, low:high] = acc[h][place, :, : high - low]
    for copy in returning:
        copy.wait()


def tail(own, left, weights):
    pieces, piece, tokens = left.shape[1:]
    count, cols = own.shape
    zero = tokens // count
    levels = pieces.bit_length() - 1
    edges = list(range(0, cols, 256)) + [cols]
    spans = list(zip(edges[:-1], edges[1:]))
    parts = len(spans)
    widths = [high - low for low, high in spans]
    scratch = [pltpu.VMEM((tokens, cols), BF)]
    scratch += [pltpu.VMEM((pieces, piece, w), F32) for w in widths]
    scratch += [pltpu.VMEM((pieces, piece, w), BF) for w in widths] * 2
    for _ in range(2):
        for w in widths:
            scratch += [pltpu.VMEM((pieces >> (s + 1), piece, w), BF) for s in range(levels)]
    owned, columns = weights.shape
    scratch += [pltpu.VMEM((zero - 1, count, owned), BF)]
    scratch += [pltpu.SemaphoreType.DMA((parts, levels + 1))] * 2
    scratch += [pltpu.SemaphoreType.DMA((parts, zero))] * 2
    scratch += [pltpu.SemaphoreType.DMA((zero,))] * 2
    return pl.pallas_call(
        functools.partial(tail_kernel, spans, min(256, owned)),
        out_shape=(
            jax.ShapeDtypeStruct((piece, columns), F32),
            jax.ShapeDtypeStruct((count, zero * owned), BF),
        ),
        in_specs=[pl.BlockSpec(memory_space=pltpu.VMEM)] * 3,
        out_specs=[pl.BlockSpec(memory_space=pltpu.VMEM)] * 2,
        scratch_shapes=scratch,
        compiler_params=pltpu.CompilerParams(collective_id=1, has_side_effects=True),
    )(own, left, weights)


def ssd_block(proj, gy, a_log, dt_bias, d_skip):
    count, inner = gy.shape
    heads = a_log.shape[0]
    width = inner // heads
    size = (proj.shape[1] - inner - heads) // 2
    xs = proj[:, :inner].astype(BF)
    bm = proj[:, inner : inner + size].astype(BF)
    cm = proj[:, inner + size : inner + 2 * size].astype(BF)
    raw = proj[:, inner + 2 * size :] + dt_bias
    dt = jax.nn.softplus(raw)
    rate = -jnp.exp(a_log)
    lower = jnp.arange(count)[:, None] >= jnp.arange(count)[None, :]
    cum = jnp.dot(lower.astype(F32), rate * dt, precision=lax.Precision.HIGHEST)
    total = cum[-1]
    growth = jnp.exp(cum)
    fade = jnp.exp(total - cum)
    x3 = xs.reshape(count, heads, width).astype(F32)
    g3 = gy.reshape(count, heads, width).astype(F32)
    xd = (x3 * dt[:, :, None]).astype(BF)
    grown = (g3 * growth[:, :, None]).astype(BF).reshape(count, inner)
    faded = (xd.astype(F32) * fade[:, :, None]).astype(BF).reshape(count, inner)
    local_f = dot(faded, bm, ((0,), (0,)))
    local_g = dot(grown, cm, ((0,), (0,)))
    shape = (heads, width, size)
    pair = jnp.stack([local_f.reshape(shape), local_g.reshape(shape)], axis=1).astype(BF)

    seq = lax.axis_size("seq")
    share = heads // seq
    marks = jnp.pad(total.reshape(seq, share), ((0, 0), (0, -share % 8)))
    marks = jnp.broadcast_to(marks[:, :, None], marks.shape + (size,))
    marks = marks.reshape(seq // 2, 2, -1, size)
    start, end = scan_states(pair.reshape(seq // 2, 2, share, 2, width, size), marks)
    start, end = start.reshape(inner, size), end.reshape(inner, size)

    spans = cum.T[:, :, None] - cum.T[:, None, :]
    decay = jnp.where(lower[None], jnp.exp(jnp.where(lower[None], spans, 0.0)), 0.0)
    scores = dot(cm, bm, ((1,), (1,)))
    mixing = (scores[None] * decay).astype(BF)
    gb3 = gy.reshape(count, heads, width)
    y_in = bdot(mixing, xd, "hts,shp->thp")
    back_in = bdot(mixing, gb3, "hts,thp->shp")
    cross = bdot(gb3, xd, "thp,shp->hts")
    mixed = jnp.sum(cross * decay, axis=0).astype(BF)

    y3 = y_in + dot(cm, start, ((1,), (1,))).reshape(x3.shape) * growth[:, :, None]
    h3 = back_in + dot(bm, end, ((1,), (1,))).reshape(x3.shape) * fade[:, :, None]
    out = y3 + d_skip[:, None] * x3
    grad_x = h3 * dt[:, :, None] + d_skip[:, None] * g3
    grad_c = dot(mixed, bm, ((1,), (0,))) + dot(grown, start, ((1,), (0,)))
    grad_b = dot(mixed, cm, ((0,), (0,))) + dot(faded, end, ((1,), (0,)))
    row = jnp.sum(g3 * y3, axis=2)
    column = jnp.sum(xd.astype(F32) * h3, axis=2)
    grad_dt = jnp.sum(x3 * h3, axis=2)
    joint = jnp.sum((start.astype(F32) * end.astype(F32)).reshape(heads, -1), axis=1)
    tail = jnp.sum(
        xd.astype(F32) * dot(bm, end, ((1,), (1,))).reshape(x3.shape) * fade[:, :, None], axis=(0, 2)
    )
    last = tail + jnp.exp(total) * joint
    grad_log = jnp.dot(
        lower.astype(F32).T, row - column, precision=lax.Precision.HIGHEST
    ) + last
    grad_raw = (grad_dt + grad_log * rate) * jax.nn.sigmoid(raw)
    gproj = jnp.concatenate(
        [
            grad_x.reshape(count, inner),
            grad_b,
            grad_c,
            grad_raw,
            jnp.zeros((count, -proj.shape[1] % 128), F32),
        ],
        axis=1,
    ).astype(BF)
    return out.reshape(count, inner).astype(BF), gproj


def per_device(tokens, w_in, a_log, dt_bias, d_skip, grad_y):
    count, width = tokens.shape[1:]
    inner = grad_y.shape[2]
    heads = a_log.shape[0]
    columns = w_in.shape[1]
    exact = columns - heads
    zero = lax.axis_size("zero")
    seq = lax.axis_size("seq")
    here = lax.axis_index("zero")
    owned = width // zero
    rows = tokens.reshape(count, width)

    def columns_of(z):
        return lax.dynamic_slice_in_dim(rows, z * owned, owned, axis=1)

    guests = [shift(columns_of((here + s) % zero), "zero", s) for s in range(1, zero)]
    proj = jnp.dot(columns_of(here), w_in, preferred_element_type=F32)
    for s, guest in zip(range(1, zero), guests):
        part = jnp.dot(guest, w_in, preferred_element_type=F32)
        wide = shift(part[:, :exact].astype(BF), "zero", zero - s)
        narrow = shift(part[:, exact:], "zero", zero - s)
        proj = proj + jnp.concatenate([wide.astype(F32), narrow], axis=1)

    piece = width // (seq * zero)
    cut = rows.reshape(count, seq, zero, piece)

    def pieces_of(z):
        return lax.dynamic_index_in_dim(cut, z, 2, keepdims=False).reshape(count, seq * piece)

    theirs = [shift(pieces_of((here + s) % zero), "zero", s) for s in range(1, zero)]

    y_out, gproj = ssd_block(proj, grad_y.reshape(count, inner), a_log, dt_bias, d_skip)

    left = jnp.concatenate([pieces_of(here)] + theirs, axis=0)
    left = left.reshape(left.shape[0], seq // 2, 2, piece).transpose(2, 1, 3, 0)
    grad_w, grad_tokens = tail(gproj, left, w_in)
    grad_tokens = grad_tokens.reshape(1, count, width)
    return (y_out.reshape(1, count, inner), grad_tokens, grad_w)


def solution(mesh):
    placed = (P("zero", "seq", None), P("zero", None), P(), P(), P(), P("zero", "seq", None))
    return jax.shard_map(
        per_device,
        mesh=mesh,
        in_specs=placed,
        out_specs=(P("zero", "seq", None), P("zero", "seq", None), P(("seq", "zero"), None)),
        check_vma=False,
    )
```

```python
import functools

import jax
import jax.numpy as jnp
from jax import lax
from jax.experimental import pallas as pl
from jax.experimental.pallas import tpu as pltpu
from jax.sharding import PartitionSpec as P

BF = jnp.bfloat16
F32 = jnp.float32
MESH = pl.DeviceIdType.MESH


def shift(value, axis, step):
    count = lax.axis_size(axis)
    return lax.ppermute(value, axis, [(i, (i + step) % count) for i in range(count)])


def dot(a, b, dims):
    return lax.dot_general(a, b, (dims, ((), ())), preferred_element_type=F32)


def bdot(a, b, spec):
    return jnp.einsum(spec, a, b, preferred_element_type=F32)


def greet(peers, mates=()):
    barrier = pltpu.get_barrier_semaphore()
    for peer in peers:
        pl.semaphore_signal(barrier, inc=1, device_id={"seq": peer}, device_id_type=MESH)
    for mate in mates:
        pl.semaphore_signal(barrier, inc=1, device_id={"zero": mate}, device_id_type=MESH)
    pl.semaphore_wait(barrier, len(peers) + len(mates))


def remote(src, dst, send, recv, peer):
    return pltpu.make_async_remote_copy(
        src_ref=src,
        dst_ref=dst,
        send_sem=send,
        recv_sem=recv,
        device_id={"seq": peer},
        device_id_type=MESH,
    )


def mate(src, dst, send, recv, peer):
    return pltpu.make_async_remote_copy(
        src_ref=src,
        dst_ref=dst,
        send_sem=send,
        recv_sem=recv,
        device_id={"zero": peer},
        device_id_type=MESH,
    )


def head_kernel(
    zero, inner, rows, stored, xs, pair, raw, weights, guest, kept, made, narrow, back, thin,
    send, recv, load
):
    here = lax.axis_index("zero")
    columns, owned = weights.shape
    exact = made.shape[2]
    heads = columns - exact
    after = [lax.rem(here + s, zero) for s in range(zero)]
    before = [lax.rem(here + zero - s, zero) for s in range(zero)]
    fetch = pltpu.make_async_copy(stored, weights, load)
    fetch.start()
    greet([], after[1:])

    def columns_of(z):
        return pl.ds(pl.multiple_of(z * owned, 128), owned)

    coming = []
    for s in range(1, zero):
        copy = mate(rows.at[:, columns_of(after[s])], guest.at[s - 1], send.at[s, 0], recv.at[s, 0], after[s])
        copy.start()
        coming.append(copy)
    edges = list(range(0, inner, 256)) + [inner]
    spans = [(inner, exact)] + list(zip(edges[:-1], edges[1:]))
    fetch.wait()
    mine = rows[:, columns_of(here)]
    for low, high in spans + [(exact, columns)]:
        kept[:, low:high] = dot(mine, weights[low:high], ((1,), (1,)))
    going = {}
    narrow[...] = jnp.zeros(narrow.shape, F32)
    for s in range(1, zero):
        coming[s - 1].wait()
        narrow[s - 1, :, :heads] = dot(guest[s - 1], weights[exact:], ((1,), (1,)))
        copy = mate(narrow.at[s - 1], thin.at[s - 1], send.at[s, 1], recv.at[s, 1], before[s])
        copy.start()
        going[s, -1] = copy
        for i, (low, high) in enumerate(spans):
            value = dot(guest[s - 1], weights[low:high], ((1,), (1,)))
            made[s - 1, :, low:high] = value.astype(BF)
            copy = mate(
                made.at[s - 1, :, low:high],
                back.at[s - 1, :, low:high],
                send.at[s, 2 + i],
                recv.at[s, 2 + i],
                before[s],
            )
            copy.start()
            going[s, i] = copy
    total = kept[:, exact:]
    for s in range(1, zero):
        going[s, -1].wait()
        total = total + thin[s - 1, :, :heads]
    raw[...] = total
    for i, (low, high) in enumerate(spans):
        total = kept[:, low:high]
        for s in range(1, zero):
            going[s, i].wait()
            total = total + back[s - 1, :, low:high].astype(F32)
        if i:
            xs[:, low:high] = total.astype(BF)
        else:
            pair[...] = total.astype(BF)


def head(rows, weights, inner, heads):
    count, width = rows.shape
    columns, owned = weights.shape
    zero = width // owned
    exact = columns - heads
    steps = 3 + -(-inner // 256)
    return pl.pallas_call(
        functools.partial(head_kernel, zero, inner),
        out_shape=(
            jax.ShapeDtypeStruct((count, inner), BF),
            jax.ShapeDtypeStruct((count, exact - inner), BF),
            jax.ShapeDtypeStruct((count, heads), F32),
        ),
        in_specs=[pl.BlockSpec(memory_space=pltpu.VMEM), pl.BlockSpec(memory_space=pl.ANY)],
        out_specs=[pl.BlockSpec(memory_space=pltpu.VMEM)] * 3,
        scratch_shapes=[
            pltpu.VMEM((columns, owned), BF),
            pltpu.VMEM((zero - 1, count, owned), BF),
            pltpu.VMEM((count, columns), F32),
            pltpu.VMEM((zero - 1, count, exact), BF),
            pltpu.VMEM((zero - 1, count, 128), F32),
            pltpu.VMEM((zero - 1, count, exact), BF),
            pltpu.VMEM((zero - 1, count, 128), F32),
            pltpu.SemaphoreType.DMA((zero, steps)),
            pltpu.SemaphoreType.DMA((zero, steps)),
            pltpu.SemaphoreType.DMA,
        ],
        compiler_params=pltpu.CompilerParams(collective_id=2, has_side_effects=True),
    )(rows, weights)


def scan_kernel(
    pair, totals, guests, start, end, held, both, marks, joined, sums, got, lengths, made, back, final, wide,
    send, recv, local, leave, enter
):
    chips, _, share = pair.shape[:3]
    me = lax.axis_index("seq")
    core, chip = lax.rem(me, 2), lax.div(me, 2)
    sibling = me + 1 - 2 * core
    places = [lax.rem(chip + d, chips) for d in range(1, chips)]
    peers = [place * 2 + core for place in places]
    here = lax.axis_index("zero")
    zero = guests.shape[0] + 1
    after = [lax.rem(here + s, zero) for s in range(zero)]
    greet([sibling] + peers, after[1:])
    crossing = [
        mate(guests.at[s - 1], held.at[s - 1], leave.at[s - 1], enter.at[s - 1], after[s])
        for s in range(1, zero)
    ]
    for copy in crossing:
        copy.start()

    def move(copies):
        for copy in copies:
            copy.start()
        for copy in copies:
            copy.wait()

    move(
        [
            remote(pair.at[:, 1 - core], both.at[core], send.at[0, 0], recv.at[0, 0], sibling),
            remote(totals.at[:, 1 - core], marks.at[core], send.at[1, 0], recv.at[1, 0], sibling),
            pltpu.make_async_copy(pair.at[:, core], both.at[core], local.at[0]),
            pltpu.make_async_copy(totals.at[:, core], marks.at[core], local.at[1]),
        ]
    )

    def gain(ref, *at):
        return jnp.exp(ref[at])

    for k in range(chips):
        sums[k] = marks[0, k] + marks[1, k]
        for j in range(share):
            row = pl.ds(j, 1)
            joined[k, j, 0] = (
                gain(marks, 1, k, row) * both[0, k, j, 0].astype(F32)
                + both[1, k, j, 0].astype(F32)
            ).astype(BF)
            joined[k, j, 1] = (
                gain(marks, 0, k, row) * both[1, k, j, 1].astype(F32)
                + both[0, k, j, 1].astype(F32)
            ).astype(BF)
    copies = []
    for d, (place, peer) in enumerate(zip(places, peers)):
        copies.append(remote(joined.at[place], got.at[chip], send.at[2, d], recv.at[2, d], peer))
        copies.append(remote(sums.at[place], lengths.at[chip], send.at[3, d], recv.at[3, d], peer))
    copies.append(pltpu.make_async_copy(joined.at[chip], got.at[chip], local.at[2]))
    copies.append(pltpu.make_async_copy(sums.at[chip], lengths.at[chip], local.at[3]))
    move(copies)

    for j in range(share):
        row = pl.ds(j, 1)
        run = jnp.zeros(pair.shape[4:], F32)
        for k in range(chips):
            made[k, j, 0] = run.astype(BF)
            if k < chips - 1:
                run = gain(lengths, k, row) * run + got[k, j, 0].astype(F32)
        run = jnp.zeros(pair.shape[4:], F32)
        for k in reversed(range(chips)):
            made[k, j, 1] = run.astype(BF)
            if k > 0:
                run = gain(lengths, k, row) * run + got[k, j, 1].astype(F32)
    copies = [
        remote(made.at[place], back.at[chip], send.at[4, d], recv.at[4, d], peer)
        for d, (place, peer) in enumerate(zip(places, peers))
    ]
    move(copies + [pltpu.make_async_copy(made.at[chip], back.at[chip], local.at[4])])

    for k in range(chips):
        for j in range(share):
            row = pl.ds(j, 1)
            first, last = back[k, j, 0], back[k, j, 1]
            final[0, k, j, 0] = first
            final[1, k, j, 1] = last
            final[1, k, j, 0] = (
                gain(marks, 0, k, row) * first.astype(F32) + both[0, k, j, 0].astype(F32)
            ).astype(BF)
            final[0, k, j, 1] = (
                gain(marks, 1, k, row) * last.astype(F32) + both[1, k, j, 1].astype(F32)
            ).astype(BF)
    move(
        [
            remote(final.at[1 - core], wide.at[core], send.at[5, 0], recv.at[5, 0], sibling),
            pltpu.make_async_copy(final.at[core], wide.at[core], local.at[5]),
        ]
    )
    for parity in range(2):
        start[:, parity] = wide[parity, :, :, 0]
        end[:, parity] = wide[parity, :, :, 1]
    for copy in crossing:
        copy.wait()


def scan_states(pair, totals, guests):
    chips, _, share, _, rows, lanes = pair.shape
    state = jax.ShapeDtypeStruct((chips, 2, share, rows, lanes), BF)
    half = (chips,) + pair.shape[2:]
    short = (chips,) + totals.shape[2:]
    return pl.pallas_call(
        scan_kernel,
        out_shape=(state, state, jax.ShapeDtypeStruct(guests.shape, BF)),
        in_specs=[pl.BlockSpec(memory_space=pltpu.VMEM)] * 3,
        out_specs=[pl.BlockSpec(memory_space=pltpu.VMEM)] * 3,
        scratch_shapes=[
            pltpu.VMEM((2,) + half, BF),
            pltpu.VMEM((2,) + short, F32),
            pltpu.VMEM(half, BF),
            pltpu.VMEM(short, F32),
            pltpu.VMEM(half, BF),
            pltpu.VMEM(short, F32),
            pltpu.VMEM(half, BF),
            pltpu.VMEM(half, BF),
            pltpu.VMEM((2,) + half, BF),
            pltpu.VMEM((2,) + half, BF),
            pltpu.SemaphoreType.DMA((6, chips)),
            pltpu.SemaphoreType.DMA((6, chips)),
            pltpu.SemaphoreType.DMA((6,)),
            pltpu.SemaphoreType.DMA(guests.shape[:1]),
            pltpu.SemaphoreType.DMA(guests.shape[:1]),
        ],
        compiler_params=pltpu.CompilerParams(collective_id=0, has_side_effects=True),
    )(pair, totals, guests)


def tail_kernel(spans, tile, own, left, stored, out, grads, right, weights, *scratch):
    seq, zero = 2 * left.shape[1], left.shape[3] // own.shape[0]
    levels = (seq // 2).bit_length() - 1
    me, here = lax.axis_index("seq"), lax.axis_index("zero")
    core, place = lax.rem(me, 2), lax.div(me, 2)
    bits = [lax.rem(lax.div(place, 1 << b), 2) for b in range(levels)]
    sibling = me + 1 - 2 * core
    partners = [me + (1 - 2 * bits[b]) * (2 << b) for b in range(levels)]
    after = [lax.rem(here + s, zero) for s in range(zero)]
    before = [lax.rem(here + zero - s, zero) for s in range(zero)]
    load = pltpu.make_async_copy(stored, weights, scratch[-1])
    load.start()
    scratch = scratch[:-1]
    greet([sibling] + partners, after[1:])
    pieces, piece, tokens = left.shape[1:]
    count = own.shape[0]
    parts = len(spans)
    up = list(range(levels))
    orders = [up[1:] + up[:1]] + [up] * (parts - 1)
    acc, away, come = (scratch[i * parts : (i + 1) * parts] for i in range(3))
    rest = scratch[3 * parts : -7]
    outs = [rest[h * levels : (h + 1) * levels] for h in range(parts)]
    ins = [rest[(parts + h) * levels : (parts + h + 1) * levels] for h in range(parts)]
    made, send, recv, put, got, leave, enter = scratch[-7:]

    arriving = []
    for h, (low, high) in enumerate(spans):
        arriving.append([])
        for s in range(1, zero):
            copy = pltpu.make_async_remote_copy(
                src_ref=own.at[:, low:high],
                dst_ref=right.at[s * count : (s + 1) * count, low:high],
                send_sem=put.at[h, s],
                recv_sem=got.at[h, s],
                device_id={"zero": after[s]},
                device_id_type=MESH,
            )
            copy.start()
            arriving[h].append(copy)
    right[:count] = own[...]

    columns, owned = weights.shape
    base = pl.multiple_of(here * owned, 128)

    def project(rows, target, first):
        @pl.loop(0, owned // tile)
        def _(i):
            at = pl.multiple_of(i * tile, 128)
            value = dot(rows[:, :columns], weights[:, pl.ds(at, tile)], ((1,), (0,)))
            target[:, pl.ds(pl.multiple_of(first + at, 128), tile)] = value.astype(BF)


    def multiply(side, h, target):
        low, high = spans[h]
        rows = left[side].reshape(pieces * piece, tokens)
        value = jnp.dot(rows, right[:, low:high], preferred_element_type=F32)
        target[...] = value.reshape(target.shape).astype(target.dtype)

    first = []

    def front(h):
        for copy in arriving[h]:
            copy.wait()
        multiply(1 - core, h, away[h])
        copy = remote(away[h], come[h], send.at[h, levels], recv.at[h, levels], sibling)
        copy.start()
        first.append(copy)
        multiply(core, h, acc[h])

    def join(h):
        first[h].wait()

        @pl.loop(0, pieces)
        def _(i):
            acc[h][i] += come[h][i].astype(F32)

    def subsets(rest):
        found = [0]
        for b in rest:
            found = found + [value + (1 << b) for value in found]
        return found

    flying = {}

    def begin(h, s):
        order = orders[h]
        b = order[s]
        base = sum((bits[f] * (1 << f) for f in order[:s]), 0)
        for j, extra in enumerate(subsets(order[s + 1 :])):
            outs[h][s][j] = acc[h][base + (1 - bits[b]) * (1 << b) + extra].astype(BF)
        copy = remote(outs[h][s], ins[h][s], send.at[h, s], recv.at[h, s], partners[b])
        copy.start()
        flying[h] = copy

    def finish(h, s):
        flying[h].wait()
        order = orders[h]
        base = sum((bits[f] * (1 << f) for f in order[: s + 1]), 0)
        for j, extra in enumerate(subsets(order[s + 1 :])):
            acc[h][base + extra] += ins[h][s][j].astype(F32)

    lag, skew = 4, 2
    returning = []
    for k in range(parts + lag + skew * levels):
        if k < parts:
            front(k)
        if 1 <= k <= parts:
            join(k - 1)
            begin(k - 1, 0)
        if k == parts:
            load.wait()
            for s in range(1, zero):
                project(right.at[s * count : (s + 1) * count], made.at[s - 1], 0)
                copy = pltpu.make_async_remote_copy(
                    src_ref=made.at[s - 1],
                    dst_ref=grads.at[:, pl.ds(base, owned)],
                    send_sem=leave.at[s],
                    recv_sem=enter.at[s],
                    device_id={"zero": before[s]},
                    device_id_type=MESH,
                )
                copy.start()
                returning.append(copy)
            project(own, grads, base)
        for s in reversed(range(levels)):
            h = k - lag - skew * s
            if 0 <= h < parts:
                finish(h, s)
                if s + 1 < levels:
                    begin(h, s + 1)
                else:
                    low, high = spans[h][0], min(spans[h][1], columns)
                    out[:, low:high] = acc[h][place, :, : high - low]
    for copy in returning:
        copy.wait()


def tail(own, left, weights):
    pieces, piece, tokens = left.shape[1:]
    count, cols = own.shape
    zero = tokens // count
    levels = pieces.bit_length() - 1
    edges = [0] + list(range(128, cols, 256)) + [cols]
    spans = list(zip(edges[:-1], edges[1:]))
    parts = len(spans)
    widths = [high - low for low, high in spans]
    scratch = [pltpu.VMEM((tokens, cols), BF), pltpu.VMEM(weights.shape, BF)]
    scratch += [pltpu.VMEM((pieces, piece, w), F32) for w in widths]
    scratch += [pltpu.VMEM((pieces, piece, w), BF) for w in widths] * 2
    for _ in range(2):
        for w in widths:
            scratch += [pltpu.VMEM((pieces >> (s + 1), piece, w), BF) for s in range(levels)]
    columns, owned = weights.shape
    scratch += [pltpu.VMEM((zero - 1, count, owned), BF)]
    scratch += [pltpu.SemaphoreType.DMA((parts, levels + 1))] * 2
    scratch += [pltpu.SemaphoreType.DMA((parts, zero))] * 2
    scratch += [pltpu.SemaphoreType.DMA((zero,))] * 2 + [pltpu.SemaphoreType.DMA]
    return pl.pallas_call(
        functools.partial(tail_kernel, spans, min(256, owned)),
        out_shape=(
            jax.ShapeDtypeStruct((piece, columns), F32),
            jax.ShapeDtypeStruct((count, zero * owned), BF),
        ),
        in_specs=[pl.BlockSpec(memory_space=pltpu.VMEM)] * 2
        + [pl.BlockSpec(memory_space=pl.ANY)],
        out_specs=[pl.BlockSpec(memory_space=pltpu.VMEM)] * 2,
        scratch_shapes=scratch,
        compiler_params=pltpu.CompilerParams(collective_id=1, has_side_effects=True),
    )(own, left, weights)


def ssd_block(xs, joined, raw, gy, guests, a_log, dt_bias, d_skip):
    count, inner = gy.shape
    heads = a_log.shape[0]
    width = inner // heads
    size = joined.shape[1] // 2
    bm, cm = joined[:, :size], joined[:, size:]
    raw = raw + dt_bias
    dt = jax.nn.softplus(raw)
    rate = -jnp.exp(a_log)
    lower = jnp.arange(count)[:, None] >= jnp.arange(count)[None, :]
    cum = jnp.dot(lower.astype(F32), rate * dt, precision=lax.Precision.HIGHEST)
    total = cum[-1]
    growth = jnp.exp(cum)
    fade = jnp.exp(total - cum)
    x3 = xs.reshape(count, heads, width).astype(F32)
    g3 = gy.reshape(count, heads, width).astype(F32)
    xd = (x3 * dt[:, :, None]).astype(BF)
    grown = (g3 * growth[:, :, None]).astype(BF).reshape(count, inner)
    faded = (xd.astype(F32) * fade[:, :, None]).astype(BF).reshape(count, inner)
    local_f = dot(faded, bm, ((0,), (0,)))
    local_g = dot(grown, cm, ((0,), (0,)))
    shape = (heads, width, size)
    pair = jnp.stack([local_f.reshape(shape), local_g.reshape(shape)], axis=1).astype(BF)

    seq = lax.axis_size("seq")
    share = heads // seq
    marks = jnp.pad(total.reshape(seq, share), ((0, 0), (0, -share % 8)))
    marks = jnp.broadcast_to(marks[:, :, None], marks.shape + (size,))
    marks = marks.reshape(seq // 2, 2, -1, size)
    start, end, held = scan_states(
        pair.reshape(seq // 2, 2, share, 2, width, size), marks, guests
    )
    start, end = start.reshape(inner, size), end.reshape(inner, size)

    spans = cum.T[:, :, None] - cum.T[:, None, :]
    decay = jnp.where(lower[None], jnp.exp(jnp.where(lower[None], spans, 0.0)), 0.0)
    scores = dot(cm, bm, ((1,), (1,)))
    mixing = (scores[None] * decay).astype(BF)
    gb3 = gy.reshape(count, heads, width)
    y_in = bdot(mixing, xd, "hts,shp->thp")
    back_in = bdot(mixing, gb3, "hts,thp->shp")
    cross = bdot(gb3, xd, "thp,shp->hts")
    mixed = jnp.sum(cross * decay, axis=0).astype(BF)

    y3 = y_in + dot(cm, start, ((1,), (1,))).reshape(x3.shape) * growth[:, :, None]
    h3 = back_in + dot(bm, end, ((1,), (1,))).reshape(x3.shape) * fade[:, :, None]
    out = y3 + d_skip[:, None] * x3
    grad_x = h3 * dt[:, :, None] + d_skip[:, None] * g3
    grad_c = dot(mixed, bm, ((1,), (0,))) + dot(grown, start, ((1,), (0,)))
    grad_b = dot(mixed, cm, ((0,), (0,))) + dot(faded, end, ((1,), (0,)))
    row = jnp.sum(g3 * y3, axis=2)
    column = jnp.sum(xd.astype(F32) * h3, axis=2)
    grad_dt = jnp.sum(x3 * h3, axis=2)
    joint = jnp.sum((start.astype(F32) * end.astype(F32)).reshape(heads, -1), axis=1)
    tail = jnp.sum(
        xd.astype(F32) * dot(bm, end, ((1,), (1,))).reshape(x3.shape) * fade[:, :, None], axis=(0, 2)
    )
    last = tail + jnp.exp(total) * joint
    grad_log = jnp.dot(
        lower.astype(F32).T, row - column, precision=lax.Precision.HIGHEST
    ) + last
    grad_raw = (grad_dt + grad_log * rate) * jax.nn.sigmoid(raw)
    gproj = jnp.concatenate(
        [
            grad_x.reshape(count, inner),
            grad_b,
            grad_c,
            grad_raw,
            jnp.zeros((count, -(inner + 2 * size + heads) % 128), F32),
        ],
        axis=1,
    ).astype(BF)
    return out.reshape(count, inner).astype(BF), gproj, held


def per_device(tokens, w_in, a_log, dt_bias, d_skip, grad_y):
    count, width = tokens.shape[1:]
    inner = grad_y.shape[2]
    heads = a_log.shape[0]
    zero = lax.axis_size("zero")
    seq = lax.axis_size("seq")
    here = lax.axis_index("zero")
    rows = tokens.reshape(count, width)

    stored = w_in.T
    xs, joined, raw = head(rows, stored, inner, heads)

    piece = width // (seq * zero)
    cut = rows.reshape(count, seq, zero, piece)

    def pieces_of(z):
        return lax.dynamic_index_in_dim(cut, z, 2, keepdims=False).reshape(count, seq * piece)

    guests = jnp.stack([pieces_of((here + s) % zero) for s in range(1, zero)])
    y_out, gproj, held = ssd_block(
        xs, joined, raw, grad_y.reshape(count, inner), guests, a_log, dt_bias, d_skip
    )

    left = jnp.concatenate([pieces_of(here)[None], held], axis=0)
    left = left.reshape(zero * count, seq * piece)
    left = left.reshape(left.shape[0], seq // 2, 2, piece).transpose(2, 1, 3, 0)
    grad_w, grad_tokens = tail(gproj, left, stored)
    grad_tokens = grad_tokens.reshape(1, count, width)
    return (y_out.reshape(1, count, inner), grad_tokens, grad_w)


def solution(mesh):
    placed = (P("zero", "seq", None), P("zero", None), P(), P(), P(), P("zero", "seq", None))
    return jax.shard_map(
        per_device,
        mesh=mesh,
        in_specs=placed,
        out_specs=(P("zero", "seq", None), P("zero", "seq", None), P(("seq", "zero"), None)),
        check_vma=False,
    )
```

```python
import functools

import jax
import jax.numpy as jnp
from jax import lax
from jax.experimental import pallas as pl
from jax.experimental.pallas import tpu as pltpu
from jax.sharding import PartitionSpec as P

BF = jnp.bfloat16
F32 = jnp.float32
MESH = pl.DeviceIdType.MESH
LAGS = (0, 1, 3, 5, 6)


def dot(a, b, dims):
    return lax.dot_general(a, b, (dims, ((), ())), preferred_element_type=F32)


def greet(peers, mates=()):
    barrier = pltpu.get_barrier_semaphore()
    for peer in peers:
        pl.semaphore_signal(barrier, inc=1, device_id={"seq": peer}, device_id_type=MESH)
    for mate in mates:
        pl.semaphore_signal(barrier, inc=1, device_id={"zero": mate}, device_id_type=MESH)
    pl.semaphore_wait(barrier, len(peers) + len(mates))


def remote(src, dst, send, recv, peer):
    return pltpu.make_async_remote_copy(
        src_ref=src,
        dst_ref=dst,
        send_sem=send,
        recv_sem=recv,
        device_id={"seq": peer},
        device_id_type=MESH,
    )


def mate(src, dst, send, recv, peer):
    return pltpu.make_async_remote_copy(
        src_ref=src,
        dst_ref=dst,
        send_sem=send,
        recv_sem=recv,
        device_id={"zero": peer},
        device_id_type=MESH,
    )


def head_kernel(
    zero, inner, rows, stored, xs, pair, raw, weights, guest, kept, made, narrow, back, thin,
    send, recv, load
):
    here = lax.axis_index("zero")
    columns, owned = weights.shape
    exact = made.shape[2]
    heads = columns - exact
    after = [lax.rem(here + s, zero) for s in range(zero)]
    before = [lax.rem(here + zero - s, zero) for s in range(zero)]
    fetch = pltpu.make_async_copy(stored, weights, load)
    fetch.start()
    greet([], after[1:])

    def columns_of(z):
        return pl.ds(pl.multiple_of(z * owned, 128), owned)

    coming = []
    for s in range(1, zero):
        copy = mate(rows.at[:, columns_of(after[s])], guest.at[s - 1], send.at[s, 0], recv.at[s, 0], after[s])
        copy.start()
        coming.append(copy)
    edges = list(range(0, inner, 256)) + [inner]
    spans = [(inner, exact)] + list(zip(edges[:-1], edges[1:]))
    fetch.wait()
    mine = rows[:, columns_of(here)]
    for low, high in spans + [(exact, columns)]:
        kept[:, low:high] = dot(mine, weights[low:high], ((1,), (1,)))
    going = {}
    narrow[...] = jnp.zeros(narrow.shape, F32)
    for s in range(1, zero):
        coming[s - 1].wait()
        narrow[s - 1, :, :heads] = dot(guest[s - 1], weights[exact:], ((1,), (1,)))
        copy = mate(narrow.at[s - 1], thin.at[s - 1], send.at[s, 1], recv.at[s, 1], before[s])
        copy.start()
        going[s, -1] = copy
        for i, (low, high) in enumerate(spans):
            value = dot(guest[s - 1], weights[low:high], ((1,), (1,)))
            made[s - 1, :, low:high] = value.astype(BF)
            copy = mate(
                made.at[s - 1, :, low:high],
                back.at[s - 1, :, low:high],
                send.at[s, 2 + i],
                recv.at[s, 2 + i],
                before[s],
            )
            copy.start()
            going[s, i] = copy
    total = kept[:, exact:]
    for s in range(1, zero):
        going[s, -1].wait()
        total = total + thin[s - 1, :, :heads]
    raw[...] = total
    for i, (low, high) in enumerate(spans):
        total = kept[:, low:high]
        for s in range(1, zero):
            going[s, i].wait()
            total = total + back[s - 1, :, low:high].astype(F32)
        if i:
            xs[:, low:high] = total.astype(BF)
        else:
            pair[...] = total.astype(BF)


def head(rows, weights, inner, heads):
    count, width = rows.shape
    columns, owned = weights.shape
    zero = width // owned
    exact = columns - heads
    steps = 3 + -(-inner // 256)
    return pl.pallas_call(
        functools.partial(head_kernel, zero, inner),
        out_shape=(
            jax.ShapeDtypeStruct((count, inner), BF),
            jax.ShapeDtypeStruct((count, exact - inner), BF),
            jax.ShapeDtypeStruct((count, heads), F32),
        ),
        in_specs=[pl.BlockSpec(memory_space=pltpu.VMEM), pl.BlockSpec(memory_space=pl.ANY)],
        out_specs=[pl.BlockSpec(memory_space=pltpu.VMEM)] * 3,
        scratch_shapes=[
            pltpu.VMEM((columns, owned), BF),
            pltpu.VMEM((zero - 1, count, owned), BF),
            pltpu.VMEM((count, columns), F32),
            pltpu.VMEM((zero - 1, count, exact), BF),
            pltpu.VMEM((zero - 1, count, 128), F32),
            pltpu.VMEM((zero - 1, count, exact), BF),
            pltpu.VMEM((zero - 1, count, 128), F32),
            pltpu.SemaphoreType.DMA((zero, steps)),
            pltpu.SemaphoreType.DMA((zero, steps)),
            pltpu.SemaphoreType.DMA,
        ],
        compiler_params=pltpu.CompilerParams(collective_id=2, has_side_effects=True),
    )(rows, weights)


def tail_kernel(spans, tile, own, mine, held, stored, out, grads, right, weights, left, *scratch):
    seq, zero = 2 * left.shape[1], left.shape[3] // own.shape[0]
    levels = (seq // 2).bit_length() - 1
    me, here = lax.axis_index("seq"), lax.axis_index("zero")
    core, place = lax.rem(me, 2), lax.div(me, 2)
    bits = [lax.rem(lax.div(place, 1 << b), 2) for b in range(levels)]
    sibling = me + 1 - 2 * core
    partners = [me + (1 - 2 * bits[b]) * (2 << b) for b in range(levels)]
    after = [lax.rem(here + s, zero) for s in range(zero)]
    before = [lax.rem(here + zero - s, zero) for s in range(zero)]
    load = pltpu.make_async_copy(stored, weights, scratch[-1])
    load.start()
    scratch = scratch[:-1]
    greet([sibling] + partners, after[1:])
    pieces, piece, tokens = left.shape[1:]
    count = own.shape[0]
    parts = len(spans)
    up = list(range(levels))
    orders = [up[1:] + up[:1]] + [up] * (parts - 1)
    acc, away, come = (scratch[i * parts : (i + 1) * parts] for i in range(3))
    rest = scratch[3 * parts : -7]
    outs = [rest[h * levels : (h + 1) * levels] for h in range(parts)]
    ins = [rest[(parts + h) * levels : (parts + h + 1) * levels] for h in range(parts)]
    made, send, recv, put, got, leave, enter = scratch[-7:]

    arriving = []
    for h, (low, high) in enumerate(spans):
        arriving.append([])
        for s in range(1, zero):
            copy = pltpu.make_async_remote_copy(
                src_ref=own.at[:, low:high],
                dst_ref=right.at[s * count : (s + 1) * count, low:high],
                send_sem=put.at[h, s],
                recv_sem=got.at[h, s],
                device_id={"zero": after[s]},
                device_id_type=MESH,
            )
            copy.start()
            arriving[h].append(copy)
    right[:count] = own[...]
    for way in range(2):
        for s in range(zero):
            turned = mine[way].T if s == 0 else held[s - 1, way].T
            left[way, :, :, s * count : (s + 1) * count] = turned.reshape(pieces, piece, count)

    columns, owned = weights.shape
    base = pl.multiple_of(here * owned, 128)

    def project(rows, target, first):
        @pl.loop(0, owned // tile)
        def _(i):
            at = pl.multiple_of(i * tile, 128)
            value = dot(rows[:, :columns], weights[:, pl.ds(at, tile)], ((1,), (0,)))
            target[:, pl.ds(pl.multiple_of(first + at, 128), tile)] = value.astype(BF)


    def multiply(side, h, target):
        low, high = spans[h]
        rows = left[side].reshape(pieces * piece, tokens)
        value = jnp.dot(rows, right[:, low:high], preferred_element_type=F32)
        target[...] = value.reshape(target.shape).astype(target.dtype)

    first = []

    def front(h):
        for copy in arriving[h]:
            copy.wait()
        multiply(1 - core, h, away[h])
        copy = remote(away[h], come[h], send.at[h, levels], recv.at[h, levels], sibling)
        copy.start()
        first.append(copy)
        multiply(core, h, acc[h])

    def join(h):
        first[h].wait()

        @pl.loop(0, pieces)
        def _(i):
            acc[h][i] += come[h][i].astype(F32)

    def subsets(rest):
        found = [0]
        for b in rest:
            found = found + [value + (1 << b) for value in found]
        return found

    flying = {}

    def begin(h, s):
        order = orders[h]
        b = order[s]
        base = sum((bits[f] * (1 << f) for f in order[:s]), 0)
        for j, extra in enumerate(subsets(order[s + 1 :])):
            outs[h][s][j] = acc[h][base + (1 - bits[b]) * (1 << b) + extra].astype(BF)
        copy = remote(outs[h][s], ins[h][s], send.at[h, s], recv.at[h, s], partners[b])
        copy.start()
        flying[h] = copy

    def finish(h, s):
        flying[h].wait()
        order = orders[h]
        base = sum((bits[f] * (1 << f) for f in order[: s + 1]), 0)
        for j, extra in enumerate(subsets(order[s + 1 :])):
            acc[h][base + extra] += ins[h][s][j].astype(F32)

    lag, skew = 4, 2
    returning = []
    for k in range(parts + lag + skew * levels):
        if k < parts:
            front(k)
        if 1 <= k <= parts:
            join(k - 1)
            begin(k - 1, 0)
        if k == parts:
            load.wait()
            for s in range(1, zero):
                project(right.at[s * count : (s + 1) * count], made.at[s - 1], 0)
                copy = pltpu.make_async_remote_copy(
                    src_ref=made.at[s - 1],
                    dst_ref=grads.at[:, pl.ds(base, owned)],
                    send_sem=leave.at[s],
                    recv_sem=enter.at[s],
                    device_id={"zero": before[s]},
                    device_id_type=MESH,
                )
                copy.start()
                returning.append(copy)
            project(own, grads, base)
        for s in reversed(range(levels)):
            h = k - lag - skew * s
            if 0 <= h < parts:
                finish(h, s)
                if s + 1 < levels:
                    begin(h, s + 1)
                else:
                    low, high = spans[h][0], min(spans[h][1], columns)
                    out[:, low:high] = acc[h][place, :, : high - low]
    for copy in returning:
        copy.wait()


def tail(own, mine, held, weights, pieces):
    count, cols = own.shape
    zero = held.shape[0] + 1
    piece, tokens = mine.shape[2] // pieces, zero * count
    levels = pieces.bit_length() - 1
    edges = [0] + list(range(128, cols, 256)) + [cols]
    spans = list(zip(edges[:-1], edges[1:]))
    parts = len(spans)
    widths = [high - low for low, high in spans]
    scratch = [pltpu.VMEM((tokens, cols), BF), pltpu.VMEM(weights.shape, BF)]
    scratch += [pltpu.VMEM((2, pieces, piece, tokens), BF)]
    scratch += [pltpu.VMEM((pieces, piece, w), F32) for w in widths]
    scratch += [pltpu.VMEM((pieces, piece, w), BF) for w in widths] * 2
    for _ in range(2):
        for w in widths:
            scratch += [pltpu.VMEM((pieces >> (s + 1), piece, w), BF) for s in range(levels)]
    columns, owned = weights.shape
    scratch += [pltpu.VMEM((zero - 1, count, owned), BF)]
    scratch += [pltpu.SemaphoreType.DMA((parts, levels + 1))] * 2
    scratch += [pltpu.SemaphoreType.DMA((parts, zero))] * 2
    scratch += [pltpu.SemaphoreType.DMA((zero,))] * 2 + [pltpu.SemaphoreType.DMA]
    return pl.pallas_call(
        functools.partial(tail_kernel, spans, min(256, owned)),
        out_shape=(
            jax.ShapeDtypeStruct((piece, columns), F32),
            jax.ShapeDtypeStruct((count, zero * owned), BF),
        ),
        in_specs=[pl.BlockSpec(memory_space=pltpu.VMEM)] * 3
        + [pl.BlockSpec(memory_space=pl.ANY)],
        out_specs=[pl.BlockSpec(memory_space=pltpu.VMEM)] * 2,
        scratch_shapes=scratch,
        compiler_params=pltpu.CompilerParams(collective_id=1, has_side_effects=True),
    )(own, mine, held, weights)


def core_kernel(
    width, chunk, lags, xs, joined, raws, gy, guests, scalars, y_out, gproj, held,
    spread, dts, grows, fades, xds, growns, fadeds, ins, backs, cums, turned, mark, marks, gains,
    loc, both, pairs, duo, sums, far, ret, came, fin, wide,
    tsend, trecv, send, recv, zsend, zrecv, leave, enter
):
    seq, planes = marks.shape[0], far.shape[2]
    zero = guests.shape[0] + 1
    me, here = lax.axis_index("seq"), lax.axis_index("zero")
    core, chip = lax.rem(me, 2), lax.div(me, 2)
    side, plane = lax.rem(chip, 2), lax.div(chip, 2)
    sibling, across = me + 1 - 2 * core, me + 2 - 4 * side
    peers = [lax.rem(me + d, seq) for d in range(1, seq)]
    after = [lax.rem(here + s, zero) for s in range(zero)]
    count, inner = xs.shape
    heads = raws.shape[1]
    size = joined.shape[1] // 2
    chunks = inner // chunk
    high = lax.Precision.HIGHEST
    far[...] = jnp.zeros(far.shape, BF)
    mark[...] = jnp.zeros(mark.shape, F32)
    greet(peers, after[1:])
    crossing = [
        mate(guests.at[s - 1], held.at[s - 1], leave.at[s - 1], enter.at[s - 1], after[s])
        for s in range(1, zero)
    ]
    for copy in crossing:
        copy.start()

    def iota(shape, axis):
        return lax.broadcasted_iota(jnp.int32, shape, axis)

    lower = iota((count, count), 0) >= iota((count, count), 1)
    ones = lower.astype(F32)
    first = iota((heads, inner), 0) * width
    lane = iota((heads, inner), 1)
    spread[...] = ((lane >= first) & (lane < first + width)).astype(F32)
    rate, skip = scalars[0:1, :heads], scalars[2:3, :heads]
    raw = raws[...] + scalars[1:2, :heads]
    dt = jnp.maximum(raw, 0.0) + jnp.log1p(jnp.exp(-jnp.abs(raw)))
    cum = jnp.dot(ones, rate * dt, precision=high, preferred_element_type=F32)
    total = cum[count - 1 : count]
    cums[...] = cum
    turned[...] = cum.T
    mark[0:1, :heads] = total
    marks[me] = mark[...]
    told = [
        remote(mark, marks.at[me], tsend.at[d], trecv.at[d], peer) for d, peer in enumerate(peers)
    ]
    for copy in told:
        copy.start()
    growth, fade = jnp.exp(cum), jnp.exp(total - cum)
    bm, cm = joined[:, :size], joined[:, size:]
    bt, ct = bm.T, cm.T
    skips = jnp.broadcast_to(skip, (8, heads))

    def expand(value, low, top):
        return jnp.dot(value, spread[:, low:top], precision=high, preferred_element_type=F32)

    def gather(value, low, top):
        return lax.dot_general(
            value, spread[:, low:top], (((1,), (1,)), ((), ())), precision=high,
            preferred_element_type=F32,
        )

    step = min(256, chunk)
    copies = {}

    def prepare(c):
        for low in range(c * chunk, (c + 1) * chunk, step):
            top = low + step
            own = slice(low - c * chunk, low - c * chunk + step)
            d, g, f = expand(dt, low, top), expand(growth, low, top), expand(fade, low, top)
            dts[:, low:top], grows[:, low:top], fades[:, low:top] = d, g, f
            xd = (xs[:, low:top].astype(F32) * d).astype(BF)
            grown = (gy[:, low:top].astype(F32) * g).astype(BF)
            faded = (xd.astype(F32) * f).astype(BF)
            xds[:, low:top], growns[:, low:top], fadeds[:, low:top] = xd, grown, faded
            parts = loc.shape[1:2] + loc.shape[3:5] + (step,)
            loc[c, :, 0, :, :, own] = dot(bt, faded, ((1,), (0,))).astype(BF).reshape(parts)
            loc[c, :, 1, :, :, own] = dot(ct, grown, ((1,), (0,))).astype(BF).reshape(parts)
        both[c, core] = loc[c, core]
        copies[0, c] = remote(
            loc.at[c, 1 - core], both.at[c, core], send.at[0, c], recv.at[0, c], sibling
        )
        copies[0, c].start()

    def gain(c, *rows):
        at = slice(c * chunk, (c + 1) * chunk)
        return jnp.exp(sum(gains[pl.ds(row, 1), at] for row in rows))

    def stage_pair(c):
        copies[0, c].wait()
        g0, g1 = gain(c, chip * 2), gain(c, chip * 2 + 1)
        for q in range(2):
            pairs[c, q, 0] = (
                g1 * both[c, 0, 0, q].astype(F32) + both[c, 1, 0, q].astype(F32)
            ).astype(BF)
            pairs[c, q, 1] = (
                g0 * both[c, 1, 1, q].astype(F32) + both[c, 0, 1, q].astype(F32)
            ).astype(BF)
        duo[c, side] = pairs[c, side]
        copies[1, c] = remote(
            pairs.at[c, 1 - side], duo.at[c, side], send.at[1, c], recv.at[1, c], across
        )
        copies[1, c].start()

    def along(c, way, d):
        return remote(
            sums.at[c, way],
            far.at[c, way, plane],
            zsend.at[c, way, d],
            zrecv.at[c, way, d],
            me + (4 * d if way == 0 else -4 * d),
        )

    def later(d, way):
        return plane + d < planes if way == 0 else plane >= d

    def stage_plane(c):
        copies[1, c].wait()
        g0 = gain(c, plane * 4, plane * 4 + 1)
        g1 = gain(c, plane * 4 + 2, plane * 4 + 3)
        sums[c, 0] = (g1 * duo[c, 0, 0].astype(F32) + duo[c, 1, 0].astype(F32)).astype(BF)
        sums[c, 1] = (g0 * duo[c, 1, 1].astype(F32) + duo[c, 0, 1].astype(F32)).astype(BF)
        for d in range(1, planes):
            for way in range(2):

                @pl.when(later(d, way))
                def _():
                    along(c, way, d).start()

    def stage_far(c):
        for d in range(1, planes):
            for way in range(2):

                @pl.when(later(d, 1 - way))
                def _():
                    along(c, way, d).wait_recv()

                @pl.when(later(d, way))
                def _():
                    along(c, way, d).wait_send()

        at = slice(c * chunk, (c + 1) * chunk)
        ends = []
        for way in range(2):
            run = jnp.zeros(far.shape[3:], F32)
            for k in range(planes) if way == 0 else reversed(range(planes)):
                inside = (k < plane if way == 0 else k > plane).astype(F32)
                whole = sum(gains[4 * k + i : 4 * k + i + 1, at] for i in range(4))
                run = jnp.exp(whole * inside) * run + far[c, way, k].astype(F32)
            ends.append(run)
        g0 = gain(c, plane * 4, plane * 4 + 1)
        g1 = gain(c, plane * 4 + 2, plane * 4 + 3)
        ret[c, 0, 0] = ends[0].astype(BF)
        ret[c, 1, 0] = (g0 * ends[0] + duo[c, 0, 0].astype(F32)).astype(BF)
        ret[c, 1, 1] = ends[1].astype(BF)
        ret[c, 0, 1] = (g1 * ends[1] + duo[c, 1, 1].astype(F32)).astype(BF)
        came[c, side] = ret[c, side]
        copies[2, c] = remote(
            ret.at[c, 1 - side], came.at[c, side], send.at[2, c], recv.at[2, c], across
        )
        copies[2, c].start()

    def stage_back(c):
        copies[2, c].wait()
        g0, g1 = gain(c, chip * 2), gain(c, chip * 2 + 1)
        for q in range(2):
            fin[c, 0, 0, q] = came[c, q, 0]
            fin[c, 1, 1, q] = came[c, q, 1]
            fin[c, 1, 0, q] = (
                g0 * came[c, q, 0].astype(F32) + both[c, 0, 0, q].astype(F32)
            ).astype(BF)
            fin[c, 0, 1, q] = (
                g1 * came[c, q, 1].astype(F32) + both[c, 1, 1, q].astype(F32)
            ).astype(BF)
        wide[c, core] = fin[c, core]
        copies[3, c] = remote(
            fin.at[c, 1 - core], wide.at[c, core], send.at[3, c], recv.at[3, c], sibling
        )
        copies[3, c].start()

    scores = dot(cm, bm, ((1,), (1,)))
    group = 128 // width
    state = {
        "mixed": jnp.zeros((count, count), F32),
        "c": jnp.zeros((count, size), F32),
        "b": jnp.zeros((count, size), F32),
        "log": jnp.zeros((count, heads), F32),
        "dt": jnp.zeros((count, heads), F32),
        "last": jnp.zeros((8, heads), F32),
    }
    place = iota((count, 128), 1)
    masks = [(place >= width * i) & (place < width * (i + 1)) for i in range(group)]

    def inside(p):
        low, top = p * 128, (p + 1) * 128
        x2, g2 = xds[:, low:top], gy[:, low:top]
        none = jnp.zeros_like(x2)
        decays = []
        for i in range(group):
            h = p * group + i
            spans = cums[:, h : h + 1] - turned[h : h + 1, :]
            decays.append(jnp.where(lower, jnp.exp(jnp.where(lower, spans, 0.0)), 0.0))
        mixing = jnp.concatenate([(scores * decay).astype(BF) for decay in decays], axis=1)
        stacked = jnp.concatenate([jnp.where(mask, x2, none) for mask in masks], axis=0)
        ins[:, low:top] = dot(mixing, stacked, ((1,), (0,)))
        tall = dot(mixing, g2, ((0,), (0,)))
        back = tall[:count]
        for i in range(1, group):
            back = jnp.where(masks[i], tall[i * count : (i + 1) * count], back)
        backs[:, low:top] = back
        lifted = jnp.concatenate([jnp.where(mask, g2, none) for mask in masks], axis=0)
        cross = dot(lifted, x2, ((1,), (1,)))
        for i in range(group):
            state["mixed"] += cross[i * count : (i + 1) * count] * decays[i]

    def finish(c):
        copies[3, c].wait()
        for low in range(c * chunk, (c + 1) * chunk, step):
            top = low + step
            own = slice(low - c * chunk, low - c * chunk + step)
            start = wide[c, :, 0, :, :, own].reshape(size, step)
            end = wide[c, :, 1, :, :, own].reshape(size, step)
            x, g = xs[:, low:top].astype(F32), gy[:, low:top].astype(F32)
            d, xd = dts[:, low:top], xds[:, low:top].astype(F32)
            reached = dot(bm, end, ((1,), (0,))) * fades[:, low:top]
            y3 = ins[:, low:top] + dot(cm, start, ((1,), (0,))) * grows[:, low:top]
            h3 = backs[:, low:top] + reached
            kept = expand(skips, low, top)[:1]
            y_out[:, low:top] = (y3 + kept * x).astype(BF)
            gproj[:, low:top] = (h3 * d + kept * g).astype(BF)
            state["c"] += dot(growns[:, low:top], start, ((1,), (1,)))
            state["b"] += dot(fadeds[:, low:top], end, ((1,), (1,)))
            state["log"] += gather(g * y3 - xd * h3, low, top)
            state["dt"] += gather(x * h3, low, top)
            joint = jnp.sum(start.astype(F32) * end.astype(F32), axis=0, keepdims=True)
            joint = joint * jnp.exp(gains[pl.ds(me, 1), low:top])
            last = jnp.sum(xd * reached, axis=0, keepdims=True) + joint
            state["last"] += gather(jnp.broadcast_to(last, (8, step)), low, top)

    for c in range(chunks):
        prepare(c)
    for copy in told:
        copy.wait()
    totals = marks[:, 0, :heads]
    for low in range(0, inner, step):
        gains[:, low : low + step] = expand(totals, low, low + step)
    stages = [stage_pair, stage_plane, stage_far, stage_back, finish]
    steps = chunks + lags[-1]
    fillers = list(range(inner // 128))
    per = -(-len(fillers) // lags[-1])
    for k in range(steps):
        for lag, stage in reversed(list(zip(lags, stages))):
            if 0 <= k - lag < chunks:
                if stage is finish:
                    while fillers:
                        inside(fillers.pop(0))
                stage(k - lag)
        for _ in range(per):
            if fillers:
                inside(fillers.pop(0))

    mixed = state["mixed"].astype(BF)
    gproj[:, inner : inner + size] = (dot(mixed, cm, ((0,), (0,))) + state["b"]).astype(BF)
    gproj[:, inner + size : inner + 2 * size] = (
        dot(mixed, bm, ((1,), (0,))) + state["c"]
    ).astype(BF)
    upper = (iota((count, count), 0) <= iota((count, count), 1)).astype(F32)
    grad_log = jnp.dot(upper, state["log"], precision=high, preferred_element_type=F32)
    grad_log = grad_log + state["last"][:1]
    grad_raw = (state["dt"] + grad_log * rate) * jax.nn.sigmoid(raw)
    edge = inner + 2 * size
    gproj[:, edge:] = jnp.zeros((count, gproj.shape[1] - edge), BF)
    gproj[:, edge : edge + heads] = grad_raw.astype(BF)
    for copy in crossing:
        copy.wait()


def ssd_block(xs, joined, raw, gy, guests, a_log, dt_bias, d_skip):
    count, inner = gy.shape
    heads = a_log.shape[0]
    size = joined.shape[1] // 2
    seq = lax.axis_size("seq")
    planes = seq // 4
    chunk = 512
    chunks = inner // chunk
    rows = size // 4
    scalars = jnp.stack([-jnp.exp(a_log), dt_bias, d_skip] + [jnp.zeros_like(a_log)] * 5)
    padded = -(-(inner + 2 * size + heads) // 128) * 128
    wide = pltpu.VMEM((count, inner), F32)
    thin = pltpu.VMEM((count, inner), BF)
    block = pltpu.VMEM((chunks, 2, 2, 2, rows, chunk), BF)
    half = pltpu.VMEM((chunks, 2, 2, rows, chunk), BF)
    dma = pltpu.SemaphoreType.DMA
    return pl.pallas_call(
        functools.partial(core_kernel, inner // heads, chunk, LAGS),
        out_shape=(
            jax.ShapeDtypeStruct((count, inner), BF),
            jax.ShapeDtypeStruct((count, padded), BF),
            jax.ShapeDtypeStruct(guests.shape, BF),
        ),
        in_specs=[pl.BlockSpec(memory_space=pltpu.VMEM)] * 6,
        out_specs=[pl.BlockSpec(memory_space=pltpu.VMEM)] * 3,
        scratch_shapes=[
            pltpu.VMEM((heads, inner), F32),
            wide, wide, wide, thin, thin, thin, wide, wide,
            pltpu.VMEM((count, heads), F32),
            pltpu.VMEM((heads, count), F32),
            pltpu.VMEM((8, 128), F32),
            pltpu.VMEM((seq, 8, 128), F32),
            pltpu.VMEM((seq, inner), F32),
            block, block, half, half,
            pltpu.VMEM((chunks, 2, rows, chunk), BF),
            pltpu.VMEM((chunks, 2, planes, rows, chunk), BF),
            half, half, block, block,
            dma((seq - 1,)), dma((seq - 1,)),
            dma((4, chunks)), dma((4, chunks)),
            dma((chunks, 2, planes)), dma((chunks, 2, planes)),
            dma(guests.shape[:1]), dma(guests.shape[:1]),
        ],
        compiler_params=pltpu.CompilerParams(collective_id=0, has_side_effects=True),
    )(xs, joined, raw, gy, guests, scalars)


def per_device(tokens, w_in, a_log, dt_bias, d_skip, grad_y):
    count, width = tokens.shape[1:]
    inner = grad_y.shape[2]
    heads = a_log.shape[0]
    zero = lax.axis_size("zero")
    seq = lax.axis_size("seq")
    here = lax.axis_index("zero")
    rows = tokens.reshape(count, width)

    stored = w_in.T
    xs, joined, raw = head(rows, stored, inner, heads)

    piece = width // (seq * zero)
    cut = rows.reshape(count, seq // 2, 2, zero, piece)

    def pieces_of(z):
        some = lax.dynamic_index_in_dim(cut, z, 3, keepdims=False)
        return some.transpose(2, 0, 1, 3).reshape(2, count, seq // 2 * piece)

    guests = jnp.stack([pieces_of((here + s) % zero) for s in range(1, zero)])
    y_out, gproj, held = ssd_block(
        xs, joined, raw, grad_y.reshape(count, inner), guests, a_log, dt_bias, d_skip
    )
    grad_w, grad_tokens = tail(gproj, pieces_of(here), held, stored, seq // 2)
    grad_tokens = grad_tokens.reshape(1, count, width)
    return (y_out.reshape(1, count, inner), grad_tokens, grad_w)


def solution(mesh):
    placed = (P("zero", "seq", None), P("zero", None), P(), P(), P(), P("zero", "seq", None))
    return jax.shard_map(
        per_device,
        mesh=mesh,
        in_specs=placed,
        out_specs=(P("zero", "seq", None), P("zero", "seq", None), P(("seq", "zero"), None)),
        check_vma=False,
    )
```

```python
import functools

import jax
import jax.numpy as jnp
from jax import lax
from jax.experimental import pallas as pl
from jax.experimental.pallas import tpu as pltpu
from jax.sharding import PartitionSpec as P

BF = jnp.bfloat16
F32 = jnp.float32
MESH = pl.DeviceIdType.MESH
LAGS = (0, 1, 3, 5, 6)
SPACING = (3, 3)
SWAPPED = (0, 5)


def dot(a, b, dims):
    return lax.dot_general(a, b, (dims, ((), ())), preferred_element_type=F32)


def greet(peers, mates=()):
    barrier = pltpu.get_barrier_semaphore()
    for peer in peers:
        pl.semaphore_signal(barrier, inc=1, device_id={"seq": peer}, device_id_type=MESH)
    for mate in mates:
        pl.semaphore_signal(barrier, inc=1, device_id={"zero": mate}, device_id_type=MESH)
    pl.semaphore_wait(barrier, len(peers) + len(mates))


def remote(src, dst, send, recv, peer):
    return pltpu.make_async_remote_copy(
        src_ref=src,
        dst_ref=dst,
        send_sem=send,
        recv_sem=recv,
        device_id={"seq": peer},
        device_id_type=MESH,
    )


def mate(src, dst, send, recv, peer):
    return pltpu.make_async_remote_copy(
        src_ref=src,
        dst_ref=dst,
        send_sem=send,
        recv_sem=recv,
        device_id={"zero": peer},
        device_id_type=MESH,
    )


def head_kernel(
    zero, inner, rows, stored, xs, pair, raw, weights, guest, kept, made, narrow, back, thin,
    send, recv, load
):
    here = lax.axis_index("zero")
    columns, owned = weights.shape
    exact = made.shape[2]
    heads = columns - exact
    after = [lax.rem(here + s, zero) for s in range(zero)]
    before = [lax.rem(here + zero - s, zero) for s in range(zero)]
    fetch = pltpu.make_async_copy(stored, weights, load)
    fetch.start()
    greet([], after[1:])

    def columns_of(z):
        return pl.ds(pl.multiple_of(z * owned, 128), owned)

    coming = []
    for s in range(1, zero):
        copy = mate(rows.at[:, columns_of(after[s])], guest.at[s - 1], send.at[s, 0], recv.at[s, 0], after[s])
        copy.start()
        coming.append(copy)
    edges = list(range(0, inner, 256)) + [inner]
    spans = [(inner, exact)] + list(zip(edges[:-1], edges[1:]))
    fetch.wait()
    mine = rows[:, columns_of(here)]
    for low, high in spans + [(exact, columns)]:
        kept[:, low:high] = dot(mine, weights[low:high], ((1,), (1,)))
    going = {}
    narrow[...] = jnp.zeros(narrow.shape, F32)
    for s in range(1, zero):
        coming[s - 1].wait()
        narrow[s - 1, :, :heads] = dot(guest[s - 1], weights[exact:], ((1,), (1,)))
        copy = mate(narrow.at[s - 1], thin.at[s - 1], send.at[s, 1], recv.at[s, 1], before[s])
        copy.start()
        going[s, -1] = copy
        for i, (low, high) in enumerate(spans):
            value = dot(guest[s - 1], weights[low:high], ((1,), (1,)))
            made[s - 1, :, low:high] = value.astype(BF)
            copy = mate(
                made.at[s - 1, :, low:high],
                back.at[s - 1, :, low:high],
                send.at[s, 2 + i],
                recv.at[s, 2 + i],
                before[s],
            )
            copy.start()
            going[s, i] = copy
    total = kept[:, exact:]
    for s in range(1, zero):
        going[s, -1].wait()
        total = total + thin[s - 1, :, :heads]
    raw[...] = total
    for i, (low, high) in enumerate(spans):
        total = kept[:, low:high]
        for s in range(1, zero):
            going[s, i].wait()
            total = total + back[s - 1, :, low:high].astype(F32)
        if i:
            xs[:, low:high] = total.astype(BF)
        else:
            pair[...] = total.astype(BF)


def head(rows, weights, inner, heads):
    count, width = rows.shape
    columns, owned = weights.shape
    zero = width // owned
    exact = columns - heads
    steps = 3 + -(-inner // 256)
    return pl.pallas_call(
        functools.partial(head_kernel, zero, inner),
        out_shape=(
            jax.ShapeDtypeStruct((count, inner), BF),
            jax.ShapeDtypeStruct((count, exact - inner), BF),
            jax.ShapeDtypeStruct((count, heads), F32),
        ),
        in_specs=[pl.BlockSpec(memory_space=pltpu.VMEM), pl.BlockSpec(memory_space=pl.ANY)],
        out_specs=[pl.BlockSpec(memory_space=pltpu.VMEM)] * 3,
        scratch_shapes=[
            pltpu.VMEM((columns, owned), BF),
            pltpu.VMEM((zero - 1, count, owned), BF),
            pltpu.VMEM((count, columns), F32),
            pltpu.VMEM((zero - 1, count, exact), BF),
            pltpu.VMEM((zero - 1, count, 128), F32),
            pltpu.VMEM((zero - 1, count, exact), BF),
            pltpu.VMEM((zero - 1, count, 128), F32),
            pltpu.SemaphoreType.DMA((zero, steps)),
            pltpu.SemaphoreType.DMA((zero, steps)),
            pltpu.SemaphoreType.DMA,
        ],
        compiler_params=pltpu.CompilerParams(collective_id=2, vmem_limit_bytes=14 << 20, has_side_effects=True),
    )(rows, weights)


def core_kernel(
    width, chunk, lags, spans, tile,
    xs, joined, raws, gy, rows, stored, a_log, dt_bias, d_skip, y_out, out, grads,
    spread, dts, grows, fades, xds, growns, fadeds, ins, backs, cums, turned, mark, marks, gains,
    loc, both, pairs, duo, sums, far, ret, came, fin, wide, tall, left, right, weights, made,
    tsend, trecv, send, recv, zsend, zrecv, leave, enter, *scratch
):
    seq, planes = marks.shape[0], far.shape[2]
    zero = tall.shape[2]
    load = pltpu.make_async_copy(stored, weights, scratch[-1])
    load.start()
    me, here = lax.axis_index("seq"), lax.axis_index("zero")
    core, chip = lax.rem(me, 2), lax.div(me, 2)
    side, plane = lax.rem(chip, 2), lax.div(chip, 2)
    sibling, across = me + 1 - 2 * core, me + 2 - 4 * side
    peers = [lax.rem(me + d, seq) for d in range(1, seq)]
    after = [lax.rem(here + s, zero) for s in range(zero)]
    before = [lax.rem(here + zero - s, zero) for s in range(zero)]
    count, inner = xs.shape
    heads = raws.shape[1]
    size = joined.shape[1] // 2
    chunks = inner // chunk
    high = lax.Precision.HIGHEST
    far[...] = jnp.zeros(far.shape, BF)
    mark[...] = jnp.zeros(mark.shape, F32)
    greet(peers, after[1:])
    def iota(shape, axis):
        return lax.broadcasted_iota(jnp.int32, shape, axis)

    lower = iota((count, count), 0) >= iota((count, count), 1)
    ones = lower.astype(F32)
    first = iota((heads, inner), 0) * width
    lane = iota((heads, inner), 1)
    spread[...] = ((lane >= first) & (lane < first + width)).astype(F32)
    rate, skip = -jnp.exp(a_log[...]), d_skip[...]
    raw = raws[...] + dt_bias[...]
    dt = jnp.maximum(raw, 0.0) + jnp.log1p(jnp.exp(-jnp.abs(raw)))
    cum = jnp.dot(ones, rate * dt, precision=high, preferred_element_type=F32)
    total = cum[count - 1 : count]
    cums[...] = cum
    turned[...] = cum.T
    mark[0:1, :heads] = total
    marks[me] = mark[...]
    told = [
        remote(mark, marks.at[me], tsend.at[d], trecv.at[d], peer) for d, peer in enumerate(peers)
    ]
    for copy in told:
        copy.start()
    growth, fade = jnp.exp(cum), jnp.exp(total - cum)
    bm, cm = joined[:, :size], joined[:, size:]
    bt, ct = bm.T, cm.T
    skips = jnp.broadcast_to(skip, (8, heads))

    def expand(value, low, top):
        return jnp.dot(value, spread[:, low:top], precision=high, preferred_element_type=F32)

    def gather(value, low, top):
        return lax.dot_general(
            value, spread[:, low:top], (((1,), (1,)), ((), ())), precision=high,
            preferred_element_type=F32,
        )

    step = min(256, chunk)
    copies = {}

    def prepare(c):
        for low in range(c * chunk, (c + 1) * chunk, step):
            top = low + step
            own = slice(low - c * chunk, low - c * chunk + step)
            d, g, f = expand(dt, low, top), expand(growth, low, top), expand(fade, low, top)
            dts[:, low:top], grows[:, low:top], fades[:, low:top] = d, g, f
            xd = (xs[:, low:top].astype(F32) * d).astype(BF)
            grown = (gy[:, low:top].astype(F32) * g).astype(BF)
            faded = (xd.astype(F32) * f).astype(BF)
            xds[:, low:top], growns[:, low:top], fadeds[:, low:top] = xd, grown, faded
            parts = loc.shape[1:2] + loc.shape[3:5] + (step,)
            loc[c, :, 0, :, :, own] = dot(bt, faded, ((1,), (0,))).astype(BF).reshape(parts)
            loc[c, :, 1, :, :, own] = dot(ct, grown, ((1,), (0,))).astype(BF).reshape(parts)
        both[c, core] = loc[c, core]
        copies[0, c] = remote(
            loc.at[c, 1 - core], both.at[c, core], send.at[0, c], recv.at[0, c], sibling
        )
        copies[0, c].start()

    def gain(c, *rows):
        at = slice(c * chunk, (c + 1) * chunk)
        return jnp.exp(sum(gains[pl.ds(row, 1), at] for row in rows))

    def stage_pair(c):
        copies[0, c].wait()
        g0, g1 = gain(c, chip * 2), gain(c, chip * 2 + 1)
        for q in range(2):
            pairs[c, q, 0] = (
                g1 * both[c, 0, 0, q].astype(F32) + both[c, 1, 0, q].astype(F32)
            ).astype(BF)
            pairs[c, q, 1] = (
                g0 * both[c, 1, 1, q].astype(F32) + both[c, 0, 1, q].astype(F32)
            ).astype(BF)
        duo[c, side] = pairs[c, side]
        copies[1, c] = remote(
            pairs.at[c, 1 - side], duo.at[c, side], send.at[1, c], recv.at[1, c], across
        )
        copies[1, c].start()

    def along(c, way, d):
        return remote(
            sums.at[c, way],
            far.at[c, way, plane],
            zsend.at[c, way, d],
            zrecv.at[c, way, d],
            me + (4 * d if way == 0 else -4 * d),
        )

    def later(d, way):
        return plane + d < planes if way == 0 else plane >= d

    def stage_plane(c):
        copies[1, c].wait()
        g0 = gain(c, plane * 4, plane * 4 + 1)
        g1 = gain(c, plane * 4 + 2, plane * 4 + 3)
        sums[c, 0] = (g1 * duo[c, 0, 0].astype(F32) + duo[c, 1, 0].astype(F32)).astype(BF)
        sums[c, 1] = (g0 * duo[c, 1, 1].astype(F32) + duo[c, 0, 1].astype(F32)).astype(BF)
        for d in range(1, planes):
            for way in range(2):

                @pl.when(later(d, way))
                def _():
                    along(c, way, d).start()

    def stage_far(c):
        for d in range(1, planes):
            for way in range(2):

                @pl.when(later(d, 1 - way))
                def _():
                    along(c, way, d).wait_recv()

                @pl.when(later(d, way))
                def _():
                    along(c, way, d).wait_send()

        at = slice(c * chunk, (c + 1) * chunk)
        ends = []
        for way in range(2):
            run = jnp.zeros(far.shape[3:], F32)
            for k in range(planes) if way == 0 else reversed(range(planes)):
                inside = (k < plane if way == 0 else k > plane).astype(F32)
                whole = sum(gains[4 * k + i : 4 * k + i + 1, at] for i in range(4))
                run = jnp.exp(whole * inside) * run + far[c, way, k].astype(F32)
            ends.append(run)
        g0 = gain(c, plane * 4, plane * 4 + 1)
        g1 = gain(c, plane * 4 + 2, plane * 4 + 3)
        ret[c, 0, 0] = ends[0].astype(BF)
        ret[c, 1, 0] = (g0 * ends[0] + duo[c, 0, 0].astype(F32)).astype(BF)
        ret[c, 1, 1] = ends[1].astype(BF)
        ret[c, 0, 1] = (g1 * ends[1] + duo[c, 1, 1].astype(F32)).astype(BF)
        came[c, side] = ret[c, side]
        copies[2, c] = remote(
            ret.at[c, 1 - side], came.at[c, side], send.at[2, c], recv.at[2, c], across
        )
        copies[2, c].start()

    def stage_back(c):
        copies[2, c].wait()
        g0, g1 = gain(c, chip * 2), gain(c, chip * 2 + 1)
        for q in range(2):
            fin[c, 0, 0, q] = came[c, q, 0]
            fin[c, 1, 1, q] = came[c, q, 1]
            fin[c, 1, 0, q] = (
                g0 * came[c, q, 0].astype(F32) + both[c, 0, 0, q].astype(F32)
            ).astype(BF)
            fin[c, 0, 1, q] = (
                g1 * came[c, q, 1].astype(F32) + both[c, 1, 1, q].astype(F32)
            ).astype(BF)
        wide[c, core] = fin[c, core]
        copies[3, c] = remote(
            fin.at[c, 1 - core], wide.at[c, core], send.at[3, c], recv.at[3, c], sibling
        )
        copies[3, c].start()

    scores = dot(cm, bm, ((1,), (1,)))
    group = 128 // width
    state = {
        "mixed": jnp.zeros((count, count), F32),
        "c": jnp.zeros((count, size), F32),
        "b": jnp.zeros((count, size), F32),
        "log": jnp.zeros((count, heads), F32),
        "dt": jnp.zeros((count, heads), F32),
        "last": jnp.zeros((8, heads), F32),
    }
    place = iota((count, 128), 1)
    masks = [(place >= width * i) & (place < width * (i + 1)) for i in range(group)]

    def inside(p):
        low, top = p * 128, (p + 1) * 128
        x2, g2 = xds[:, low:top], gy[:, low:top]
        none = jnp.zeros_like(x2)
        decays = []
        for i in range(group):
            h = p * group + i
            spans = cums[:, h : h + 1] - turned[h : h + 1, :]
            decays.append(jnp.where(lower, jnp.exp(jnp.where(lower, spans, 0.0)), 0.0))
        mixing = jnp.concatenate([(scores * decay).astype(BF) for decay in decays], axis=1)
        stacked = jnp.concatenate([jnp.where(mask, x2, none) for mask in masks], axis=0)
        ins[:, low:top] = dot(mixing, stacked, ((1,), (0,)))
        tall = dot(mixing, g2, ((0,), (0,)))
        back = tall[:count]
        for i in range(1, group):
            back = jnp.where(masks[i], tall[i * count : (i + 1) * count], back)
        backs[:, low:top] = back
        lifted = jnp.concatenate([jnp.where(mask, g2, none) for mask in masks], axis=0)
        cross = dot(lifted, x2, ((1,), (1,)))
        for i in range(group):
            state["mixed"] += cross[i * count : (i + 1) * count] * decays[i]

    def finish(c):
        copies[3, c].wait()
        for low in range(c * chunk, (c + 1) * chunk, step):
            top = low + step
            own = slice(low - c * chunk, low - c * chunk + step)
            start = wide[c, :, 0, :, :, own].reshape(size, step)
            end = wide[c, :, 1, :, :, own].reshape(size, step)
            x, g = xs[:, low:top].astype(F32), gy[:, low:top].astype(F32)
            d, xd = dts[:, low:top], xds[:, low:top].astype(F32)
            reached = dot(bm, end, ((1,), (0,))) * fades[:, low:top]
            y3 = ins[:, low:top] + dot(cm, start, ((1,), (0,))) * grows[:, low:top]
            h3 = backs[:, low:top] + reached
            kept = expand(skips, low, top)[:1]
            y_out[:, low:top] = (y3 + kept * x).astype(BF)
            right[:count, low:top] = (h3 * d + kept * g).astype(BF)
            state["c"] += dot(growns[:, low:top], start, ((1,), (1,)))
            state["b"] += dot(fadeds[:, low:top], end, ((1,), (1,)))
            state["log"] += gather(g * y3 - xd * h3, low, top)
            state["dt"] += gather(x * h3, low, top)
            joint = jnp.sum(start.astype(F32) * end.astype(F32), axis=0, keepdims=True)
            joint = joint * jnp.exp(gains[pl.ds(me, 1), low:top])
            last = jnp.sum(xd * reached, axis=0, keepdims=True) + joint
            state["last"] += gather(jnp.broadcast_to(last, (8, step)), low, top)

    pieces, piece, tokens = left.shape[1:]
    levels = (seq // 2).bit_length() - 1
    bits = [lax.rem(lax.div(chip, 1 << b), 2) for b in range(levels)]
    partners = [me + (1 - 2 * bits[b]) * (2 << b) for b in range(levels)]
    parts = len(spans)
    up = list(range(levels))
    orders = [up[1:] + up[:1] if h in SWAPPED else up for h in range(parts)]
    acc, away, come = (scratch[i * parts : (i + 1) * parts] for i in range(3))
    rest = scratch[3 * parts : -7]
    outs = [rest[h * levels : (h + 1) * levels] for h in range(parts)]
    inns = [rest[(parts + h) * levels : (parts + h + 1) * levels] for h in range(parts)]
    dsend, drecv, put, got, back_send, back_recv = scratch[-7:-1]
    crossing = []

    def cross():
        for low in range(0, rows.shape[1], 128):
            block = rows[:, low : low + 128].astype(F32).T.reshape(128 // piece, piece, count)
            for i in range(128 // piece):
                q = low // piece + i
                tall[q // (2 * zero), q // zero % 2, q % zero] = block[i].astype(BF)
        for way in range(2):
            for s in range(1, zero):
                copy = mate(
                    tall.at[:, way, after[s]],
                    left.at[way, :, :, s * count : (s + 1) * count],
                    leave.at[way, s - 1],
                    enter.at[way, s - 1],
                    after[s],
                )
                copy.start()
                crossing.append(copy)
            left[way, :, :, :count] = tall[:, way, here]

    arriving = {}

    def ready(h):
        low, high = spans[h]
        arriving[h] = []
        for s in range(1, zero):
            copy = mate(
                right.at[:count, low:high],
                right.at[s * count : (s + 1) * count, low:high],
                put.at[h, s],
                got.at[h, s],
                after[s],
            )
            copy.start()
            arriving[h].append(copy)

    columns, owned = weights.shape
    mine_at = pl.multiple_of(here * owned, 128)

    def project(values, target, origin):
        @pl.loop(0, owned // tile)
        def _(i):
            at = pl.multiple_of(i * tile, 128)
            value = dot(values[:, :columns], weights[:, pl.ds(at, tile)], ((1,), (0,)))
            target[:, pl.ds(pl.multiple_of(origin + at, 128), tile)] = value.astype(BF)


    def multiply(side, h, target):
        low, high = spans[h]
        lines = left[side].reshape(pieces * piece, tokens)
        value = jnp.dot(lines, right[:, low:high], preferred_element_type=F32)
        target[...] = value.reshape(target.shape).astype(target.dtype)

    pushed = []

    def front(h):
        for copy in arriving[h]:
            copy.wait()
        multiply(1 - core, h, away[h])
        copy = remote(away[h], come[h], dsend.at[h, levels], drecv.at[h, levels], sibling)
        copy.start()
        pushed.append(copy)
        multiply(core, h, acc[h])

    def join(h):
        pushed[h].wait()

        @pl.loop(0, pieces)
        def _(i):
            acc[h][i] += come[h][i].astype(F32)

    def subsets(rest):
        found = [0]
        for b in rest:
            found = found + [value + (1 << b) for value in found]
        return found

    flying = {}

    def begin(h, s):
        order = orders[h]
        b = order[s]
        base = sum((bits[f] * (1 << f) for f in order[:s]), 0)
        for j, extra in enumerate(subsets(order[s + 1 :])):
            outs[h][s][j] = acc[h][base + (1 - bits[b]) * (1 << b) + extra].astype(BF)
        copy = remote(outs[h][s], inns[h][s], dsend.at[h, s], drecv.at[h, s], partners[b])
        copy.start()
        flying[h] = copy

    def settle(h, s):
        flying[h].wait()
        order = orders[h]
        base = sum((bits[f] * (1 << f) for f in order[: s + 1]), 0)
        for j, extra in enumerate(subsets(order[s + 1 :])):
            acc[h][base + extra] += inns[h][s][j].astype(F32)

    lag, skew = SPACING
    returning = []

    def advance(k):
        if k < parts:
            front(k)
        if 1 <= k <= parts:
            join(k - 1)
            begin(k - 1, 0)
        if k == parts:
            load.wait()
            for s in range(1, zero):
                project(right.at[s * count : (s + 1) * count], made.at[s - 1], 0)
                copy = mate(
                    made.at[s - 1],
                    grads.at[:, pl.ds(mine_at, owned)],
                    back_send.at[s],
                    back_recv.at[s],
                    before[s],
                )
                copy.start()
                returning.append(copy)
            project(right.at[:count], grads, mine_at)
        for s in reversed(range(levels)):
            h = k - lag - skew * s
            if 0 <= h < parts:
                settle(h, s)
                if s + 1 < levels:
                    begin(h, s + 1)
                else:
                    low, high = spans[h][0], min(spans[h][1], columns)
                    out[:, low:high] = acc[h][chip, :, : high - low]

    for c in range(chunks):
        prepare(c)
    for copy in told:
        copy.wait()
    totals = marks[:, 0, :heads]
    for low in range(0, inner, step):
        gains[:, low : low + step] = expand(totals, low, low + step)
    stages = [stage_pair, stage_plane, stage_far, stage_back, finish]
    steps = chunks + lags[-1]
    fillers = list(range(inner // 128))
    per = -(-len(fillers) // lags[-1])
    moved = 0
    for k in range(steps):
        for lagging, stage in reversed(list(zip(lags, stages))):
            c = k - lagging
            if 0 <= c < chunks:
                if stage is finish:
                    while fillers and fillers[0] * 128 < (c + 1) * chunk:
                        inside(fillers.pop(0))
                stage(c)
                if stage is finish:
                    for h in range(parts):
                        if c * chunk <= spans[h][0] < (c + 1) * chunk:
                            ready(h)
        if k == 0:
            cross()
        for _ in range(per):
            if fillers:
                inside(fillers.pop(0))
        if k == lags[-1] + 1:
            for copy in crossing:
                copy.wait()
        if k > lags[-1]:
            while spans[moved][0] < (k - lags[-1]) * chunk:
                advance(moved)
                moved += 1

    mixed = state["mixed"].astype(BF)
    right[:count, inner : inner + size] = (dot(mixed, cm, ((0,), (0,))) + state["b"]).astype(BF)
    right[:count, inner + size : inner + 2 * size] = (
        dot(mixed, bm, ((1,), (0,))) + state["c"]
    ).astype(BF)
    upper = (iota((count, count), 0) <= iota((count, count), 1)).astype(F32)
    grad_log = jnp.dot(upper, state["log"], precision=high, preferred_element_type=F32)
    grad_log = grad_log + state["last"][:1]
    grad_raw = (state["dt"] + grad_log * rate) * jax.nn.sigmoid(raw)
    edge = inner + 2 * size
    right[:count, edge:] = jnp.zeros((count, right.shape[1] - edge), BF)
    right[:count, edge : edge + heads] = grad_raw.astype(BF)
    for h in range(parts):
        if spans[h][0] >= inner:
            ready(h)
    for k in range(moved, parts + lag + skew * levels):
        advance(k)
    for copy in returning:
        copy.wait()


def ssd_block(xs, joined, raw, gy, rows, weights, a_log, dt_bias, d_skip):
    count, inner = gy.shape
    heads = a_log.shape[0]
    size = joined.shape[1] // 2
    columns, owned = weights.shape
    seq, zero = lax.axis_size("seq"), lax.axis_size("zero")
    planes, pieces = seq // 4, seq // 2
    piece, tokens = owned // seq, zero * count
    levels = pieces.bit_length() - 1
    chunk = 512
    chunks = inner // chunk
    quarter = size // 4
    padded = -(-columns // 128) * 128
    edges = list(range(0, padded, 256)) + [padded]
    spans = list(zip(edges[:-1], edges[1:]))
    parts = len(spans)
    widths = [high - low for low, high in spans]
    tall = pltpu.VMEM((count, inner), F32)
    thin = pltpu.VMEM((count, inner), BF)
    block = pltpu.VMEM((chunks, 2, 2, 2, quarter, chunk), BF)
    half = pltpu.VMEM((chunks, 2, 2, quarter, chunk), BF)
    dma = pltpu.SemaphoreType.DMA
    scratch = [
        pltpu.VMEM((heads, inner), F32),
        tall, tall, tall, thin, thin, thin, tall, tall,
        pltpu.VMEM((count, heads), F32),
        pltpu.VMEM((heads, count), F32),
        pltpu.VMEM((8, 128), F32),
        pltpu.VMEM((seq, 8, 128), F32),
        pltpu.VMEM((seq, inner), F32),
        block, block, half, half,
        pltpu.VMEM((chunks, 2, quarter, chunk), BF),
        pltpu.VMEM((chunks, 2, planes, quarter, chunk), BF),
        half, half, block, block,
        pltpu.VMEM((pieces, 2, zero, piece, count), BF),
        pltpu.VMEM((2, pieces, piece, tokens), BF),
        pltpu.VMEM((tokens, padded), BF),
        pltpu.VMEM(weights.shape, BF),
        pltpu.VMEM((zero - 1, count, owned), BF),
        dma((seq - 1,)), dma((seq - 1,)),
        dma((4, chunks)), dma((4, chunks)),
        dma((chunks, 2, planes)), dma((chunks, 2, planes)),
        dma((2, zero - 1)), dma((2, zero - 1)),
    ]
    scratch += [pltpu.VMEM((pieces, piece, w), F32) for w in widths]
    scratch += [pltpu.VMEM((pieces, piece, w), BF) for w in widths] * 2
    for _ in range(2):
        for w in widths:
            scratch += [pltpu.VMEM((pieces >> (s + 1), piece, w), BF) for s in range(levels)]
    scratch += [dma((parts, levels + 1))] * 2 + [dma((parts, zero))] * 2 + [dma((zero,))] * 2
    scratch += [dma]
    local = pl.BlockSpec(memory_space=pltpu.VMEM)
    return pl.pallas_call(
        functools.partial(core_kernel, inner // heads, chunk, LAGS, spans, min(256, owned)),
        out_shape=(
            jax.ShapeDtypeStruct((count, inner), BF),
            jax.ShapeDtypeStruct((piece, columns), F32),
            jax.ShapeDtypeStruct((count, zero * owned), BF),
        ),
        in_specs=[local] * 5 + [pl.BlockSpec(memory_space=pl.ANY)] + [local] * 3,
        out_specs=[local] * 3,
        scratch_shapes=scratch,
        compiler_params=pltpu.CompilerParams(collective_id=0, vmem_limit_bytes=48 << 20, has_side_effects=True),
    )(xs, joined, raw, gy, rows, weights, a_log[None], dt_bias[None], d_skip[None])


def per_device(tokens, w_in, a_log, dt_bias, d_skip, grad_y):
    count, width = tokens.shape[1:]
    inner = grad_y.shape[2]
    heads = a_log.shape[0]
    rows = tokens.reshape(count, width)

    stored = w_in.T
    xs, joined, raw = head(rows, stored, inner, heads)

    y_out, grad_w, grad_tokens = ssd_block(
        xs, joined, raw, grad_y.reshape(count, inner), rows, stored, a_log, dt_bias, d_skip
    )
    grad_tokens = grad_tokens.reshape(1, count, width)
    return (y_out.reshape(1, count, inner), grad_tokens, grad_w)


def solution(mesh):
    placed = (P("zero", "seq", None), P("zero", None), P(), P(), P(), P("zero", "seq", None))
    return jax.shard_map(
        per_device,
        mesh=mesh,
        in_specs=placed,
        out_specs=(P("zero", "seq", None), P("zero", "seq", None), P(("seq", "zero"), None)),
        check_vma=False,
    )
```

```python
import functools

import jax
import jax.numpy as jnp
from jax import lax
from jax.experimental import pallas as pl
from jax.experimental.pallas import tpu as pltpu
from jax.sharding import PartitionSpec as P

BF = jnp.bfloat16
VMEM = 56 << 20
F32 = jnp.float32
MESH = pl.DeviceIdType.MESH
LAGS = (0, 1, 2, 4, 5, 6)
SPACING = (3, 3)
SWAPPED = (0, 5)


def dot(a, b, dims):
    return lax.dot_general(a, b, (dims, ((), ())), preferred_element_type=F32)


def greet(peers, mates=()):
    barrier = pltpu.get_barrier_semaphore()
    for peer in peers:
        pl.semaphore_signal(barrier, inc=1, device_id={"seq": peer}, device_id_type=MESH)
    for mate in mates:
        pl.semaphore_signal(barrier, inc=1, device_id={"zero": mate}, device_id_type=MESH)
    pl.semaphore_wait(barrier, len(peers) + len(mates))


def remote(src, dst, send, recv, peer):
    return pltpu.make_async_remote_copy(
        src_ref=src,
        dst_ref=dst,
        send_sem=send,
        recv_sem=recv,
        device_id={"seq": peer},
        device_id_type=MESH,
    )


def mate(src, dst, send, recv, peer):
    return pltpu.make_async_remote_copy(
        src_ref=src,
        dst_ref=dst,
        send_sem=send,
        recv_sem=recv,
        device_id={"zero": peer},
        device_id_type=MESH,
    )


def core_kernel(
    width, chunk, lags, spans, tile,
    rows, stored, gy, a_log, dt_bias, d_skip, y_out, out, grads,
    xs, joined, guest, kept, shares, narrow, returned, thinned, hsend, hrecv, spread, dts, grows, fades, xds, growns, fadeds, ins, backs, cums, turned, mark, marks, gains,
    loc, both, pairs, duo, sums, far, ret, came, fin, wide, tall, left, right, weights, made,
    tsend, trecv, send, recv, zsend, zrecv, leave, enter, *scratch
):
    seq, planes = marks.shape[0], far.shape[2]
    zero = tall.shape[2]
    load = pltpu.make_async_copy(stored, weights, scratch[-1])
    load.start()
    me, here = lax.axis_index("seq"), lax.axis_index("zero")
    core, chip = lax.rem(me, 2), lax.div(me, 2)
    side, plane = lax.rem(chip, 2), lax.div(chip, 2)
    sibling, across = me + 1 - 2 * core, me + 2 - 4 * side
    peers = [lax.rem(me + d, seq) for d in range(1, seq)]
    after = [lax.rem(here + s, zero) for s in range(zero)]
    before = [lax.rem(here + zero - s, zero) for s in range(zero)]
    count, inner = xs.shape
    heads = a_log.shape[1]
    columns, owned = weights.shape
    exact = columns - heads
    size = joined.shape[1] // 2
    chunks = inner // chunk
    high = lax.Precision.HIGHEST
    far[...] = jnp.zeros(far.shape, BF)
    mark[...] = jnp.zeros(mark.shape, F32)
    narrow[...] = jnp.zeros(narrow.shape, F32)
    greet(peers, after[1:])

    def columns_of(z):
        return pl.ds(pl.multiple_of(z * owned, 128), owned)

    coming = []
    for s in range(1, zero):
        copy = mate(
            rows.at[:, columns_of(after[s])],
            guest.at[s - 1],
            hsend.at[s, 0],
            hrecv.at[s, 0],
            after[s],
        )
        copy.start()
        coming.append(copy)
    step = min(256, chunk)
    slabs = [(inner, exact)] + [(low, low + step) for low in range(0, inner, step)]
    load.wait()
    for low, top in slabs + [(exact, columns)]:
        kept[:, low:top] = dot(rows[:, columns_of(here)], weights[low:top], ((1,), (1,)))
    going = {}
    for s in range(1, zero):
        coming[s - 1].wait()
        narrow[s - 1, :, :heads] = dot(guest[s - 1], weights[exact:], ((1,), (1,)))
        going[s, -1] = mate(
            narrow.at[s - 1], thinned.at[s - 1], hsend.at[s, 1], hrecv.at[s, 1], before[s]
        )
        going[s, -1].start()
        for i, (low, top) in enumerate(slabs):
            shares[s - 1, :, low:top] = dot(guest[s - 1], weights[low:top], ((1,), (1,))).astype(BF)
            going[s, i] = mate(
                shares.at[s - 1, :, low:top],
                returned.at[s - 1, :, low:top],
                hsend.at[s, 2 + i],
                hrecv.at[s, 2 + i],
                before[s],
            )
            going[s, i].start()

    def slab(i):
        low, top = slabs[i]
        value = kept[:, low:top]
        for s in range(1, zero):
            going[s, i].wait()
            value = value + returned[s - 1, :, low:top].astype(F32)
        return value.astype(BF)

    def iota(shape, axis):
        return lax.broadcasted_iota(jnp.int32, shape, axis)

    lower = iota((count, count), 0) >= iota((count, count), 1)
    ones = lower.astype(F32)
    first = iota((heads, inner), 0) * width
    lane = iota((heads, inner), 1)
    spread[...] = ((lane >= first) & (lane < first + width)).astype(F32)
    rate, skip = -jnp.exp(a_log[...]), d_skip[...]
    raw = kept[:, exact:]
    for s in range(1, zero):
        going[s, -1].wait()
        raw = raw + thinned[s - 1, :, :heads]
    raw = raw + dt_bias[...]
    dt = jnp.maximum(raw, 0.0) + jnp.log1p(jnp.exp(-jnp.abs(raw)))
    cum = jnp.dot(ones, rate * dt, precision=high, preferred_element_type=F32)
    total = cum[count - 1 : count]
    cums[...] = cum
    turned[...] = cum.T
    mark[0:1, :heads] = total
    marks[me] = mark[...]
    told = [
        remote(mark, marks.at[me], tsend.at[d], trecv.at[d], peer) for d, peer in enumerate(peers)
    ]
    for copy in told:
        copy.start()
    growth, fade = jnp.exp(cum), jnp.exp(total - cum)
    joined[...] = slab(0)
    bm, cm = joined[:, :size], joined[:, size:]
    bt, ct = bm.T, cm.T
    skips = jnp.broadcast_to(skip, (8, heads))

    def expand(value, low, top):
        return jnp.dot(value, spread[:, low:top], precision=high, preferred_element_type=F32)

    def gather(value, low, top):
        return lax.dot_general(
            value, spread[:, low:top], (((1,), (1,)), ((), ())), precision=high,
            preferred_element_type=F32,
        )

    copies = {}

    def prepare(c):
        for low in range(c * chunk, (c + 1) * chunk, step):
            top = low + step
            own = slice(low - c * chunk, low - c * chunk + step)
            xs[:, low:top] = slab(1 + low // step)
            d, g, f = expand(dt, low, top), expand(growth, low, top), expand(fade, low, top)
            dts[:, low:top], grows[:, low:top], fades[:, low:top] = d, g, f
            xd = (xs[:, low:top].astype(F32) * d).astype(BF)
            grown = (gy[:, low:top].astype(F32) * g).astype(BF)
            faded = (xd.astype(F32) * f).astype(BF)
            xds[:, low:top], growns[:, low:top], fadeds[:, low:top] = xd, grown, faded
            parts = loc.shape[1:2] + loc.shape[3:5] + (step,)
            loc[c, :, 0, :, :, own] = dot(bt, faded, ((1,), (0,))).astype(BF).reshape(parts)
            loc[c, :, 1, :, :, own] = dot(ct, grown, ((1,), (0,))).astype(BF).reshape(parts)
        both[c, core] = loc[c, core]
        copies[0, c] = remote(
            loc.at[c, 1 - core], both.at[c, core], send.at[0, c], recv.at[0, c], sibling
        )
        copies[0, c].start()

    def gain(c, *rows):
        at = slice(c * chunk, (c + 1) * chunk)
        return jnp.exp(sum(gains[pl.ds(row, 1), at] for row in rows))

    def stage_pair(c):
        copies[0, c].wait()
        g0, g1 = gain(c, chip * 2), gain(c, chip * 2 + 1)
        for q in range(2):
            pairs[c, q, 0] = (
                g1 * both[c, 0, 0, q].astype(F32) + both[c, 1, 0, q].astype(F32)
            ).astype(BF)
            pairs[c, q, 1] = (
                g0 * both[c, 1, 1, q].astype(F32) + both[c, 0, 1, q].astype(F32)
            ).astype(BF)
        duo[c, side] = pairs[c, side]
        copies[1, c] = remote(
            pairs.at[c, 1 - side], duo.at[c, side], send.at[1, c], recv.at[1, c], across
        )
        copies[1, c].start()

    def along(c, way, d):
        return remote(
            sums.at[c, way],
            far.at[c, way, plane],
            zsend.at[c, way, d],
            zrecv.at[c, way, d],
            me + (4 * d if way == 0 else -4 * d),
        )

    def later(d, way):
        return plane + d < planes if way == 0 else plane >= d

    def stage_plane(c):
        copies[1, c].wait()
        g0 = gain(c, plane * 4, plane * 4 + 1)
        g1 = gain(c, plane * 4 + 2, plane * 4 + 3)
        sums[c, 0] = (g1 * duo[c, 0, 0].astype(F32) + duo[c, 1, 0].astype(F32)).astype(BF)
        sums[c, 1] = (g0 * duo[c, 1, 1].astype(F32) + duo[c, 0, 1].astype(F32)).astype(BF)
        for d in range(1, planes):
            for way in range(2):

                @pl.when(later(d, way))
                def _():
                    along(c, way, d).start()

    def stage_far(c):
        for d in range(1, planes):
            for way in range(2):

                @pl.when(later(d, 1 - way))
                def _():
                    along(c, way, d).wait_recv()

                @pl.when(later(d, way))
                def _():
                    along(c, way, d).wait_send()

        at = slice(c * chunk, (c + 1) * chunk)
        ends = []
        for way in range(2):
            run = jnp.zeros(far.shape[3:], F32)
            for k in range(planes) if way == 0 else reversed(range(planes)):
                inside = (k < plane if way == 0 else k > plane).astype(F32)
                whole = sum(gains[4 * k + i : 4 * k + i + 1, at] for i in range(4))
                run = jnp.exp(whole * inside) * run + far[c, way, k].astype(F32)
            ends.append(run)
        g0 = gain(c, plane * 4, plane * 4 + 1)
        g1 = gain(c, plane * 4 + 2, plane * 4 + 3)
        ret[c, 0, 0] = ends[0].astype(BF)
        ret[c, 1, 0] = (g0 * ends[0] + duo[c, 0, 0].astype(F32)).astype(BF)
        ret[c, 1, 1] = ends[1].astype(BF)
        ret[c, 0, 1] = (g1 * ends[1] + duo[c, 1, 1].astype(F32)).astype(BF)
        came[c, side] = ret[c, side]
        copies[2, c] = remote(
            ret.at[c, 1 - side], came.at[c, side], send.at[2, c], recv.at[2, c], across
        )
        copies[2, c].start()

    def stage_back(c):
        copies[2, c].wait()
        g0, g1 = gain(c, chip * 2), gain(c, chip * 2 + 1)
        for q in range(2):
            fin[c, 0, 0, q] = came[c, q, 0]
            fin[c, 1, 1, q] = came[c, q, 1]
            fin[c, 1, 0, q] = (
                g0 * came[c, q, 0].astype(F32) + both[c, 0, 0, q].astype(F32)
            ).astype(BF)
            fin[c, 0, 1, q] = (
                g1 * came[c, q, 1].astype(F32) + both[c, 1, 1, q].astype(F32)
            ).astype(BF)
        wide[c, core] = fin[c, core]
        copies[3, c] = remote(
            fin.at[c, 1 - core], wide.at[c, core], send.at[3, c], recv.at[3, c], sibling
        )
        copies[3, c].start()

    scores = dot(cm, bm, ((1,), (1,)))
    group = 128 // width
    state = {
        "mixed": jnp.zeros((count, count), F32),
        "c": jnp.zeros((count, size), F32),
        "b": jnp.zeros((count, size), F32),
        "log": jnp.zeros((count, heads), F32),
        "dt": jnp.zeros((count, heads), F32),
        "last": jnp.zeros((8, heads), F32),
    }
    place = iota((count, 128), 1)
    masks = [(place >= width * i) & (place < width * (i + 1)) for i in range(group)]

    def inside(p):
        low, top = p * 128, (p + 1) * 128
        x2, g2 = xds[:, low:top], gy[:, low:top]
        none = jnp.zeros_like(x2)
        decays = []
        for i in range(group):
            h = p * group + i
            spans = cums[:, h : h + 1] - turned[h : h + 1, :]
            decays.append(jnp.where(lower, jnp.exp(jnp.where(lower, spans, 0.0)), 0.0))
        mixing = jnp.concatenate([(scores * decay).astype(BF) for decay in decays], axis=1)
        stacked = jnp.concatenate([jnp.where(mask, x2, none) for mask in masks], axis=0)
        ins[:, low:top] = dot(mixing, stacked, ((1,), (0,)))
        tall = dot(mixing, g2, ((0,), (0,)))
        back = tall[:count]
        for i in range(1, group):
            back = jnp.where(masks[i], tall[i * count : (i + 1) * count], back)
        backs[:, low:top] = back
        lifted = jnp.concatenate([jnp.where(mask, g2, none) for mask in masks], axis=0)
        cross = dot(lifted, x2, ((1,), (1,)))
        for i in range(group):
            state["mixed"] += cross[i * count : (i + 1) * count] * decays[i]

    def finish(c):
        copies[3, c].wait()
        for low in range(c * chunk, (c + 1) * chunk, step):
            top = low + step
            own = slice(low - c * chunk, low - c * chunk + step)
            start = wide[c, :, 0, :, :, own].reshape(size, step)
            end = wide[c, :, 1, :, :, own].reshape(size, step)
            x, g = xs[:, low:top].astype(F32), gy[:, low:top].astype(F32)
            d, xd = dts[:, low:top], xds[:, low:top].astype(F32)
            reached = dot(bm, end, ((1,), (0,))) * fades[:, low:top]
            y3 = ins[:, low:top] + dot(cm, start, ((1,), (0,))) * grows[:, low:top]
            h3 = backs[:, low:top] + reached
            kept = expand(skips, low, top)[:1]
            y_out[:, low:top] = (y3 + kept * x).astype(BF)
            right[:count, low:top] = (h3 * d + kept * g).astype(BF)
            state["c"] += dot(growns[:, low:top], start, ((1,), (1,)))
            state["b"] += dot(fadeds[:, low:top], end, ((1,), (1,)))
            state["log"] += gather(g * y3 - xd * h3, low, top)
            state["dt"] += gather(x * h3, low, top)
            joint = jnp.sum(start.astype(F32) * end.astype(F32), axis=0, keepdims=True)
            joint = joint * jnp.exp(gains[pl.ds(me, 1), low:top])
            last = jnp.sum(xd * reached, axis=0, keepdims=True) + joint
            state["last"] += gather(jnp.broadcast_to(last, (8, step)), low, top)

    pieces, piece, tokens = left.shape[1:]
    levels = (seq // 2).bit_length() - 1
    bits = [lax.rem(lax.div(chip, 1 << b), 2) for b in range(levels)]
    partners = [me + (1 - 2 * bits[b]) * (2 << b) for b in range(levels)]
    parts = len(spans)
    up = list(range(levels))
    orders = [up[1:] + up[:1] if h in SWAPPED else up for h in range(parts)]
    acc, away, come = (scratch[i * parts : (i + 1) * parts] for i in range(3))
    rest = scratch[3 * parts : -7]
    outs = [rest[h * levels : (h + 1) * levels] for h in range(parts)]
    inns = [rest[(parts + h) * levels : (parts + h + 1) * levels] for h in range(parts)]
    dsend, drecv, put, got, back_send, back_recv = scratch[-7:-1]
    crossing = []

    def cross():
        for low in range(0, rows.shape[1], 128):
            block = rows[:, low : low + 128].astype(F32).T.reshape(128 // piece, piece, count)
            for i in range(128 // piece):
                q = low // piece + i
                tall[q // (2 * zero), q // zero % 2, q % zero] = block[i].astype(BF)
        for way in range(2):
            for s in range(1, zero):
                copy = mate(
                    tall.at[:, way, after[s]],
                    left.at[way, :, :, s * count : (s + 1) * count],
                    leave.at[way, s - 1],
                    enter.at[way, s - 1],
                    after[s],
                )
                copy.start()
                crossing.append(copy)
            left[way, :, :, :count] = tall[:, way, here]

    arriving = {}

    def ready(h):
        low, high = spans[h]
        arriving[h] = []
        for s in range(1, zero):
            copy = mate(
                right.at[:count, low:high],
                right.at[s * count : (s + 1) * count, low:high],
                put.at[h, s],
                got.at[h, s],
                after[s],
            )
            copy.start()
            arriving[h].append(copy)

    mine_at = pl.multiple_of(here * owned, 128)

    def project(values, target, origin):
        @pl.loop(0, owned // tile)
        def _(i):
            at = pl.multiple_of(i * tile, 128)
            value = dot(values[:, :columns], weights[:, pl.ds(at, tile)], ((1,), (0,)))
            target[:, pl.ds(pl.multiple_of(origin + at, 128), tile)] = value.astype(BF)


    def multiply(side, h, target):
        low, high = spans[h]
        lines = left[side].reshape(pieces * piece, tokens)
        value = jnp.dot(lines, right[:, low:high], preferred_element_type=F32)
        target[...] = value.reshape(target.shape).astype(target.dtype)

    pushed = []

    def front(h):
        for copy in arriving[h]:
            copy.wait()
        multiply(1 - core, h, away[h])
        copy = remote(away[h], come[h], dsend.at[h, levels], drecv.at[h, levels], sibling)
        copy.start()
        pushed.append(copy)
        multiply(core, h, acc[h])

    def join(h):
        pushed[h].wait()

        @pl.loop(0, pieces)
        def _(i):
            acc[h][i] += come[h][i].astype(F32)

    def subsets(rest):
        found = [0]
        for b in rest:
            found = found + [value + (1 << b) for value in found]
        return found

    flying = {}

    def begin(h, s):
        order = orders[h]
        b = order[s]
        base = sum((bits[f] * (1 << f) for f in order[:s]), 0)
        for j, extra in enumerate(subsets(order[s + 1 :])):
            outs[h][s][j] = acc[h][base + (1 - bits[b]) * (1 << b) + extra].astype(BF)
        copy = remote(outs[h][s], inns[h][s], dsend.at[h, s], drecv.at[h, s], partners[b])
        copy.start()
        flying[h] = copy

    def settle(h, s):
        flying[h].wait()
        order = orders[h]
        base = sum((bits[f] * (1 << f) for f in order[: s + 1]), 0)
        for j, extra in enumerate(subsets(order[s + 1 :])):
            acc[h][base + extra] += inns[h][s][j].astype(F32)

    lag, skew = SPACING
    returning = []

    def advance(k):
        if k < parts:
            front(k)
        if 1 <= k <= parts:
            join(k - 1)
            begin(k - 1, 0)
        if k == parts:
            for s in range(1, zero):
                project(right.at[s * count : (s + 1) * count], made.at[s - 1], 0)
                copy = mate(
                    made.at[s - 1],
                    grads.at[:, pl.ds(mine_at, owned)],
                    back_send.at[s],
                    back_recv.at[s],
                    before[s],
                )
                copy.start()
                returning.append(copy)
            project(right.at[:count], grads, mine_at)
        for s in reversed(range(levels)):
            h = k - lag - skew * s
            if 0 <= h < parts:
                settle(h, s)
                if s + 1 < levels:
                    begin(h, s + 1)
                else:
                    low, high = spans[h][0], min(spans[h][1], columns)
                    out[:, low:high] = acc[h][chip, :, : high - low]

    def spread_totals():
        for copy in told:
            copy.wait()
        totals = marks[:, 0, :heads]
        for low in range(0, inner, step):
            gains[:, low : low + step] = expand(totals, low, low + step)

    stages = [prepare, stage_pair, stage_plane, stage_far, stage_back, finish]
    steps = chunks + lags[-1]
    fillers = list(range(inner // 128))
    per = -(-len(fillers) // lags[-1])
    moved = 0
    for k in range(steps):
        for lagging, stage in reversed(list(zip(lags, stages))):
            c = k - lagging
            if 0 <= c < chunks:
                if stage is finish:
                    while fillers and fillers[0] * 128 < (c + 1) * chunk:
                        inside(fillers.pop(0))
                if stage is stage_pair and c == 0:
                    spread_totals()
                stage(c)
                if stage is finish:
                    for h in range(parts):
                        if c * chunk <= spans[h][0] < (c + 1) * chunk:
                            ready(h)
        if k == 0:
            cross()
        for _ in range(per):
            if fillers and fillers[0] * 128 < (k + 1) * chunk:
                inside(fillers.pop(0))
        if k == lags[-1] + 1:
            for copy in crossing:
                copy.wait()
        if k > lags[-1]:
            while spans[moved][0] < (k - lags[-1]) * chunk:
                advance(moved)
                moved += 1

    mixed = state["mixed"].astype(BF)
    right[:count, inner : inner + size] = (dot(mixed, cm, ((0,), (0,))) + state["b"]).astype(BF)
    right[:count, inner + size : inner + 2 * size] = (
        dot(mixed, bm, ((1,), (0,))) + state["c"]
    ).astype(BF)
    upper = (iota((count, count), 0) <= iota((count, count), 1)).astype(F32)
    grad_log = jnp.dot(upper, state["log"], precision=high, preferred_element_type=F32)
    grad_log = grad_log + state["last"][:1]
    grad_raw = (state["dt"] + grad_log * rate) * jax.nn.sigmoid(raw)
    edge = inner + 2 * size
    right[:count, edge:] = jnp.zeros((count, right.shape[1] - edge), BF)
    right[:count, edge : edge + heads] = grad_raw.astype(BF)
    for h in range(parts):
        if spans[h][0] >= inner:
            ready(h)
    for k in range(moved, parts + lag + skew * levels):
        advance(k)
    for copy in returning:
        copy.wait()


def layer(rows, weights, gy, a_log, dt_bias, d_skip):
    count, inner = gy.shape
    heads = a_log.shape[0]
    columns, owned = weights.shape
    exact = columns - heads
    size = (exact - inner) // 2
    seq, zero = lax.axis_size("seq"), lax.axis_size("zero")
    planes, pieces = seq // 4, seq // 2
    piece, tokens = owned // seq, zero * count
    levels = pieces.bit_length() - 1
    chunk = 512
    chunks = inner // chunk
    quarter = size // 4
    padded = -(-columns // 128) * 128
    edges = list(range(0, padded, 256)) + [padded]
    spans = list(zip(edges[:-1], edges[1:]))
    parts = len(spans)
    widths = [high - low for low, high in spans]
    tall = pltpu.VMEM((count, inner), F32)
    thin = pltpu.VMEM((count, inner), BF)
    block = pltpu.VMEM((chunks, 2, 2, 2, quarter, chunk), BF)
    half = pltpu.VMEM((chunks, 2, 2, quarter, chunk), BF)
    dma = pltpu.SemaphoreType.DMA
    slabs = 3 + -(-inner // 256)
    scratch = [
        thin,
        pltpu.VMEM((count, 2 * size), BF),
        pltpu.VMEM((zero - 1, count, owned), BF),
        pltpu.VMEM((count, columns), F32),
        pltpu.VMEM((zero - 1, count, exact), BF),
        pltpu.VMEM((zero - 1, count, 128), F32),
        pltpu.VMEM((zero - 1, count, exact), BF),
        pltpu.VMEM((zero - 1, count, 128), F32),
        dma((zero, slabs)),
        dma((zero, slabs)),
        pltpu.VMEM((heads, inner), F32),
        tall, tall, tall, thin, thin, thin, tall, tall,
        pltpu.VMEM((count, heads), F32),
        pltpu.VMEM((heads, count), F32),
        pltpu.VMEM((8, 128), F32),
        pltpu.VMEM((seq, 8, 128), F32),
        pltpu.VMEM((seq, inner), F32),
        block, block, half, half,
        pltpu.VMEM((chunks, 2, quarter, chunk), BF),
        pltpu.VMEM((chunks, 2, planes, quarter, chunk), BF),
        half, half, block, block,
        pltpu.VMEM((pieces, 2, zero, piece, count), BF),
        pltpu.VMEM((2, pieces, piece, tokens), BF),
        pltpu.VMEM((tokens, padded), BF),
        pltpu.VMEM(weights.shape, BF),
        pltpu.VMEM((zero - 1, count, owned), BF),
        dma((seq - 1,)), dma((seq - 1,)),
        dma((4, chunks)), dma((4, chunks)),
        dma((chunks, 2, planes)), dma((chunks, 2, planes)),
        dma((2, zero - 1)), dma((2, zero - 1)),
    ]
    scratch += [pltpu.VMEM((pieces, piece, w), F32) for w in widths]
    scratch += [pltpu.VMEM((pieces, piece, w), BF) for w in widths] * 2
    for _ in range(2):
        for w in widths:
            scratch += [pltpu.VMEM((pieces >> (s + 1), piece, w), BF) for s in range(levels)]
    scratch += [dma((parts, levels + 1))] * 2 + [dma((parts, zero))] * 2 + [dma((zero,))] * 2
    scratch += [dma]
    local = pl.BlockSpec(memory_space=pltpu.VMEM)
    return pl.pallas_call(
        functools.partial(core_kernel, inner // heads, chunk, LAGS, spans, min(256, owned)),
        out_shape=(
            jax.ShapeDtypeStruct((count, inner), BF),
            jax.ShapeDtypeStruct((piece, columns), F32),
            jax.ShapeDtypeStruct((count, zero * owned), BF),
        ),
        in_specs=[local, pl.BlockSpec(memory_space=pl.ANY)] + [local] * 4,
        out_specs=[local] * 3,
        scratch_shapes=scratch,
        compiler_params=pltpu.CompilerParams(collective_id=0, vmem_limit_bytes=VMEM, has_side_effects=True),
    )(rows, weights, gy, a_log[None], dt_bias[None], d_skip[None])


def per_device(tokens, w_in, a_log, dt_bias, d_skip, grad_y):
    count, width = tokens.shape[1:]
    inner = grad_y.shape[2]
    rows = tokens.reshape(count, width)

    y_out, grad_w, grad_tokens = layer(
        rows, w_in.T, grad_y.reshape(count, inner), a_log, dt_bias, d_skip
    )
    grad_tokens = grad_tokens.reshape(1, count, width)
    return (y_out.reshape(1, count, inner), grad_tokens, grad_w)


def solution(mesh):
    placed = (P("zero", "seq", None), P("zero", None), P(), P(), P(), P("zero", "seq", None))
    return jax.shard_map(
        per_device,
        mesh=mesh,
        in_specs=placed,
        out_specs=(P("zero", "seq", None), P("zero", "seq", None), P(("seq", "zero"), None)),
        check_vma=False,
    )
```

```python
import functools

import jax
import jax.numpy as jnp
from jax import lax
from jax.experimental import pallas as pl
from jax.experimental.pallas import tpu as pltpu
from jax.sharding import PartitionSpec as P

BF = jnp.bfloat16
VMEM = 50 << 20
F32 = jnp.float32
MESH = pl.DeviceIdType.MESH
LAGS = (0, 1, 2, 4, 5, 6)
SPACING = (3, 3)
SWAPPED = (0, 5)


def dot(a, b, dims):
    return lax.dot_general(a, b, (dims, ((), ())), preferred_element_type=F32)


def greet(peers, mates=()):
    barrier = pltpu.get_barrier_semaphore()
    for peer in peers:
        pl.semaphore_signal(barrier, inc=1, device_id={"seq": peer}, device_id_type=MESH)
    for mate in mates:
        pl.semaphore_signal(barrier, inc=1, device_id={"zero": mate}, device_id_type=MESH)
    pl.semaphore_wait(barrier, len(peers) + len(mates))


def remote(src, dst, send, recv, peer):
    return pltpu.make_async_remote_copy(
        src_ref=src,
        dst_ref=dst,
        send_sem=send,
        recv_sem=recv,
        device_id={"seq": peer},
        device_id_type=MESH,
    )


def mate(src, dst, send, recv, peer):
    return pltpu.make_async_remote_copy(
        src_ref=src,
        dst_ref=dst,
        send_sem=send,
        recv_sem=recv,
        device_id={"zero": peer},
        device_id_type=MESH,
    )


def core_kernel(
    width, chunk, lags, spans, tile,
    rows, stored, gy, a_log, dt_bias, d_skip, y_out, out, grads,
    xs, joined, guest, kept, shares, narrow, returned, thinned, hsend, hrecv, spread, dts, grows, fades, xds, growns, fadeds, ins, backs, cums, turned, mark, marks, gains,
    loc, both, pairs, duo, sums, far, ret, came, fin, wide, tall, left, right, weights, made,
    tsend, trecv, send, recv, zsend, zrecv, leave, enter, *scratch
):
    seq, planes = marks.shape[0], far.shape[2]
    zero = tall.shape[2]
    load = pltpu.make_async_copy(stored, weights, scratch[-1])
    load.start()
    me, here = lax.axis_index("seq"), lax.axis_index("zero")
    core, chip = lax.rem(me, 2), lax.div(me, 2)
    side, plane = lax.rem(chip, 2), lax.div(chip, 2)
    sibling, across = me + 1 - 2 * core, me + 2 - 4 * side
    peers = [lax.rem(me + d, seq) for d in range(1, seq)]
    after = [lax.rem(here + s, zero) for s in range(zero)]
    before = [lax.rem(here + zero - s, zero) for s in range(zero)]
    count, inner = xs.shape
    heads = a_log.shape[1]
    columns, owned = weights.shape
    exact = columns - heads
    size = joined.shape[1] // 2
    chunks = inner // chunk
    high = lax.Precision.HIGHEST
    far[...] = jnp.zeros(far.shape, BF)
    mark[...] = jnp.zeros(mark.shape, F32)
    narrow[...] = jnp.zeros(narrow.shape, F32)
    greet(peers, after[1:])

    def columns_of(z):
        return pl.ds(pl.multiple_of(z * owned, 128), owned)

    coming = []
    for s in range(1, zero):
        copy = mate(
            rows.at[:, columns_of(after[s])],
            guest.at[s - 1],
            hsend.at[s, 0],
            hrecv.at[s, 0],
            after[s],
        )
        copy.start()
        coming.append(copy)
    step = min(256, chunk)
    slabs = [(inner, exact)] + [(low, low + step) for low in range(0, inner, step)]
    load.wait()
    for low, top in slabs + [(exact, columns)]:
        kept[:, low:top] = dot(rows[:, columns_of(here)], weights[low:top], ((1,), (1,)))
    going = {}
    for s in range(1, zero):
        coming[s - 1].wait()
        narrow[s - 1, :, :heads] = dot(guest[s - 1], weights[exact:], ((1,), (1,)))
        going[s, -1] = mate(
            narrow.at[s - 1], thinned.at[s - 1], hsend.at[s, 1], hrecv.at[s, 1], before[s]
        )
        going[s, -1].start()
        for i, (low, top) in enumerate(slabs):
            shares[s - 1, :, low:top] = dot(guest[s - 1], weights[low:top], ((1,), (1,))).astype(BF)
            going[s, i] = mate(
                shares.at[s - 1, :, low:top],
                returned.at[s - 1, :, low:top],
                hsend.at[s, 2 + i],
                hrecv.at[s, 2 + i],
                before[s],
            )
            going[s, i].start()

    def slab(i):
        low, top = slabs[i]
        value = kept[:, low:top]
        for s in range(1, zero):
            going[s, i].wait()
            value = value + returned[s - 1, :, low:top].astype(F32)
        return value.astype(BF)

    def iota(shape, axis):
        return lax.broadcasted_iota(jnp.int32, shape, axis)

    lower = iota((count, count), 0) >= iota((count, count), 1)
    ones = lower.astype(F32)
    first = iota((heads, inner), 0) * width
    lane = iota((heads, inner), 1)
    spread[...] = ((lane >= first) & (lane < first + width)).astype(F32)
    rate, skip = -jnp.exp(a_log[...]), d_skip[...]
    raw = kept[:, exact:]
    for s in range(1, zero):
        going[s, -1].wait()
        raw = raw + thinned[s - 1, :, :heads]
    raw = raw + dt_bias[...]
    dt = jnp.maximum(raw, 0.0) + jnp.log1p(jnp.exp(-jnp.abs(raw)))
    cum = jnp.dot(ones, rate * dt, precision=high, preferred_element_type=F32)
    total = cum[count - 1 : count]
    cums[...] = cum
    turned[...] = cum.T
    mark[0:1, :heads] = total
    marks[me] = mark[...]
    told = [
        remote(mark, marks.at[me], tsend.at[d], trecv.at[d], peer) for d, peer in enumerate(peers)
    ]
    for copy in told:
        copy.start()
    growth, fade = jnp.exp(cum), jnp.exp(total - cum)
    joined[...] = slab(0)
    bm, cm = joined[:, :size], joined[:, size:]
    bt, ct = bm.T, cm.T
    skips = jnp.broadcast_to(skip, (8, heads))

    def expand(value, low, top):
        return jnp.dot(value, spread[:, low:top], precision=high, preferred_element_type=F32)

    def gather(value, low, top):
        return lax.dot_general(
            value, spread[:, low:top], (((1,), (1,)), ((), ())), precision=high,
            preferred_element_type=F32,
        )

    copies = {}

    def prepare(c):
        for low in range(c * chunk, (c + 1) * chunk, step):
            top = low + step
            own = slice(low - c * chunk, low - c * chunk + step)
            xs[:, low:top] = slab(1 + low // step)
            d, g, f = expand(dt, low, top), expand(growth, low, top), expand(fade, low, top)
            dts[:, low:top], grows[:, low:top], fades[:, low:top] = d, g, f
            xd = (xs[:, low:top].astype(F32) * d).astype(BF)
            grown = (gy[:, low:top].astype(F32) * g).astype(BF)
            faded = (xd.astype(F32) * f).astype(BF)
            xds[:, low:top], growns[:, low:top], fadeds[:, low:top] = xd, grown, faded
            parts = loc.shape[1:2] + loc.shape[3:5] + (step,)
            loc[c, :, 0, :, :, own] = dot(bt, faded, ((1,), (0,))).astype(BF).reshape(parts)
            loc[c, :, 1, :, :, own] = dot(ct, grown, ((1,), (0,))).astype(BF).reshape(parts)
        both[c, core] = loc[c, core]
        copies[0, c] = remote(
            loc.at[c, 1 - core], both.at[c, core], send.at[0, c], recv.at[0, c], sibling
        )
        copies[0, c].start()

    def gain(c, *rows):
        at = slice(c * chunk, (c + 1) * chunk)
        return jnp.exp(sum(gains[pl.ds(row, 1), at] for row in rows))

    def stage_pair(c):
        copies[0, c].wait()
        g0, g1 = gain(c, chip * 2), gain(c, chip * 2 + 1)
        for q in range(2):
            pairs[c, q, 0] = (
                g1 * both[c, 0, 0, q].astype(F32) + both[c, 1, 0, q].astype(F32)
            ).astype(BF)
            pairs[c, q, 1] = (
                g0 * both[c, 1, 1, q].astype(F32) + both[c, 0, 1, q].astype(F32)
            ).astype(BF)
        duo[c, side] = pairs[c, side]
        copies[1, c] = remote(
            pairs.at[c, 1 - side], duo.at[c, side], send.at[1, c], recv.at[1, c], across
        )
        copies[1, c].start()

    def along(c, way, d):
        return remote(
            sums.at[c, way],
            far.at[c, way, plane],
            zsend.at[c, way, d],
            zrecv.at[c, way, d],
            me + (4 * d if way == 0 else -4 * d),
        )

    def later(d, way):
        return plane + d < planes if way == 0 else plane >= d

    def stage_plane(c):
        copies[1, c].wait()
        g0 = gain(c, plane * 4, plane * 4 + 1)
        g1 = gain(c, plane * 4 + 2, plane * 4 + 3)
        sums[c, 0] = (g1 * duo[c, 0, 0].astype(F32) + duo[c, 1, 0].astype(F32)).astype(BF)
        sums[c, 1] = (g0 * duo[c, 1, 1].astype(F32) + duo[c, 0, 1].astype(F32)).astype(BF)
        for d in range(1, planes):
            for way in range(2):

                @pl.when(later(d, way))
                def _():
                    along(c, way, d).start()

    def stage_far(c):
        for d in range(1, planes):
            for way in range(2):

                @pl.when(later(d, 1 - way))
                def _():
                    along(c, way, d).wait_recv()

                @pl.when(later(d, way))
                def _():
                    along(c, way, d).wait_send()

        at = slice(c * chunk, (c + 1) * chunk)
        ends = []
        for way in range(2):
            run = jnp.zeros(far.shape[3:], F32)
            for k in range(planes) if way == 0 else reversed(range(planes)):
                inside = (k < plane if way == 0 else k > plane).astype(F32)
                whole = sum(gains[4 * k + i : 4 * k + i + 1, at] for i in range(4))
                run = jnp.exp(whole * inside) * run + far[c, way, k].astype(F32)
            ends.append(run)
        g0 = gain(c, plane * 4, plane * 4 + 1)
        g1 = gain(c, plane * 4 + 2, plane * 4 + 3)
        ret[c, 0, 0] = ends[0].astype(BF)
        ret[c, 1, 0] = (g0 * ends[0] + duo[c, 0, 0].astype(F32)).astype(BF)
        ret[c, 1, 1] = ends[1].astype(BF)
        ret[c, 0, 1] = (g1 * ends[1] + duo[c, 1, 1].astype(F32)).astype(BF)
        came[c, side] = ret[c, side]
        copies[2, c] = remote(
            ret.at[c, 1 - side], came.at[c, side], send.at[2, c], recv.at[2, c], across
        )
        copies[2, c].start()

    def stage_back(c):
        copies[2, c].wait()
        g0, g1 = gain(c, chip * 2), gain(c, chip * 2 + 1)
        for q in range(2):
            fin[c, 0, 0, q] = came[c, q, 0]
            fin[c, 1, 1, q] = came[c, q, 1]
            fin[c, 1, 0, q] = (
                g0 * came[c, q, 0].astype(F32) + both[c, 0, 0, q].astype(F32)
            ).astype(BF)
            fin[c, 0, 1, q] = (
                g1 * came[c, q, 1].astype(F32) + both[c, 1, 1, q].astype(F32)
            ).astype(BF)
        wide[c, core] = fin[c, core]
        copies[3, c] = remote(
            fin.at[c, 1 - core], wide.at[c, core], send.at[3, c], recv.at[3, c], sibling
        )
        copies[3, c].start()

    scores = dot(cm, bm, ((1,), (1,)))
    group = 128 // width
    state = {
        "mixed": jnp.zeros((count, count), F32),
        "c": jnp.zeros((count, size), F32),
        "b": jnp.zeros((count, size), F32),
        "log": jnp.zeros((count, heads), F32),
        "dt": jnp.zeros((count, heads), F32),
        "last": jnp.zeros((8, heads), F32),
    }
    place = iota((count, 128), 1)
    masks = [(place >= width * i) & (place < width * (i + 1)) for i in range(group)]

    def inside(p):
        low, top = p * 128, (p + 1) * 128
        x2, g2 = xds[:, low:top], gy[:, low:top]
        none = jnp.zeros_like(x2)
        decays = []
        for i in range(group):
            h = p * group + i
            spans = cums[:, h : h + 1] - turned[h : h + 1, :]
            decays.append(jnp.where(lower, jnp.exp(jnp.where(lower, spans, 0.0)), 0.0))
        mixing = jnp.concatenate([(scores * decay).astype(BF) for decay in decays], axis=1)
        stacked = jnp.concatenate([jnp.where(mask, x2, none) for mask in masks], axis=0)
        ins[:, low:top] = dot(mixing, stacked, ((1,), (0,)))
        tall = dot(mixing, g2, ((0,), (0,)))
        back = tall[:count]
        for i in range(1, group):
            back = jnp.where(masks[i], tall[i * count : (i + 1) * count], back)
        backs[:, low:top] = back
        lifted = jnp.concatenate([jnp.where(mask, g2, none) for mask in masks], axis=0)
        cross = dot(lifted, x2, ((1,), (1,)))
        for i in range(group):
            state["mixed"] += cross[i * count : (i + 1) * count] * decays[i]

    def finish(c):
        copies[3, c].wait()
        for low in range(c * chunk, (c + 1) * chunk, step):
            top = low + step
            own = slice(low - c * chunk, low - c * chunk + step)
            start = wide[c, :, 0, :, :, own].reshape(size, step)
            end = wide[c, :, 1, :, :, own].reshape(size, step)
            x, g = xs[:, low:top].astype(F32), gy[:, low:top].astype(F32)
            d, xd = dts[:, low:top], xds[:, low:top].astype(F32)
            reached = dot(bm, end, ((1,), (0,))) * fades[:, low:top]
            y3 = ins[:, low:top] + dot(cm, start, ((1,), (0,))) * grows[:, low:top]
            h3 = backs[:, low:top] + reached
            kept = expand(skips, low, top)[:1]
            y_out[:, low:top] = (y3 + kept * x).astype(BF)
            right[:count, low:top] = (h3 * d + kept * g).astype(BF)
            state["c"] += dot(growns[:, low:top], start, ((1,), (1,)))
            state["b"] += dot(fadeds[:, low:top], end, ((1,), (1,)))
            state["log"] += gather(g * y3 - xd * h3, low, top)
            state["dt"] += gather(x * h3, low, top)
            joint = jnp.sum(start.astype(F32) * end.astype(F32), axis=0, keepdims=True)
            joint = joint * jnp.exp(gains[pl.ds(me, 1), low:top])
            last = jnp.sum(xd * reached, axis=0, keepdims=True) + joint
            state["last"] += gather(jnp.broadcast_to(last, (8, step)), low, top)

    pieces, piece, tokens = left.shape[1:]
    levels = (seq // 2).bit_length() - 1
    bits = [lax.rem(lax.div(chip, 1 << b), 2) for b in range(levels)]
    partners = [me + (1 - 2 * bits[b]) * (2 << b) for b in range(levels)]
    parts = len(spans)
    up = list(range(levels))
    orders = [up[1:] + up[:1] if h in SWAPPED else up for h in range(parts)]
    acc, away, come = (scratch[i * parts : (i + 1) * parts] for i in range(3))
    rest = scratch[3 * parts : -7]
    outs = [rest[h * levels : (h + 1) * levels] for h in range(parts)]
    inns = [rest[(parts + h) * levels : (parts + h + 1) * levels] for h in range(parts)]
    dsend, drecv, put, got, back_send, back_recv = scratch[-7:-1]
    crossing = []

    def cross():
        for low in range(0, rows.shape[1], 128):
            block = rows[:, low : low + 128].astype(F32).T.reshape(128 // piece, piece, count)
            for i in range(128 // piece):
                q = low // piece + i
                tall[q // (2 * zero), q // zero % 2, q % zero] = block[i].astype(BF)
        for way in range(2):
            for s in range(1, zero):
                copy = mate(
                    tall.at[:, way, after[s]],
                    left.at[way, :, :, s * count : (s + 1) * count],
                    leave.at[way, s - 1],
                    enter.at[way, s - 1],
                    after[s],
                )
                copy.start()
                crossing.append(copy)
            left[way, :, :, :count] = tall[:, way, here]

    arriving = {}

    def ready(h):
        low, high = spans[h]
        arriving[h] = []
        for s in range(1, zero):
            copy = mate(
                right.at[:count, low:high],
                right.at[s * count : (s + 1) * count, low:high],
                put.at[h, s],
                got.at[h, s],
                after[s],
            )
            copy.start()
            arriving[h].append(copy)

    mine_at = pl.multiple_of(here * owned, 128)

    def project(values, target, origin):
        @pl.loop(0, owned // tile)
        def _(i):
            at = pl.multiple_of(i * tile, 128)
            value = dot(values[:, :columns], weights[:, pl.ds(at, tile)], ((1,), (0,)))
            target[:, pl.ds(pl.multiple_of(origin + at, 128), tile)] = value.astype(BF)


    def multiply(side, h, target):
        low, high = spans[h]
        lines = left[side].reshape(pieces * piece, tokens)
        value = jnp.dot(lines, right[:, low:high], preferred_element_type=F32)
        target[...] = value.reshape(target.shape).astype(target.dtype)

    pushed = []

    def front(h):
        for copy in arriving[h]:
            copy.wait()
        multiply(1 - core, h, away[h])
        copy = remote(away[h], come[h], dsend.at[h, levels], drecv.at[h, levels], sibling)
        copy.start()
        pushed.append(copy)
        multiply(core, h, acc[h])

    def join(h):
        pushed[h].wait()

        @pl.loop(0, pieces)
        def _(i):
            acc[h][i] += come[h][i].astype(F32)

    def subsets(rest):
        found = [0]
        for b in rest:
            found = found + [value + (1 << b) for value in found]
        return found

    flying = {}

    def begin(h, s):
        order = orders[h]
        b = order[s]
        base = sum((bits[f] * (1 << f) for f in order[:s]), 0)
        for j, extra in enumerate(subsets(order[s + 1 :])):
            outs[h][s][j] = acc[h][base + (1 - bits[b]) * (1 << b) + extra].astype(BF)
        copy = remote(outs[h][s], inns[h][s], dsend.at[h, s], drecv.at[h, s], partners[b])
        copy.start()
        flying[h] = copy

    def settle(h, s):
        flying[h].wait()
        order = orders[h]
        base = sum((bits[f] * (1 << f) for f in order[: s + 1]), 0)
        for j, extra in enumerate(subsets(order[s + 1 :])):
            acc[h][base + extra] += inns[h][s][j].astype(F32)

    lag, skew = SPACING
    returning = []

    def advance(k):
        if k < parts:
            front(k)
        if 1 <= k <= parts:
            join(k - 1)
            begin(k - 1, 0)
        if k == parts:
            for s in range(1, zero):
                project(right.at[s * count : (s + 1) * count], made.at[s - 1], 0)
                copy = mate(
                    made.at[s - 1],
                    grads.at[:, pl.ds(mine_at, owned)],
                    back_send.at[s],
                    back_recv.at[s],
                    before[s],
                )
                copy.start()
                returning.append(copy)
            project(right.at[:count], grads, mine_at)
        for s in reversed(range(levels)):
            h = k - lag - skew * s
            if 0 <= h < parts:
                settle(h, s)
                if s + 1 < levels:
                    begin(h, s + 1)
                else:
                    low, high = spans[h][0], min(spans[h][1], columns)
                    out[:, low:high] = acc[h][chip, :, : high - low]

    def spread_totals():
        for copy in told:
            copy.wait()
        totals = marks[:, 0, :heads]
        for low in range(0, inner, step):
            gains[:, low : low + step] = expand(totals, low, low + step)

    stages = [prepare, stage_pair, stage_plane, stage_far, stage_back, finish]
    steps = chunks + lags[-1]
    fillers = list(range(inner // 128))
    per = -(-len(fillers) // lags[-1])
    moved = 0
    for k in range(steps):
        for lagging, stage in reversed(list(zip(lags, stages))):
            c = k - lagging
            if 0 <= c < chunks:
                if stage is finish:
                    while fillers and fillers[0] * 128 < (c + 1) * chunk:
                        inside(fillers.pop(0))
                if stage is stage_pair and c == 0:
                    spread_totals()
                stage(c)
                if stage is finish:
                    for h in range(parts):
                        if c * chunk <= spans[h][0] < (c + 1) * chunk:
                            ready(h)
        if k == 0:
            cross()
        for _ in range(per):
            if fillers and fillers[0] * 128 < (k + 1) * chunk:
                inside(fillers.pop(0))
        if k == lags[-1] + 1:
            for copy in crossing:
                copy.wait()
        if k > lags[-1]:
            while spans[moved][0] < (k - lags[-1]) * chunk:
                advance(moved)
                moved += 1

    mixed = state["mixed"].astype(BF)
    right[:count, inner : inner + size] = (dot(mixed, cm, ((0,), (0,))) + state["b"]).astype(BF)
    right[:count, inner + size : inner + 2 * size] = (
        dot(mixed, bm, ((1,), (0,))) + state["c"]
    ).astype(BF)
    upper = (iota((count, count), 0) <= iota((count, count), 1)).astype(F32)
    grad_log = jnp.dot(upper, state["log"], precision=high, preferred_element_type=F32)
    grad_log = grad_log + state["last"][:1]
    grad_raw = (state["dt"] + grad_log * rate) * jax.nn.sigmoid(raw)
    edge = inner + 2 * size
    right[:count, edge:] = jnp.zeros((count, right.shape[1] - edge), BF)
    right[:count, edge : edge + heads] = grad_raw.astype(BF)
    for h in range(parts):
        if spans[h][0] >= inner:
            ready(h)
    for k in range(moved, parts + lag + skew * levels):
        advance(k)
    for copy in returning:
        copy.wait()


def layer(rows, weights, gy, a_log, dt_bias, d_skip):
    count, inner = gy.shape
    heads = a_log.shape[0]
    columns, owned = weights.shape
    exact = columns - heads
    size = (exact - inner) // 2
    seq, zero = lax.axis_size("seq"), lax.axis_size("zero")
    planes, pieces = seq // 4, seq // 2
    piece, tokens = owned // seq, zero * count
    levels = pieces.bit_length() - 1
    chunk = 512
    chunks = inner // chunk
    quarter = size // 4
    padded = -(-columns // 128) * 128
    edges = list(range(0, padded, 256)) + [padded]
    spans = list(zip(edges[:-1], edges[1:]))
    parts = len(spans)
    widths = [high - low for low, high in spans]
    tall = pltpu.VMEM((count, inner), F32)
    thin = pltpu.VMEM((count, inner), BF)
    block = pltpu.VMEM((chunks, 2, 2, 2, quarter, chunk), BF)
    half = pltpu.VMEM((chunks, 2, 2, quarter, chunk), BF)
    dma = pltpu.SemaphoreType.DMA
    slabs = 3 + -(-inner // 256)
    scratch = [
        thin,
        pltpu.VMEM((count, 2 * size), BF),
        pltpu.VMEM((zero - 1, count, owned), BF),
        pltpu.VMEM((count, columns), F32),
        pltpu.VMEM((zero - 1, count, exact), BF),
        pltpu.VMEM((zero - 1, count, 128), F32),
        pltpu.VMEM((zero - 1, count, exact), BF),
        pltpu.VMEM((zero - 1, count, 128), F32),
        dma((zero, slabs)),
        dma((zero, slabs)),
        pltpu.VMEM((heads, inner), F32),
        tall, tall, tall, thin, thin, thin, tall, tall,
        pltpu.VMEM((count, heads), F32),
        pltpu.VMEM((heads, count), F32),
        pltpu.VMEM((8, 128), F32),
        pltpu.VMEM((seq, 8, 128), F32),
        pltpu.VMEM((seq, inner), F32),
        block, block, half, half,
        pltpu.VMEM((chunks, 2, quarter, chunk), BF),
        pltpu.VMEM((chunks, 2, planes, quarter, chunk), BF),
        half, half, block, block,
        pltpu.VMEM((pieces, 2, zero, piece, count), BF),
        pltpu.VMEM((2, pieces, piece, tokens), BF),
        pltpu.VMEM((tokens, padded), BF),
        pltpu.VMEM(weights.shape, BF),
        pltpu.VMEM((zero - 1, count, owned), BF),
        dma((seq - 1,)), dma((seq - 1,)),
        dma((4, chunks)), dma((4, chunks)),
        dma((chunks, 2, planes)), dma((chunks, 2, planes)),
        dma((2, zero - 1)), dma((2, zero - 1)),
    ]
    scratch += [pltpu.VMEM((pieces, piece, w), F32) for w in widths]
    scratch += [pltpu.VMEM((pieces, piece, w), BF) for w in widths] * 2
    for _ in range(2):
        for w in widths:
            scratch += [pltpu.VMEM((pieces >> (s + 1), piece, w), BF) for s in range(levels)]
    scratch += [dma((parts, levels + 1))] * 2 + [dma((parts, zero))] * 2 + [dma((zero,))] * 2
    scratch += [dma]
    local = pl.BlockSpec(memory_space=pltpu.VMEM)
    return pl.pallas_call(
        functools.partial(core_kernel, inner // heads, chunk, LAGS, spans, min(256, owned)),
        out_shape=(
            jax.ShapeDtypeStruct((count, inner), BF),
            jax.ShapeDtypeStruct((piece, columns), F32),
            jax.ShapeDtypeStruct((count, zero * owned), BF),
        ),
        in_specs=[local, pl.BlockSpec(memory_space=pl.ANY)] + [local] * 4,
        out_specs=[local] * 3,
        scratch_shapes=scratch,
        compiler_params=pltpu.CompilerParams(collective_id=0, vmem_limit_bytes=VMEM, has_side_effects=True),
    )(rows, weights, gy, a_log[None], dt_bias[None], d_skip[None])


def per_device(tokens, w_in, a_log, dt_bias, d_skip, grad_y):
    count, width = tokens.shape[1:]
    inner = grad_y.shape[2]
    rows = tokens.reshape(count, width)

    y_out, grad_w, grad_tokens = layer(
        rows, w_in.T, grad_y.reshape(count, inner), a_log, dt_bias, d_skip
    )
    grad_tokens = grad_tokens.reshape(1, count, width)
    return (y_out.reshape(1, count, inner), grad_tokens, grad_w)


def solution(mesh):
    placed = (P("zero", "seq", None), P("zero", None), P(), P(), P(), P("zero", "seq", None))
    return jax.shard_map(
        per_device,
        mesh=mesh,
        in_specs=placed,
        out_specs=(P("zero", "seq", None), P("zero", "seq", None), P(("seq", "zero"), None)),
        check_vma=False,
    )
```

```python
import functools

import jax
import jax.numpy as jnp
from jax import lax
from jax.experimental import pallas as pl
from jax.experimental.pallas import tpu as pltpu
from jax.sharding import PartitionSpec as P

BF = jnp.bfloat16
VMEM = 50 << 20
F32 = jnp.float32
MESH = pl.DeviceIdType.MESH
LAGS = (0, 1, 2, 4, 5, 6)
SPACING = (3, 4)
SWAPPED = (0, 5)


def dot(a, b, dims):
    return lax.dot_general(a, b, (dims, ((), ())), preferred_element_type=F32)


def greet(peers, mates=()):
    barrier = pltpu.get_barrier_semaphore()
    for peer in peers:
        pl.semaphore_signal(barrier, inc=1, device_id={"seq": peer}, device_id_type=MESH)
    for mate in mates:
        pl.semaphore_signal(barrier, inc=1, device_id={"zero": mate}, device_id_type=MESH)
    pl.semaphore_wait(barrier, len(peers) + len(mates))


def remote(src, dst, send, recv, peer):
    return pltpu.make_async_remote_copy(
        src_ref=src,
        dst_ref=dst,
        send_sem=send,
        recv_sem=recv,
        device_id={"seq": peer},
        device_id_type=MESH,
    )


def mate(src, dst, send, recv, peer):
    return pltpu.make_async_remote_copy(
        src_ref=src,
        dst_ref=dst,
        send_sem=send,
        recv_sem=recv,
        device_id={"zero": peer},
        device_id_type=MESH,
    )


def core_kernel(
    width, chunk, lags, spans, tile,
    far_rows, stored, far_gy, far_a, far_bias, far_skip, y_out, out, grads,
    rows, gy, a_log, dt_bias, d_skip, fetched, xs, joined, guest, kept, shares, narrow, returned, thinned, hsend, hrecv, spread, dts, grows, fades, xds, growns, fadeds, ins, backs, cums, turned, mark, marks, gains,
    loc, both, pairs, duo, sums, far, ret, came, fin, wide, tall, left, right, weights, made,
    tsend, trecv, send, recv, zsend, zrecv, leave, enter, *scratch
):
    seq, planes = marks.shape[0], far.shape[2]
    zero = tall.shape[2]
    load = pltpu.make_async_copy(stored, weights, scratch[-1])
    fetches = [
        pltpu.make_async_copy(source, target, fetched.at[i])
        for i, (source, target) in enumerate(
            [(far_rows, rows), (far_gy, gy), (far_a, a_log), (far_bias, dt_bias), (far_skip, d_skip)]
        )
    ]
    for copy in fetches:
        copy.start()
    load.start()
    me, here = lax.axis_index("seq"), lax.axis_index("zero")
    core, chip = lax.rem(me, 2), lax.div(me, 2)
    side, plane = lax.rem(chip, 2), lax.div(chip, 2)
    sibling, across = me + 1 - 2 * core, me + 2 - 4 * side
    peers = [lax.rem(me + d, seq) for d in range(1, seq)]
    after = [lax.rem(here + s, zero) for s in range(zero)]
    before = [lax.rem(here + zero - s, zero) for s in range(zero)]
    count, inner = xs.shape
    heads = a_log.shape[1]
    columns, owned = weights.shape
    exact = columns - heads
    size = joined.shape[1] // 2
    chunks = inner // chunk
    high = lax.Precision.HIGHEST
    far[...] = jnp.zeros(far.shape, BF)
    mark[...] = jnp.zeros(mark.shape, F32)
    narrow[...] = jnp.zeros(narrow.shape, F32)
    greet(peers, after[1:])
    for copy in fetches:
        copy.wait()

    def columns_of(z):
        return pl.ds(pl.multiple_of(z * owned, 128), owned)

    coming = []
    for s in range(1, zero):
        copy = mate(
            rows.at[:, columns_of(after[s])],
            guest.at[s - 1],
            hsend.at[s, 0],
            hrecv.at[s, 0],
            after[s],
        )
        copy.start()
        coming.append(copy)
    step = min(256, chunk)
    slabs = [(inner, exact)] + [(low, low + step) for low in range(0, inner, step)]
    load.wait()
    for low, top in slabs + [(exact, columns)]:
        kept[:, low:top] = dot(rows[:, columns_of(here)], weights[low:top], ((1,), (1,)))
    going = {}
    for s in range(1, zero):
        coming[s - 1].wait()
        narrow[s - 1, :, :heads] = dot(guest[s - 1], weights[exact:], ((1,), (1,)))
        going[s, -1] = mate(
            narrow.at[s - 1], thinned.at[s - 1], hsend.at[s, 1], hrecv.at[s, 1], before[s]
        )
        going[s, -1].start()
        for i, (low, top) in enumerate(slabs):
            shares[s - 1, :, low:top] = dot(guest[s - 1], weights[low:top], ((1,), (1,))).astype(BF)
            going[s, i] = mate(
                shares.at[s - 1, :, low:top],
                returned.at[s - 1, :, low:top],
                hsend.at[s, 2 + i],
                hrecv.at[s, 2 + i],
                before[s],
            )
            going[s, i].start()

    def slab(i):
        low, top = slabs[i]
        value = kept[:, low:top]
        for s in range(1, zero):
            going[s, i].wait()
            value = value + returned[s - 1, :, low:top].astype(F32)
        return value.astype(BF)

    def iota(shape, axis):
        return lax.broadcasted_iota(jnp.int32, shape, axis)

    lower = iota((count, count), 0) >= iota((count, count), 1)
    ones = lower.astype(F32)
    first = iota((heads, inner), 0) * width
    lane = iota((heads, inner), 1)
    spread[...] = ((lane >= first) & (lane < first + width)).astype(F32)
    rate, skip = -jnp.exp(a_log[...]), d_skip[...]
    raw = kept[:, exact:]
    for s in range(1, zero):
        going[s, -1].wait()
        raw = raw + thinned[s - 1, :, :heads]
    raw = raw + dt_bias[...]
    dt = jnp.maximum(raw, 0.0) + jnp.log1p(jnp.exp(-jnp.abs(raw)))
    cum = jnp.dot(ones, rate * dt, precision=high, preferred_element_type=F32)
    total = cum[count - 1 : count]
    cums[...] = cum
    turned[...] = cum.T
    mark[0:1, :heads] = total
    marks[me] = mark[...]
    told = [
        remote(mark, marks.at[me], tsend.at[d], trecv.at[d], peer) for d, peer in enumerate(peers)
    ]
    for copy in told:
        copy.start()
    growth, fade = jnp.exp(cum), jnp.exp(total - cum)
    joined[...] = slab(0)
    bm, cm = joined[:, :size], joined[:, size:]
    bt, ct = bm.T, cm.T
    skips = jnp.broadcast_to(skip, (8, heads))

    def expand(value, low, top):
        return jnp.dot(value, spread[:, low:top], precision=high, preferred_element_type=F32)

    def gather(value, low, top):
        return lax.dot_general(
            value, spread[:, low:top], (((1,), (1,)), ((), ())), precision=high,
            preferred_element_type=F32,
        )

    copies = {}

    def prepare(c):
        for low in range(c * chunk, (c + 1) * chunk, step):
            top = low + step
            own = slice(low - c * chunk, low - c * chunk + step)
            xs[:, low:top] = slab(1 + low // step)
            d, g, f = expand(dt, low, top), expand(growth, low, top), expand(fade, low, top)
            dts[:, low:top], grows[:, low:top], fades[:, low:top] = d, g, f
            xd = (xs[:, low:top].astype(F32) * d).astype(BF)
            grown = (gy[:, low:top].astype(F32) * g).astype(BF)
            faded = (xd.astype(F32) * f).astype(BF)
            xds[:, low:top], growns[:, low:top], fadeds[:, low:top] = xd, grown, faded
            parts = loc.shape[1:2] + loc.shape[3:5] + (step,)
            loc[c, :, 0, :, :, own] = dot(bt, faded, ((1,), (0,))).astype(BF).reshape(parts)
            loc[c, :, 1, :, :, own] = dot(ct, grown, ((1,), (0,))).astype(BF).reshape(parts)
        both[c, core] = loc[c, core]
        copies[0, c] = remote(
            loc.at[c, 1 - core], both.at[c, core], send.at[0, c], recv.at[0, c], sibling
        )
        copies[0, c].start()

    def gain(c, *rows):
        at = slice(c * chunk, (c + 1) * chunk)
        return jnp.exp(sum(gains[pl.ds(row, 1), at] for row in rows))

    def stage_pair(c):
        copies[0, c].wait()
        g0, g1 = gain(c, chip * 2), gain(c, chip * 2 + 1)
        for q in range(2):
            pairs[c, q, 0] = (
                g1 * both[c, 0, 0, q].astype(F32) + both[c, 1, 0, q].astype(F32)
            ).astype(BF)
            pairs[c, q, 1] = (
                g0 * both[c, 1, 1, q].astype(F32) + both[c, 0, 1, q].astype(F32)
            ).astype(BF)
        duo[c, side] = pairs[c, side]
        copies[1, c] = remote(
            pairs.at[c, 1 - side], duo.at[c, side], send.at[1, c], recv.at[1, c], across
        )
        copies[1, c].start()

    def along(c, way, d):
        return remote(
            sums.at[c, way],
            far.at[c, way, plane],
            zsend.at[c, way, d],
            zrecv.at[c, way, d],
            me + (4 * d if way == 0 else -4 * d),
        )

    def later(d, way):
        return plane + d < planes if way == 0 else plane >= d

    def stage_plane(c):
        copies[1, c].wait()
        g0 = gain(c, plane * 4, plane * 4 + 1)
        g1 = gain(c, plane * 4 + 2, plane * 4 + 3)
        sums[c, 0] = (g1 * duo[c, 0, 0].astype(F32) + duo[c, 1, 0].astype(F32)).astype(BF)
        sums[c, 1] = (g0 * duo[c, 1, 1].astype(F32) + duo[c, 0, 1].astype(F32)).astype(BF)
        for d in range(1, planes):
            for way in range(2):

                @pl.when(later(d, way))
                def _():
                    along(c, way, d).start()

    def stage_far(c):
        for d in range(1, planes):
            for way in range(2):

                @pl.when(later(d, 1 - way))
                def _():
                    along(c, way, d).wait_recv()

                @pl.when(later(d, way))
                def _():
                    along(c, way, d).wait_send()

        at = slice(c * chunk, (c + 1) * chunk)
        ends = []
        for way in range(2):
            run = jnp.zeros(far.shape[3:], F32)
            for k in range(planes) if way == 0 else reversed(range(planes)):
                inside = (k < plane if way == 0 else k > plane).astype(F32)
                whole = sum(gains[4 * k + i : 4 * k + i + 1, at] for i in range(4))
                run = jnp.exp(whole * inside) * run + far[c, way, k].astype(F32)
            ends.append(run)
        g0 = gain(c, plane * 4, plane * 4 + 1)
        g1 = gain(c, plane * 4 + 2, plane * 4 + 3)
        ret[c, 0, 0] = ends[0].astype(BF)
        ret[c, 1, 0] = (g0 * ends[0] + duo[c, 0, 0].astype(F32)).astype(BF)
        ret[c, 1, 1] = ends[1].astype(BF)
        ret[c, 0, 1] = (g1 * ends[1] + duo[c, 1, 1].astype(F32)).astype(BF)
        came[c, side] = ret[c, side]
        copies[2, c] = remote(
            ret.at[c, 1 - side], came.at[c, side], send.at[2, c], recv.at[2, c], across
        )
        copies[2, c].start()

    def stage_back(c):
        copies[2, c].wait()
        g0, g1 = gain(c, chip * 2), gain(c, chip * 2 + 1)
        for q in range(2):
            fin[c, 0, 0, q] = came[c, q, 0]
            fin[c, 1, 1, q] = came[c, q, 1]
            fin[c, 1, 0, q] = (
                g0 * came[c, q, 0].astype(F32) + both[c, 0, 0, q].astype(F32)
            ).astype(BF)
            fin[c, 0, 1, q] = (
                g1 * came[c, q, 1].astype(F32) + both[c, 1, 1, q].astype(F32)
            ).astype(BF)
        wide[c, core] = fin[c, core]
        copies[3, c] = remote(
            fin.at[c, 1 - core], wide.at[c, core], send.at[3, c], recv.at[3, c], sibling
        )
        copies[3, c].start()

    scores = dot(cm, bm, ((1,), (1,)))
    group = 128 // width
    state = {
        "mixed": jnp.zeros((count, count), F32),
        "c": jnp.zeros((count, size), F32),
        "b": jnp.zeros((count, size), F32),
        "log": jnp.zeros((count, heads), F32),
        "dt": jnp.zeros((count, heads), F32),
        "last": jnp.zeros((8, heads), F32),
    }
    place = iota((count, 128), 1)
    masks = [(place >= width * i) & (place < width * (i + 1)) for i in range(group)]

    def inside(p):
        low, top = p * 128, (p + 1) * 128
        x2, g2 = xds[:, low:top], gy[:, low:top]
        none = jnp.zeros_like(x2)
        decays = []
        for i in range(group):
            h = p * group + i
            spans = cums[:, h : h + 1] - turned[h : h + 1, :]
            decays.append(jnp.where(lower, jnp.exp(jnp.where(lower, spans, 0.0)), 0.0))
        mixing = jnp.concatenate([(scores * decay).astype(BF) for decay in decays], axis=1)
        stacked = jnp.concatenate([jnp.where(mask, x2, none) for mask in masks], axis=0)
        ins[:, low:top] = dot(mixing, stacked, ((1,), (0,)))
        tall = dot(mixing, g2, ((0,), (0,)))
        back = tall[:count]
        for i in range(1, group):
            back = jnp.where(masks[i], tall[i * count : (i + 1) * count], back)
        backs[:, low:top] = back
        lifted = jnp.concatenate([jnp.where(mask, g2, none) for mask in masks], axis=0)
        cross = dot(lifted, x2, ((1,), (1,)))
        for i in range(group):
            state["mixed"] += cross[i * count : (i + 1) * count] * decays[i]

    def finish(c):
        copies[3, c].wait()
        for low in range(c * chunk, (c + 1) * chunk, step):
            top = low + step
            own = slice(low - c * chunk, low - c * chunk + step)
            start = wide[c, :, 0, :, :, own].reshape(size, step)
            end = wide[c, :, 1, :, :, own].reshape(size, step)
            x, g = xs[:, low:top].astype(F32), gy[:, low:top].astype(F32)
            d, xd = dts[:, low:top], xds[:, low:top].astype(F32)
            reached = dot(bm, end, ((1,), (0,))) * fades[:, low:top]
            y3 = ins[:, low:top] + dot(cm, start, ((1,), (0,))) * grows[:, low:top]
            h3 = backs[:, low:top] + reached
            kept = expand(skips, low, top)[:1]
            y_out[:, low:top] = (y3 + kept * x).astype(BF)
            right[:count, low:top] = (h3 * d + kept * g).astype(BF)
            state["c"] += dot(growns[:, low:top], start, ((1,), (1,)))
            state["b"] += dot(fadeds[:, low:top], end, ((1,), (1,)))
            state["log"] += gather(g * y3 - xd * h3, low, top)
            state["dt"] += gather(x * h3, low, top)
            joint = jnp.sum(start.astype(F32) * end.astype(F32), axis=0, keepdims=True)
            joint = joint * jnp.exp(gains[pl.ds(me, 1), low:top])
            last = jnp.sum(xd * reached, axis=0, keepdims=True) + joint
            state["last"] += gather(jnp.broadcast_to(last, (8, step)), low, top)

    pieces, piece, tokens = left.shape[1:]
    levels = (seq // 2).bit_length() - 1
    bits = [lax.rem(lax.div(chip, 1 << b), 2) for b in range(levels)]
    partners = [me + (1 - 2 * bits[b]) * (2 << b) for b in range(levels)]
    parts = len(spans)
    up = list(range(levels))
    orders = [up[1:] + up[:1] if h in SWAPPED else up for h in range(parts)]
    acc, away, come = (scratch[i * parts : (i + 1) * parts] for i in range(3))
    rest = scratch[3 * parts : -7]
    outs = [rest[h * levels : (h + 1) * levels] for h in range(parts)]
    inns = [rest[(parts + h) * levels : (parts + h + 1) * levels] for h in range(parts)]
    dsend, drecv, put, got, back_send, back_recv = scratch[-7:-1]
    crossing = []

    def cross():
        for low in range(0, rows.shape[1], 128):
            block = rows[:, low : low + 128].astype(F32).T.reshape(128 // piece, piece, count)
            for i in range(128 // piece):
                q = low // piece + i
                tall[q // (2 * zero), q // zero % 2, q % zero] = block[i].astype(BF)
        for way in range(2):
            for s in range(1, zero):
                copy = mate(
                    tall.at[:, way, after[s]],
                    left.at[way, :, :, s * count : (s + 1) * count],
                    leave.at[way, s - 1],
                    enter.at[way, s - 1],
                    after[s],
                )
                copy.start()
                crossing.append(copy)
            left[way, :, :, :count] = tall[:, way, here]

    arriving = {}

    def ready(h):
        low, high = spans[h]
        arriving[h] = []
        for s in range(1, zero):
            copy = mate(
                right.at[:count, low:high],
                right.at[s * count : (s + 1) * count, low:high],
                put.at[h, s],
                got.at[h, s],
                after[s],
            )
            copy.start()
            arriving[h].append(copy)

    mine_at = pl.multiple_of(here * owned, 128)

    def project(values, target, origin):
        @pl.loop(0, owned // tile)
        def _(i):
            at = pl.multiple_of(i * tile, 128)
            value = dot(values[:, :columns], weights[:, pl.ds(at, tile)], ((1,), (0,)))
            target[:, pl.ds(pl.multiple_of(origin + at, 128), tile)] = value.astype(BF)


    def multiply(side, h, target):
        low, high = spans[h]
        lines = left[side].reshape(pieces * piece, tokens)
        value = jnp.dot(lines, right[:, low:high], preferred_element_type=F32)
        target[...] = value.reshape(target.shape).astype(target.dtype)

    pushed = []

    def front(h):
        for copy in arriving[h]:
            copy.wait()
        multiply(1 - core, h, away[h])
        copy = remote(away[h], come[h], dsend.at[h, levels], drecv.at[h, levels], sibling)
        copy.start()
        pushed.append(copy)
        multiply(core, h, acc[h])

    def join(h):
        pushed[h].wait()

        @pl.loop(0, pieces)
        def _(i):
            acc[h][i] += come[h][i].astype(F32)

    def subsets(rest):
        found = [0]
        for b in rest:
            found = found + [value + (1 << b) for value in found]
        return found

    flying = {}

    def begin(h, s):
        order = orders[h]
        b = order[s]
        base = sum((bits[f] * (1 << f) for f in order[:s]), 0)
        for j, extra in enumerate(subsets(order[s + 1 :])):
            outs[h][s][j] = acc[h][base + (1 - bits[b]) * (1 << b) + extra].astype(BF)
        copy = remote(outs[h][s], inns[h][s], dsend.at[h, s], drecv.at[h, s], partners[b])
        copy.start()
        flying[h] = copy

    def settle(h, s):
        flying[h].wait()
        order = orders[h]
        base = sum((bits[f] * (1 << f) for f in order[: s + 1]), 0)
        for j, extra in enumerate(subsets(order[s + 1 :])):
            acc[h][base + extra] += inns[h][s][j].astype(F32)

    lag, skew = SPACING
    returning = []

    def advance(k):
        if k < parts:
            front(k)
        if 1 <= k <= parts:
            join(k - 1)
            begin(k - 1, 0)
        if k == parts:
            for s in range(1, zero):
                project(right.at[s * count : (s + 1) * count], made.at[s - 1], 0)
                copy = mate(
                    made.at[s - 1],
                    grads.at[:, pl.ds(mine_at, owned)],
                    back_send.at[s],
                    back_recv.at[s],
                    before[s],
                )
                copy.start()
                returning.append(copy)
            project(right.at[:count], grads, mine_at)
        for s in reversed(range(levels)):
            h = k - lag - skew * s
            if 0 <= h < parts:
                settle(h, s)
                if s + 1 < levels:
                    begin(h, s + 1)
                else:
                    low, high = spans[h][0], min(spans[h][1], columns)
                    out[:, low:high] = acc[h][chip, :, : high - low]

    def spread_totals():
        for copy in told:
            copy.wait()
        totals = marks[:, 0, :heads]
        for low in range(0, inner, step):
            gains[:, low : low + step] = expand(totals, low, low + step)

    stages = [prepare, stage_pair, stage_plane, stage_far, stage_back, finish]
    steps = chunks + lags[-1]
    fillers = list(range(inner // 128))
    per = -(-len(fillers) // lags[-1])
    moved = 0
    for k in range(steps):
        for lagging, stage in reversed(list(zip(lags, stages))):
            c = k - lagging
            if 0 <= c < chunks:
                if stage is finish:
                    while fillers and fillers[0] * 128 < (c + 1) * chunk:
                        inside(fillers.pop(0))
                if stage is stage_pair and c == 0:
                    spread_totals()
                stage(c)
                if stage is finish:
                    for h in range(parts):
                        if c * chunk <= spans[h][0] < (c + 1) * chunk:
                            ready(h)
        if k == 0:
            cross()
        for _ in range(per):
            if fillers and fillers[0] * 128 < (k + 1) * chunk:
                inside(fillers.pop(0))
        if k == lags[-1] + 1:
            for copy in crossing:
                copy.wait()
        if k > lags[-1]:
            while spans[moved][0] < (k - lags[-1]) * chunk:
                advance(moved)
                moved += 1

    mixed = state["mixed"].astype(BF)
    right[:count, inner : inner + size] = (dot(mixed, cm, ((0,), (0,))) + state["b"]).astype(BF)
    right[:count, inner + size : inner + 2 * size] = (
        dot(mixed, bm, ((1,), (0,))) + state["c"]
    ).astype(BF)
    upper = (iota((count, count), 0) <= iota((count, count), 1)).astype(F32)
    grad_log = jnp.dot(upper, state["log"], precision=high, preferred_element_type=F32)
    grad_log = grad_log + state["last"][:1]
    grad_raw = (state["dt"] + grad_log * rate) * jax.nn.sigmoid(raw)
    edge = inner + 2 * size
    right[:count, edge:] = jnp.zeros((count, right.shape[1] - edge), BF)
    right[:count, edge : edge + heads] = grad_raw.astype(BF)
    for h in range(parts):
        if spans[h][0] >= inner:
            ready(h)
    for k in range(moved, parts + lag + skew * levels):
        advance(k)
    for copy in returning:
        copy.wait()


def layer(rows, weights, gy, a_log, dt_bias, d_skip):
    count, inner = gy.shape
    heads = a_log.shape[0]
    columns, owned = weights.shape
    exact = columns - heads
    size = (exact - inner) // 2
    seq, zero = lax.axis_size("seq"), lax.axis_size("zero")
    planes, pieces = seq // 4, seq // 2
    piece, tokens = owned // seq, zero * count
    levels = pieces.bit_length() - 1
    chunk = 512
    chunks = inner // chunk
    quarter = size // 4
    padded = -(-columns // 128) * 128
    edges = list(range(0, padded, 256)) + [padded]
    spans = list(zip(edges[:-1], edges[1:]))
    parts = len(spans)
    widths = [high - low for low, high in spans]
    tall = pltpu.VMEM((count, inner), F32)
    thin = pltpu.VMEM((count, inner), BF)
    block = pltpu.VMEM((chunks, 2, 2, 2, quarter, chunk), BF)
    half = pltpu.VMEM((chunks, 2, 2, quarter, chunk), BF)
    dma = pltpu.SemaphoreType.DMA
    slabs = 3 + -(-inner // 256)
    scalar = pltpu.VMEM((1, heads), F32)
    scratch = [
        pltpu.VMEM(rows.shape, BF),
        thin,
        scalar,
        scalar,
        scalar,
        dma((5,)),
        thin,
        pltpu.VMEM((count, 2 * size), BF),
        pltpu.VMEM((zero - 1, count, owned), BF),
        pltpu.VMEM((count, columns), F32),
        pltpu.VMEM((zero - 1, count, exact), BF),
        pltpu.VMEM((zero - 1, count, 128), F32),
        pltpu.VMEM((zero - 1, count, exact), BF),
        pltpu.VMEM((zero - 1, count, 128), F32),
        dma((zero, slabs)),
        dma((zero, slabs)),
        pltpu.VMEM((heads, inner), F32),
        tall, tall, tall, thin, thin, thin, tall, tall,
        pltpu.VMEM((count, heads), F32),
        pltpu.VMEM((heads, count), F32),
        pltpu.VMEM((8, 128), F32),
        pltpu.VMEM((seq, 8, 128), F32),
        pltpu.VMEM((seq, inner), F32),
        block, block, half, half,
        pltpu.VMEM((chunks, 2, quarter, chunk), BF),
        pltpu.VMEM((chunks, 2, planes, quarter, chunk), BF),
        half, half, block, block,
        pltpu.VMEM((pieces, 2, zero, piece, count), BF),
        pltpu.VMEM((2, pieces, piece, tokens), BF),
        pltpu.VMEM((tokens, padded), BF),
        pltpu.VMEM(weights.shape, BF),
        pltpu.VMEM((zero - 1, count, owned), BF),
        dma((seq - 1,)), dma((seq - 1,)),
        dma((4, chunks)), dma((4, chunks)),
        dma((chunks, 2, planes)), dma((chunks, 2, planes)),
        dma((2, zero - 1)), dma((2, zero - 1)),
    ]
    scratch += [pltpu.VMEM((pieces, piece, w), F32) for w in widths]
    scratch += [pltpu.VMEM((pieces, piece, w), BF) for w in widths] * 2
    for _ in range(2):
        for w in widths:
            scratch += [pltpu.VMEM((pieces >> (s + 1), piece, w), BF) for s in range(levels)]
    scratch += [dma((parts, levels + 1))] * 2 + [dma((parts, zero))] * 2 + [dma((zero,))] * 2
    scratch += [dma]
    local = pl.BlockSpec(memory_space=pltpu.VMEM)
    return pl.pallas_call(
        functools.partial(core_kernel, inner // heads, chunk, LAGS, spans, min(256, owned)),
        out_shape=(
            jax.ShapeDtypeStruct((count, inner), BF),
            jax.ShapeDtypeStruct((piece, columns), F32),
            jax.ShapeDtypeStruct((count, zero * owned), BF),
        ),
        in_specs=[pl.BlockSpec(memory_space=pltpu.HBM)] * 6,
        out_specs=[local] * 3,
        scratch_shapes=scratch,
        compiler_params=pltpu.CompilerParams(collective_id=0, vmem_limit_bytes=VMEM, has_side_effects=True),
    )(rows, weights, gy, a_log[None], dt_bias[None], d_skip[None])


def per_device(tokens, w_in, a_log, dt_bias, d_skip, grad_y):
    count, width = tokens.shape[1:]
    inner = grad_y.shape[2]
    rows = tokens.reshape(count, width)

    y_out, grad_w, grad_tokens = layer(
        rows, w_in.T, grad_y.reshape(count, inner), a_log, dt_bias, d_skip
    )
    grad_tokens = grad_tokens.reshape(1, count, width)
    return (y_out.reshape(1, count, inner), grad_tokens, grad_w)


def solution(mesh):
    placed = (P("zero", "seq", None), P("zero", None), P(), P(), P(), P("zero", "seq", None))
    return jax.shard_map(
        per_device,
        mesh=mesh,
        in_specs=placed,
        out_specs=(P("zero", "seq", None), P("zero", "seq", None), P(("seq", "zero"), None)),
        check_vma=False,
    )
```
